16 devices in a mesh: data: 2 (over y, z), seq: 8 (over x, core).
Axes of the slice: x: 4, y: 2, z: 1, core: 2. Of those that a mesh axis runs over, the one named last changes fastest.
The devices are a block of a 4x4x8 slice.
Arguments:
- tokens: bfloat16 [16, 2048, 3072], P('data', 'seq'), parts along dimension 0
- theta_q: bfloat16 [3072, 3072], replicated
- theta_k: bfloat16 [3072, 3072], replicated
- theta_v: bfloat16 [3072, 3072], replicated
- w_out: bfloat16 [3072, 3072], replicated
- w_init: float32 [48, 64, 64], replicated
- inner_lr: float32 [48], replicated
Outputs:
- output: bfloat16 [16, 2048, 3072], P('data', 'seq'), parts along dimension 0
There are 2 independent parts. The reference program is written for one: setup_inputs(seed, part) draws one part's arguments, and reference() takes and returns one part's arrays. A program takes and returns all parts, laid end to end along the dimension named above; an argument that names none is the same for every part.
All inputs are finite; a program needn't handle non-finite values.
Results may differ from the reference program's by a relative error of at most 0.00243997.
Values are sent between devices in bfloat16 or wider.
A program may use at most 768 MiB of HBM per device.

```python
import jax
import jax.numpy as jnp
from jax import lax

BATCH = 8
SEQ = 2048
D = 3072
HEADS = 48
HEAD = 64
MINI_BATCH = 16


def setup_inputs(seed: int = 0, part: int = 0) -> dict:
    root_key = jax.random.key(seed)
    shared = jax.random.split(root_key, 6)
    part_key = jax.random.fold_in(jax.random.key(seed + 1), part)
    width_qkv = HEADS * HEAD
    scale_in = D ** -0.5
    tokens = jax.random.normal(part_key, (BATCH, SEQ, D), jnp.float32)
    theta_q = jax.random.normal(shared[0], (D, width_qkv), jnp.float32) * scale_in
    theta_k = jax.random.normal(shared[1], (D, width_qkv), jnp.float32) * scale_in
    theta_v = jax.random.normal(shared[2], (D, width_qkv), jnp.float32) * scale_in
    w_out = jax.random.normal(shared[3], (width_qkv, D), jnp.float32) * width_qkv ** -0.5
    w_init = jax.random.normal(shared[4], (HEADS, HEAD, HEAD), jnp.float32) * HEAD ** -0.5
    inner_lr = jax.random.uniform(shared[5], (HEADS,), jnp.float32, 1.0, 3.0) * (MINI_BATCH / (2.0 * SEQ))
    return {
        "tokens": tokens.astype(jnp.bfloat16),
        "theta_q": theta_q.astype(jnp.bfloat16),
        "theta_k": theta_k.astype(jnp.bfloat16),
        "theta_v": theta_v.astype(jnp.bfloat16),
        "w_out": w_out.astype(jnp.bfloat16),
        "w_init": w_init,
        "inner_lr": inner_lr,
    }


def reference(tokens, theta_q, theta_k, theta_v, w_out, w_init, inner_lr):
    n_blocks = SEQ // MINI_BATCH
    width_qkv = HEADS * HEAD
    flat_tokens = tokens.reshape(BATCH * SEQ, D)

    def project(theta):
        projected = jnp.dot(flat_tokens, theta, preferred_element_type=jnp.float32).astype(jnp.bfloat16)
        return jnp.moveaxis(projected.reshape(BATCH, n_blocks, MINI_BATCH, HEADS, HEAD), 1, 0)

    step_size = ((2.0 / MINI_BATCH) * inner_lr)[None, :, None, None]

    def update(w_state, block_in):
        q_blk = block_in[0].astype(jnp.float32)
        k_blk = block_in[1].astype(jnp.float32)
        v_blk = block_in[2].astype(jnp.float32)
        residual = jnp.einsum("bthd,bhde->bthe", k_blk, w_state) - v_blk
        gradient = jnp.einsum("bthd,bthe->bhde", k_blk, residual)
        w_state = w_state - step_size * gradient
        return w_state, jnp.einsum("bthd,bhde->bthe", q_blk, w_state)

    w_start = jnp.broadcast_to(w_init[None], (BATCH, HEADS, HEAD, HEAD))
    _, inner_out = lax.scan(update, w_start, (project(theta_q), project(theta_k), project(theta_v)))
    inner_out = jnp.moveaxis(inner_out, 0, 1).reshape(BATCH * SEQ, width_qkv).astype(jnp.bfloat16)
    result = jnp.dot(inner_out, w_out, preferred_element_type=jnp.float32).astype(jnp.bfloat16)
    return result.reshape(BATCH, SEQ, D)
```

```python
import functools

import jax
import jax.numpy as jnp
from jax import lax
from jax.experimental import pallas as pl
from jax.experimental.pallas import tpu as pltpu
from jax.sharding import PartitionSpec as P

MINI_BATCH = 16
HEADS_PER_GROUP = 4
STEPS_PER_TRIP = 5
bf16, f32 = jnp.bfloat16, jnp.float32


def split3(x):
    a = x.astype(bf16)
    rest = x - a.astype(f32)
    b = rest.astype(bf16)
    return a, b, (rest - b.astype(f32)).astype(bf16)


def per_head_rows(x, low):
    rows = []
    for half in range(2):
        y = x[:, half * 128:(half + 1) * 128]
        turned = pltpu.roll(y, 64, 1)
        rows += [jnp.where(low, y, turned), jnp.where(low, turned, y)]
    return rows


def own_columns(z, low, first):
    t = MINI_BATCH
    return jnp.concatenate([
        jnp.where(low, z[first:first + t, :128], z[first + t:first + 2 * t, :128]),
        jnp.where(low, z[first + 2 * t:first + 3 * t, 128:], z[first + 3 * t:first + 4 * t, 128:])], axis=1)


def times_w(rows, w):
    m = jnp.concatenate(rows, axis=0)
    lhs = jnp.concatenate([m, m], axis=1)
    rhs = jnp.concatenate([*split3(w), jnp.zeros(w.shape, bf16)], axis=0)
    return jnp.dot(lhs, rhs, preferred_element_type=f32)


def k_transposed_times(k_rows, r, low):
    zero = jnp.zeros((MINI_BATCH, 128), bf16)
    rows = []
    for part in split3(r):
        a, b = part[:, :128], part[:, 128:]
        rows += [jnp.concatenate([jnp.where(low, a, zero), zero], axis=1), jnp.concatenate([jnp.where(low, zero, a), zero], axis=1),
                 jnp.concatenate([zero, jnp.where(low, b, zero)], axis=1), jnp.concatenate([zero, jnp.where(low, zero, b)], axis=1)]
    rhs = jnp.concatenate([*rows, jnp.zeros((4 * MINI_BATCH, 256), bf16)], axis=0)
    k_mat = jnp.concatenate(k_rows, axis=0)
    turned = jnp.concatenate([k_mat, k_mat], axis=0).T[:64]
    lhs = jnp.concatenate([turned, turned], axis=1)
    return jnp.dot(lhs, rhs, preferred_element_type=f32)


def inner_kernel(n_seq, n_batch, tok_dev, n_groups, q_hbm, k_hbm, v_hbm, w_init_ref, eta_ref, o_hbm,
                 q_buf, k_buf, v_buf, w_buf, in_sem, out_sem, send_sem, recv_sem):
    me = lax.axis_index("seq")
    barrier = pltpu.get_barrier_semaphore()

    def columns(g):
        return pl.ds(pl.multiple_of(g * 256, 256), 256)

    def loads(g):
        slot = lax.rem(g, 2)
        return [pltpu.make_async_copy(hbm.at[:, columns(g)], buf.at[slot], in_sem.at[i, slot])
                for i, (hbm, buf) in enumerate(((q_hbm, q_buf), (k_hbm, k_buf), (v_hbm, v_buf)))]

    def result(g):
        slot = lax.rem(g, 2)
        return pltpu.make_async_copy(q_buf.at[slot], o_hbm.at[:, columns(g)], out_sem.at[slot])

    def hand_on(g):
        return pltpu.make_async_remote_copy(w_buf.at[g], w_buf.at[g], send_sem.at[g], recv_sem.at[g],
                                            device_id={"seq": lax.rem(me + 1, n_seq)}, device_id_type=pl.DeviceIdType.MESH)

    for copy in loads(0):
        copy.start()

    for peer in (lax.rem(me + 1, n_seq), lax.rem(me + n_seq - 1, n_seq)):
        pl.semaphore_signal(barrier, inc=1, device_id={"seq": peer}, device_id_type=pl.DeviceIdType.MESH)
    pl.semaphore_wait(barrier, 2)

    low = lax.broadcasted_iota(jnp.int32, (MINI_BATCH, 128), 1) < 64
    n_steps = tok_dev // MINI_BATCH

    def group(g, _):
        slot = lax.rem(g, 2)

        @pl.when(g >= 1)
        def _():
            result(g - 1).wait()

        @pl.when(g + 1 < n_groups)
        def _():
            for copy in loads(g + 1):
                copy.start()

        for copy in loads(g):
            copy.wait()

        @pl.when(me == 0)
        def _():
            for b in range(n_batch):
                w_buf[g, b] = w_init_ref[g]

        @pl.when(me > 0)
        def _():
            hand_on(g).wait_recv()

        eta = eta_ref[g]

        def rows_of(b, j):
            start = b * tok_dev + j * MINI_BATCH
            return pl.ds(start if isinstance(start, int) else pl.multiple_of(start, MINI_BATCH), MINI_BATCH)

        def step(j, with_k, with_q):
            k_rows, z = {}, {}
            for b in range(n_batch):
                rows = []
                if with_k:
                    k_rows[b] = per_head_rows(k_buf[slot, rows_of(b, j), :], low)
                    rows += k_rows[b]
                if with_q:
                    rows += per_head_rows(q_buf[slot, rows_of(b, j - 1), :], low)
                prod = times_w(rows, w_buf[g, b])
                if with_k:
                    z[b] = own_columns(prod, low, 0)
                if with_q:
                    q_buf[slot, rows_of(b, j - 1), :] = own_columns(prod, low, 4 * MINI_BATCH if with_k else 0).astype(bf16)
            if with_k:
                for b in range(n_batch):
                    r = (z[b] - v_buf[slot, rows_of(b, j), :].astype(f32)) * eta
                    w_buf[g, b] -= k_transposed_times(k_rows[b], r, low)

        step(0, True, False)

        def trip(i, _):
            for s in range(STEPS_PER_TRIP):
                step(1 + i * STEPS_PER_TRIP + s, True, True)
            return 0

        lax.fori_loop(0, (n_steps - 1) // STEPS_PER_TRIP, trip, 0)

        @pl.when(me < n_seq - 1)
        def _():
            hand_on(g).start()

        step(n_steps, False, True)
        result(g).start()
        return 0

    lax.fori_loop(0, n_groups, group, 0)
    result(n_groups - 1).wait()

    @pl.when(me < n_seq - 1)
    def _():
        for g in range(n_groups):
            hand_on(g).wait_send()


def solution(mesh):
    n_seq = mesh.shape["seq"]

    def per_device(tokens, theta_q, theta_k, theta_v, w_out, w_init, inner_lr):
        n_batch, tok_dev, width_d = tokens.shape
        n_heads, head_dim, _ = w_init.shape
        n_groups = n_heads // HEADS_PER_GROUP
        n_rows, width = n_batch * tok_dev, n_heads * head_dim
        flat = tokens.reshape(n_rows, width_d)
        q, k, v = (jnp.dot(flat, theta, preferred_element_type=f32).astype(bf16) for theta in (theta_q, theta_k, theta_v))
        w_start = w_init.reshape(n_groups, HEADS_PER_GROUP, head_dim, head_dim).transpose(0, 2, 1, 3).reshape(n_groups, head_dim, 4 * head_dim)
        eta = jnp.repeat((2.0 / MINI_BATCH) * inner_lr, head_dim).reshape(n_groups, 1, 4 * head_dim)
        hbm, vmem = pl.BlockSpec(memory_space=pl.ANY), pl.BlockSpec(memory_space=pltpu.VMEM)
        slab = pltpu.VMEM((2, n_rows, 4 * head_dim), bf16)
        o = pl.pallas_call(
            functools.partial(inner_kernel, n_seq, n_batch, tok_dev, n_groups),
            out_shape=jax.ShapeDtypeStruct((n_rows, width), bf16),
            in_specs=[hbm, hbm, hbm, vmem, vmem], out_specs=hbm,
            scratch_shapes=[slab, slab, slab, pltpu.VMEM((n_groups, n_batch, head_dim, 4 * head_dim), f32),
                            pltpu.SemaphoreType.DMA((3, 2)), pltpu.SemaphoreType.DMA((2,)),
                            pltpu.SemaphoreType.DMA((n_groups,)), pltpu.SemaphoreType.DMA((n_groups,))],
            compiler_params=pltpu.CompilerParams(collective_id=0, has_side_effects=True, vmem_limit_bytes=48 * 1024 * 1024),
            name="inner",
        )(q, k, v, w_start, eta)
        result = jnp.dot(o, w_out, preferred_element_type=f32).astype(bf16)
        return result.reshape(n_batch, tok_dev, width_d)

    tok_spec = P("data", "seq", None)
    return jax.shard_map(per_device, mesh=mesh, in_specs=(tok_spec, P(), P(), P(), P(), P(), P()), out_specs=tok_spec, check_vma=False)
```

```python
import functools

import jax
import jax.numpy as jnp
from jax import lax
from jax.experimental import pallas as pl
from jax.experimental.pallas import tpu as pltpu
from jax.sharding import PartitionSpec as P

MINI_BATCH = 16
HEADS_PER_GROUP = 4
STEPS_PER_TRIP = 5
bf16, f32 = jnp.bfloat16, jnp.float32


def split3(x):
    a = x.astype(bf16)
    rest = x - a.astype(f32)
    b = rest.astype(bf16)
    return a, b, (rest - b.astype(f32)).astype(bf16)


def per_head_rows(x, low):
    rows = []
    for half in range(2):
        y = x[:, half * 128:(half + 1) * 128]
        turned = pltpu.roll(y, 64, 1)
        rows += [jnp.where(low, y, turned), jnp.where(low, turned, y)]
    return rows


def own_columns(z, low, first):
    t = MINI_BATCH
    return jnp.concatenate([
        jnp.where(low, z[first:first + t, :128], z[first + t:first + 2 * t, :128]),
        jnp.where(low, z[first + 2 * t:first + 3 * t, 128:], z[first + 3 * t:first + 4 * t, 128:])], axis=1)


def times_w(rows, w):
    m = jnp.concatenate(rows, axis=0)
    lhs = jnp.concatenate([m, m], axis=1)
    rhs = jnp.concatenate([*split3(w), jnp.zeros(w.shape, bf16)], axis=0)
    return jnp.dot(lhs, rhs, preferred_element_type=f32)


def k_transposed_times(k_rows, r, low):
    zero = jnp.zeros((MINI_BATCH, 128), bf16)
    rows = []
    for part in split3(r):
        a, b = part[:, :128], part[:, 128:]
        rows += [jnp.concatenate([jnp.where(low, a, zero), zero], axis=1), jnp.concatenate([jnp.where(low, zero, a), zero], axis=1),
                 jnp.concatenate([zero, jnp.where(low, b, zero)], axis=1), jnp.concatenate([zero, jnp.where(low, zero, b)], axis=1)]
    rhs = jnp.concatenate([*rows, jnp.zeros((4 * MINI_BATCH, 256), bf16)], axis=0)
    k_mat = jnp.concatenate(k_rows, axis=0)
    turned = jnp.concatenate([k_mat, k_mat], axis=0).T[:64]
    lhs = jnp.concatenate([turned, turned], axis=1)
    return jnp.dot(lhs, rhs, preferred_element_type=f32)


def inner_kernel(n_seq, n_batch, tok_dev, n_groups, q_hbm, k_hbm, v_hbm, w_init_ref, eta_ref, o_hbm,
                 q_buf, k_buf, v_buf, w_buf, w_now, in_sem, out_sem, send_sem, recv_sem):
    me = lax.axis_index("seq")
    barrier = pltpu.get_barrier_semaphore()

    def columns(g):
        return pl.ds(pl.multiple_of(g * 256, 256), 256)

    def loads(g):
        slot = lax.rem(g, 2)
        return [pltpu.make_async_copy(hbm.at[:, columns(g)], buf.at[slot], in_sem.at[i, slot])
                for i, (hbm, buf) in enumerate(((q_hbm, q_buf), (k_hbm, k_buf), (v_hbm, v_buf)))]

    def result(g):
        slot = lax.rem(g, 2)
        return pltpu.make_async_copy(q_buf.at[slot], o_hbm.at[:, columns(g)], out_sem.at[slot])

    def hand_on(g):
        return pltpu.make_async_remote_copy(w_buf.at[g], w_buf.at[g], send_sem.at[g], recv_sem.at[g],
                                            device_id={"seq": lax.rem(me + 1, n_seq)}, device_id_type=pl.DeviceIdType.MESH)

    for copy in loads(0):
        copy.start()

    for peer in (lax.rem(me + 1, n_seq), lax.rem(me + n_seq - 1, n_seq)):
        pl.semaphore_signal(barrier, inc=1, device_id={"seq": peer}, device_id_type=pl.DeviceIdType.MESH)
    pl.semaphore_wait(barrier, 2)

    low = lax.broadcasted_iota(jnp.int32, (MINI_BATCH, 128), 1) < 64
    n_steps = tok_dev // MINI_BATCH

    def group(g, _):
        slot = lax.rem(g, 2)

        @pl.when(g >= 1)
        def _():
            result(g - 1).wait()

        @pl.when(g + 1 < n_groups)
        def _():
            for copy in loads(g + 1):
                copy.start()

        for copy in loads(g):
            copy.wait()

        @pl.when(me == 0)
        def _():
            for b in range(n_batch):
                w_now[b] = w_init_ref[g]

        @pl.when(me > 0)
        def _():
            hand_on(g).wait_recv()
            w_now[...] = w_buf[g]

        eta = eta_ref[g]

        def rows_of(b, j):
            start = b * tok_dev + j * MINI_BATCH
            return pl.ds(start if isinstance(start, int) else pl.multiple_of(start, MINI_BATCH), MINI_BATCH)

        def step(j, with_k, with_q):
            k_rows, rows, z = {}, {}, {}
            for b in range(n_batch):
                rows[b] = []
                if with_k:
                    k_rows[b] = per_head_rows(k_buf[slot, rows_of(b, j), :], low)
                    rows[b] += k_rows[b]
                if with_q:
                    rows[b] += per_head_rows(q_buf[slot, rows_of(b, j - 1), :], low)
            prod = {b: times_w(rows[b], w_now[b]) for b in range(n_batch)}
            if with_k:
                z = {b: own_columns(prod[b], low, 0) for b in range(n_batch)}
            if with_q:
                for b in range(n_batch):
                    q_buf[slot, rows_of(b, j - 1), :] = own_columns(prod[b], low, 4 * MINI_BATCH if with_k else 0).astype(bf16)
            if with_k:
                for b in range(n_batch):
                    r = (z[b] - v_buf[slot, rows_of(b, j), :].astype(f32)) * eta
                    w_now[b] -= k_transposed_times(k_rows[b], r, low)

        step(0, True, False)

        def trip(i, _):
            for s in range(STEPS_PER_TRIP):
                step(1 + i * STEPS_PER_TRIP + s, True, True)
            return 0

        lax.fori_loop(0, (n_steps - 1) // STEPS_PER_TRIP, trip, 0)

        @pl.when(me < n_seq - 1)
        def _():
            w_buf[g] = w_now[...]
            hand_on(g).start()

        step(n_steps, False, True)
        result(g).start()
        return 0

    lax.fori_loop(0, n_groups, group, 0)
    result(n_groups - 1).wait()

    @pl.when(me < n_seq - 1)
    def _():
        for g in range(n_groups):
            hand_on(g).wait_send()


def solution(mesh):
    n_seq = mesh.shape["seq"]

    def per_device(tokens, theta_q, theta_k, theta_v, w_out, w_init, inner_lr):
        n_batch, tok_dev, width_d = tokens.shape
        n_heads, head_dim, _ = w_init.shape
        n_groups = n_heads // HEADS_PER_GROUP
        n_rows, width = n_batch * tok_dev, n_heads * head_dim
        flat = tokens.reshape(n_rows, width_d)
        q, k, v = (jnp.dot(flat, theta, preferred_element_type=f32).astype(bf16) for theta in (theta_q, theta_k, theta_v))
        w_start = w_init.reshape(n_groups, HEADS_PER_GROUP, head_dim, head_dim).transpose(0, 2, 1, 3).reshape(n_groups, head_dim, 4 * head_dim)
        eta = jnp.repeat((2.0 / MINI_BATCH) * inner_lr, head_dim).reshape(n_groups, 1, 4 * head_dim)
        hbm, vmem = pl.BlockSpec(memory_space=pl.ANY), pl.BlockSpec(memory_space=pltpu.VMEM)
        slab = pltpu.VMEM((2, n_rows, 4 * head_dim), bf16)
        o = pl.pallas_call(
            functools.partial(inner_kernel, n_seq, n_batch, tok_dev, n_groups),
            out_shape=jax.ShapeDtypeStruct((n_rows, width), bf16),
            in_specs=[hbm, hbm, hbm, vmem, vmem], out_specs=hbm,
            scratch_shapes=[slab, slab, slab, pltpu.VMEM((n_groups, n_batch, head_dim, 4 * head_dim), f32),
                            pltpu.VMEM((n_batch, head_dim, 4 * head_dim), f32),
                            pltpu.SemaphoreType.DMA((3, 2)), pltpu.SemaphoreType.DMA((2,)),
                            pltpu.SemaphoreType.DMA((n_groups,)), pltpu.SemaphoreType.DMA((n_groups,))],
            compiler_params=pltpu.CompilerParams(collective_id=0, has_side_effects=True, vmem_limit_bytes=48 * 1024 * 1024),
            name="inner",
        )(q, k, v, w_start, eta)
        result = jnp.dot(o, w_out, preferred_element_type=f32).astype(bf16)
        return result.reshape(n_batch, tok_dev, width_d)

    tok_spec = P("data", "seq", None)
    return jax.shard_map(per_device, mesh=mesh, in_specs=(tok_spec, P(), P(), P(), P(), P(), P()), out_specs=tok_spec, check_vma=False)
```

```python
import functools

import jax
import jax.numpy as jnp
from jax import lax
from jax.experimental import pallas as pl
from jax.experimental.pallas import tpu as pltpu
from jax.sharding import PartitionSpec as P

MINI_BATCH = 16
HEADS_PER_GROUP = 4
STEPS_PER_TRIP = 15
bf16, f32 = jnp.bfloat16, jnp.float32


def split3(x):
    a = x.astype(bf16)
    rest = x - a.astype(f32)
    b = rest.astype(bf16)
    return a, b, (rest - b.astype(f32)).astype(bf16)


def per_head_rows(x, low):
    rows = []
    for half in range(2):
        y = x[:, half * 128:(half + 1) * 128]
        turned = pltpu.roll(y, 64, 1)
        rows += [jnp.where(low, y, turned), jnp.where(low, turned, y)]
    return rows


def own_columns(z, low, first):
    t = MINI_BATCH
    return jnp.concatenate([
        jnp.where(low, z[first:first + t, :128], z[first + t:first + 2 * t, :128]),
        jnp.where(low, z[first + 2 * t:first + 3 * t, 128:], z[first + 3 * t:first + 4 * t, 128:])], axis=1)


def times_w(rows, w):
    m = jnp.concatenate(rows, axis=0)
    lhs = jnp.concatenate([m, m], axis=1)
    rhs = jnp.concatenate([*split3(w), jnp.zeros(w.shape, bf16)], axis=0)
    return jnp.dot(lhs, rhs, preferred_element_type=f32)


def k_transposed_times(k_rows, r, low):
    zero = jnp.zeros((MINI_BATCH, 128), bf16)
    rows = []
    for part in split3(r):
        a, b = part[:, :128], part[:, 128:]
        rows += [jnp.concatenate([jnp.where(low, a, zero), zero], axis=1), jnp.concatenate([jnp.where(low, zero, a), zero], axis=1),
                 jnp.concatenate([zero, jnp.where(low, b, zero)], axis=1), jnp.concatenate([zero, jnp.where(low, zero, b)], axis=1)]
    rhs = jnp.concatenate([*rows, jnp.zeros((4 * MINI_BATCH, 256), bf16)], axis=0)
    k_mat = jnp.concatenate(k_rows, axis=0)
    turned = jnp.concatenate([k_mat, k_mat], axis=0).T[:64]
    lhs = jnp.concatenate([turned, turned], axis=1)
    return jnp.dot(lhs, rhs, preferred_element_type=f32)


def fused_kernel(n_seq, n_batch, tok_dev, n_groups, x_hbm, theta_k_hbm, theta_v_hbm, theta_q_hbm, w_init_hbm, eta_ref, o_hbm,
                 x_buf, kvq_buf, theta_buf, tile_buf, o_buf, z_buf, w_buf, w_now, x_sem, theta_sem, out_sem, init_sem, send_sem, recv_sem):
    me = lax.axis_index("seq")
    lag = me
    n_rows = n_batch * tok_dev
    n_steps = tok_dev // MINI_BATCH
    chunk = n_rows // n_steps
    depth = x_buf.shape[1]
    thetas = (theta_k_hbm, theta_v_hbm, theta_q_hbm)
    barrier = pltpu.get_barrier_semaphore()

    def columns(g):
        return pl.ds(pl.multiple_of(g * 256, 256), 256)

    def theta_copy(kind, g):
        return pltpu.make_async_copy(thetas[kind].at[:, columns(g)], theta_buf.at[lax.rem(3 * g + kind, 2)], theta_sem.at[lax.rem(3 * g + kind, 2)])

    def start_theta(tile):
        g = tile // 3
        for kind in range(3):
            @pl.when((lax.rem(tile, 3) == kind) & (tile < 3 * n_groups))
            def _():
                theta_copy(kind, g).start()

    def wait_theta(tile):
        slot = lax.rem(tile, 2)
        pltpu.make_async_copy(theta_k_hbm.at[:, pl.ds(0, 256)], theta_buf.at[slot], theta_sem.at[slot]).wait()

    def result(g):
        return pltpu.make_async_copy(o_buf, o_hbm.at[:, columns(g)], out_sem)

    def hand_on(g):
        return pltpu.make_async_remote_copy(w_buf.at[g], w_buf.at[g], send_sem.at[g], recv_sem.at[g],
                                            device_id={"seq": lax.rem(me + 1, n_seq)}, device_id_type=pl.DeviceIdType.MESH)

    def first_w(g, b):
        return pltpu.make_async_copy(w_init_hbm.at[g], w_buf.at[g, b], init_sem.at[g])

    def x_copy(i):
        rows = pl.ds(i * (n_rows // 2), n_rows // 2)
        return pltpu.make_async_copy(x_hbm.at[rows], x_buf.at[rows], x_sem.at[i])

    start_theta(jnp.int32(0))
    for i in range(2):
        x_copy(i).start()

    @pl.when(me == 0)
    def _():
        def body(g, _):
            for b in range(n_batch):
                first_w(g, b).start()
            return 0
        lax.fori_loop(0, n_groups, body, 0)

    for peer in (lax.rem(me + 1, n_seq), lax.rem(me + n_seq - 1, n_seq)):
        pl.semaphore_signal(barrier, inc=1, device_id={"seq": peer}, device_id_type=pl.DeviceIdType.MESH)
    pl.semaphore_wait(barrier, 2)
    for i in range(2):
        x_copy(i).wait()

    low = lax.broadcasted_iota(jnp.int32, (MINI_BATCH, 128), 1) < 64

    def whole_tile(tile):
        g, kind, slot = tile // 3, lax.rem(tile, 3), lax.rem(tile, 2)
        wait_theta(tile)
        start_theta(tile + 1)
        for i in range(2):
            rows = pl.ds(i * (n_rows // 2), n_rows // 2)
            kvq_buf[kind, g, rows, :] = jnp.dot(x_buf[rows, :], theta_buf[slot], preferred_element_type=f32).astype(bf16)

    def inner(g, tile):
        slot = lax.rem(tile, 2)

        @pl.when(tile < 3 * n_groups)
        def _():
            wait_theta(tile)
            start_theta(tile + 1)

        @pl.when(me == 0)
        def _():
            for b in range(n_batch):
                first_w(g, b).wait()

        @pl.when(me > 0)
        def _():
            hand_on(g).wait_recv()

        @pl.when(g > 0)
        def _():
            result(g - 1).wait()

        w_now[...] = w_buf[g]
        eta = eta_ref[g]

        def rows_of(b, j):
            start = b * tok_dev + j * MINI_BATCH
            return pl.ds(start if isinstance(start, int) else pl.multiple_of(start, MINI_BATCH), MINI_BATCH)

        half = n_batch // 2

        def multiply(b, j, with_k, with_q):
            rows = per_head_rows(kvq_buf[0, g, rows_of(b, j), :], low) if with_k else []
            if with_q:
                rows = rows + per_head_rows(kvq_buf[2, g, rows_of(b, j - 1), :], low)
            prod = times_w(rows, w_now[b])
            if with_k:
                z_buf[b] = own_columns(prod, low, 0)
            if with_q:
                o_buf[rows_of(b, j - 1), :] = own_columns(prod, low, 4 * MINI_BATCH if with_k else 0).astype(bf16)

        def update(b, j):
            r = (z_buf[b] - kvq_buf[1, g, rows_of(b, j), :].astype(f32)) * eta
            w_now[b] -= k_transposed_times(per_head_rows(kvq_buf[0, g, rows_of(b, j), :], low), r, low)

        def step(j, first=False):
            part = pl.ds(j * chunk if isinstance(j, int) else pl.multiple_of(j * chunk, chunk), chunk)
            tile_part = jnp.dot(x_buf[part, :], theta_buf[slot], preferred_element_type=f32)
            for b in range(half):
                multiply(b, j, True, not first)
                if not first:
                    update(half + b, j - 1)
            for b in range(half):
                multiply(half + b, j, True, not first)
                update(b, j)
            tile_buf[part, :] = tile_part.astype(bf16)

        step(0, True)

        def trip(i, _):
            for s in range(STEPS_PER_TRIP):
                step(1 + i * STEPS_PER_TRIP + s)
            return 0

        lax.fori_loop(0, (n_steps - 1) // STEPS_PER_TRIP, trip, 0)
        for b in range(half):
            update(half + b, n_steps - 1)

        @pl.when(me < n_seq - 1)
        def _():
            w_buf[g] = w_now[...]
            hand_on(g).start()

        for b in range(n_batch):
            multiply(b, n_steps, False, True)
        result(g).start()

        @pl.when(tile < 3 * n_groups)
        def _():
            kvq_buf[lax.rem(tile, 3), tile // 3] = tile_buf[...]

    def slot_body(s, _):
        g = s - 1 - lag

        @pl.when(g >= 0)
        def _():
            inner(g, 3 * s)

        def rest(kind, _):
            whole_tile(3 * s + kind)
            return 0

        @pl.when(s < n_groups)
        def _():
            lax.fori_loop(jnp.where(g >= 0, 1, 0), 3, rest, 0)
        return 0

    lax.fori_loop(0, n_groups + 1 + lag, slot_body, 0)

    result(n_groups - 1).wait()

    @pl.when(me < n_seq - 1)
    def _():
        for g in range(n_groups):
            hand_on(g).wait_send()


def solution(mesh):
    n_seq = mesh.shape["seq"]

    def per_device(tokens, theta_q, theta_k, theta_v, w_out, w_init, inner_lr):
        n_batch, tok_dev, width_d = tokens.shape
        n_heads, head_dim, _ = w_init.shape
        n_groups = n_heads // HEADS_PER_GROUP
        n_rows, width = n_batch * tok_dev, n_heads * head_dim
        flat = tokens.reshape(n_rows, width_d)
        w_start = w_init.reshape(n_groups, HEADS_PER_GROUP, head_dim, head_dim).transpose(0, 2, 1, 3).reshape(n_groups, head_dim, 4 * head_dim)
        eta = jnp.repeat((2.0 / MINI_BATCH) * inner_lr, head_dim).reshape(n_groups, 1, 4 * head_dim)
        hbm, vmem = pl.BlockSpec(memory_space=pl.ANY), pl.BlockSpec(memory_space=pltpu.VMEM)
        o = pl.pallas_call(
            functools.partial(fused_kernel, n_seq, n_batch, tok_dev, n_groups),
            out_shape=jax.ShapeDtypeStruct((n_rows, width), bf16),
            in_specs=[hbm] * 5 + [vmem], out_specs=hbm,
            scratch_shapes=[pltpu.VMEM((n_rows, width_d), bf16), pltpu.VMEM((3, n_groups, n_rows, 256), bf16),
                            pltpu.VMEM((2, width_d, 256), bf16), pltpu.VMEM((n_rows, 256), bf16), pltpu.VMEM((n_rows, 256), bf16), pltpu.VMEM((n_batch, MINI_BATCH, 256), f32),
                            pltpu.VMEM((n_groups, n_batch, head_dim, 4 * head_dim), f32),
                            pltpu.VMEM((n_batch, head_dim, 4 * head_dim), f32),
                            pltpu.SemaphoreType.DMA((2,)), pltpu.SemaphoreType.DMA((2,)), pltpu.SemaphoreType.DMA,
                            pltpu.SemaphoreType.DMA((n_groups,)), pltpu.SemaphoreType.DMA((n_groups,)), pltpu.SemaphoreType.DMA((n_groups,))],
            compiler_params=pltpu.CompilerParams(collective_id=0, has_side_effects=True, vmem_limit_bytes=67043328),
            name="fused",
        )(flat, theta_k, theta_v, theta_q, w_start, eta)
        result = jnp.dot(o, w_out, preferred_element_type=f32).astype(bf16)
        return result.reshape(n_batch, tok_dev, width_d)

    tok_spec = P("data", "seq", None)
    return jax.shard_map(per_device, mesh=mesh, in_specs=(tok_spec, P(), P(), P(), P(), P(), P()), out_specs=tok_spec, check_vma=False)
```

```python
import functools

import jax
import jax.numpy as jnp
from jax import lax
from jax.experimental import pallas as pl
from jax.experimental.pallas import tpu as pltpu
from jax.sharding import PartitionSpec as P

MINI_BATCH = 16
HEADS_PER_GROUP = 4
STEPS_PER_TRIP = 15
SCHEDULE = ((0, 7), (1, 6), (2, 4), (3, 1), (3, 0), (3, 0), (5, 0), (7, 0))
bf16, f32 = jnp.bfloat16, jnp.float32


def split3(x):
    a = x.astype(bf16)
    rest = x - a.astype(f32)
    b = rest.astype(bf16)
    return a, b, (rest - b.astype(f32)).astype(bf16)


def per_head_rows(x, low):
    rows = []
    for half in range(2):
        y = x[:, half * 128:(half + 1) * 128]
        turned = pltpu.roll(y, 64, 1)
        rows += [jnp.where(low, y, turned), jnp.where(low, turned, y)]
    return rows


def own_columns(z, low, first):
    t = MINI_BATCH
    return jnp.concatenate([
        jnp.where(low, z[first:first + t, :128], z[first + t:first + 2 * t, :128]),
        jnp.where(low, z[first + 2 * t:first + 3 * t, 128:], z[first + 3 * t:first + 4 * t, 128:])], axis=1)


def times_w(rows, w):
    m = jnp.concatenate(rows, axis=0)
    lhs = jnp.concatenate([m, m], axis=1)
    rhs = jnp.concatenate([*split3(w), jnp.zeros(w.shape, bf16)], axis=0)
    return jnp.dot(lhs, rhs, preferred_element_type=f32)


def k_transposed_times(k_rows, r, low):
    zero = jnp.zeros((MINI_BATCH, 128), bf16)
    rows = []
    for part in split3(r):
        a, b = part[:, :128], part[:, 128:]
        rows += [jnp.concatenate([jnp.where(low, a, zero), zero], axis=1), jnp.concatenate([jnp.where(low, zero, a), zero], axis=1),
                 jnp.concatenate([zero, jnp.where(low, b, zero)], axis=1), jnp.concatenate([zero, jnp.where(low, zero, b)], axis=1)]
    rhs = jnp.concatenate([*rows, jnp.zeros((4 * MINI_BATCH, 256), bf16)], axis=0)
    k_mat = jnp.concatenate(k_rows, axis=0)
    turned = jnp.concatenate([k_mat, k_mat], axis=0).T[:64]
    lhs = jnp.concatenate([turned, turned], axis=1)
    return jnp.dot(lhs, rhs, preferred_element_type=f32)


def fused_kernel(n_seq, n_batch, tok_dev, n_groups, x_hbm, theta_k_hbm, theta_v_hbm, theta_q_hbm, w_init_hbm, eta_ref, o_hbm,
                 x_buf, kvq_buf, theta_buf, tile_buf, o_buf, z_buf, w_buf, w_now, w_send, x_sem, theta_sem, out_sem, init_sem, send_sem, recv_sem):
    me = lax.axis_index("seq")
    lag, n_late = jnp.int32(0), jnp.int32(0)
    for place, (ahead, late) in enumerate(SCHEDULE):
        lag = jnp.where(me == place, ahead, lag)
        n_late = jnp.where(me == place, late, n_late)
    n_tiles = 3 * n_groups
    n_rows = n_batch * tok_dev
    n_steps = tok_dev // MINI_BATCH
    chunk = n_rows // n_steps
    depth = x_buf.shape[1]
    thetas = (theta_k_hbm, theta_v_hbm, theta_q_hbm)
    barrier = pltpu.get_barrier_semaphore()

    def columns(g):
        return pl.ds(pl.multiple_of(g * 256, 256), 256)

    def tile_at(c):
        early, body = 2 * n_late, c - 2 * n_late
        kind = jnp.where(c < early, lax.rem(c, 2), jnp.where(c < n_tiles - n_late, lax.rem(body, 3), 2))
        g = jnp.where(c < early, c // 2, jnp.where(c < n_tiles - n_late, n_late + body // 3, c - (n_tiles - n_late)))
        return kind, g

    def start_theta(c):
        kind, g = tile_at(c)
        for i in range(3):
            @pl.when((kind == i) & (c < n_tiles))
            def _():
                pltpu.make_async_copy(thetas[i].at[:, columns(g)], theta_buf.at[lax.rem(c, 2)], theta_sem.at[lax.rem(c, 2)]).start()

    def wait_theta(c):
        slot = lax.rem(c, 2)
        pltpu.make_async_copy(theta_k_hbm.at[:, pl.ds(0, 256)], theta_buf.at[slot], theta_sem.at[slot]).wait()

    def result(g):
        return pltpu.make_async_copy(o_buf, o_hbm.at[:, columns(g)], out_sem)

    def hand_on(g):
        return pltpu.make_async_remote_copy(w_send, w_buf.at[g], send_sem, recv_sem.at[g],
                                            device_id={"seq": lax.rem(me + 1, n_seq)}, device_id_type=pl.DeviceIdType.MESH)

    def first_w(g, b):
        return pltpu.make_async_copy(w_init_hbm.at[g], w_buf.at[g, b], init_sem.at[g])

    def x_copy(i):
        rows = pl.ds(i * (n_rows // 2), n_rows // 2)
        return pltpu.make_async_copy(x_hbm.at[rows], x_buf.at[rows], x_sem.at[i])

    start_theta(jnp.int32(0))
    for i in range(2):
        x_copy(i).start()

    @pl.when(me == 0)
    def _():
        def body(g, _):
            for b in range(n_batch):
                first_w(g, b).start()
            return 0
        lax.fori_loop(0, n_groups, body, 0)

    for peer in (lax.rem(me + 1, n_seq), lax.rem(me + n_seq - 1, n_seq)):
        pl.semaphore_signal(barrier, inc=1, device_id={"seq": peer}, device_id_type=pl.DeviceIdType.MESH)
    pl.semaphore_wait(barrier, 2)
    for i in range(2):
        x_copy(i).wait()

    low = lax.broadcasted_iota(jnp.int32, (MINI_BATCH, 128), 1) < 64

    def whole_tile(c):
        kind, g = tile_at(c)
        slot = lax.rem(c, 2)
        wait_theta(c)
        start_theta(c + 1)
        for i in range(2):
            rows = pl.ds(i * (n_rows // 2), n_rows // 2)
            kvq_buf[kind, g, rows, :] = jnp.dot(x_buf[rows, :], theta_buf[slot], preferred_element_type=f32).astype(bf16)

    def inner(g, first_time, c):
        slot = lax.rem(c, 2)
        has_q = jnp.logical_not(first_time) | (g >= n_late)

        @pl.when(c < n_tiles)
        def _():
            wait_theta(c)
            start_theta(c + 1)

        @pl.when((me == 0) & first_time)
        def _():
            for b in range(n_batch):
                first_w(g, b).wait()

        @pl.when((me > 0) & first_time)
        def _():
            hand_on(g).wait_recv()

        @pl.when(has_q & jnp.where(first_time, g > n_late, (g > 0) | (n_late < n_groups)))
        def _():
            result(0).wait()

        w_now[...] = w_buf[g]
        eta = eta_ref[g]

        def rows_of(b, j):
            start = b * tok_dev + j * MINI_BATCH
            return pl.ds(start if isinstance(start, int) else pl.multiple_of(start, MINI_BATCH), MINI_BATCH)

        half = n_batch // 2

        def multiply(b, j, with_k, with_q):
            rows = per_head_rows(kvq_buf[0, g, rows_of(b, j), :], low) if with_k else []
            if with_q:
                rows = rows + per_head_rows(kvq_buf[2, g, rows_of(b, j - 1), :], low)
            prod = times_w(rows, w_now[b])
            if with_k:
                z_buf[b] = own_columns(prod, low, 0)
            if with_q:
                o_buf[rows_of(b, j - 1), :] = own_columns(prod, low, 4 * MINI_BATCH if with_k else 0).astype(bf16)

        def update(b, j):
            r = (z_buf[b] - kvq_buf[1, g, rows_of(b, j), :].astype(f32)) * eta
            w_now[b] -= k_transposed_times(per_head_rows(kvq_buf[0, g, rows_of(b, j), :], low), r, low)

        def step(j, first=False):
            part = pl.ds(j * chunk if isinstance(j, int) else pl.multiple_of(j * chunk, chunk), chunk)
            tile_part = jnp.dot(x_buf[part, :], theta_buf[slot], preferred_element_type=f32)
            for b in range(half):
                multiply(b, j, True, not first)
                if not first:
                    update(half + b, j - 1)
            for b in range(half):
                multiply(half + b, j, True, not first)
                update(b, j)
            tile_buf[part, :] = tile_part.astype(bf16)

        step(0, True)

        def trip(i, _):
            for s in range(STEPS_PER_TRIP):
                step(1 + i * STEPS_PER_TRIP + s)
            return 0

        lax.fori_loop(0, (n_steps - 1) // STEPS_PER_TRIP, trip, 0)
        for b in range(half):
            update(half + b, n_steps - 1)

        @pl.when((me < n_seq - 1) & first_time & (g > 0))
        def _():
            hand_on(0).wait_send()

        @pl.when((me < n_seq - 1) & first_time)
        def _():
            w_send[...] = w_now[...]
            hand_on(g).start()

        for b in range(n_batch):
            multiply(b, n_steps, False, True)

        @pl.when(has_q)
        def _():
            result(g).start()

        @pl.when(c < n_tiles)
        def _():
            kind, of = tile_at(c)
            kvq_buf[kind, of] = tile_buf[...]

    def slot_body(s, _):
        first_time = s <= n_groups + lag
        g = jnp.where(first_time, s - 1 - lag, s - (n_groups + 1 + lag))
        fresh = s < n_groups
        c = jnp.where(fresh, 2 * s + jnp.maximum(s - n_late, 0), n_tiles - n_late + s - n_groups)

        @pl.when(g >= 0)
        def _():
            inner(g, first_time, c)

        def rest(i, _):
            whole_tile(c + i)
            return 0

        @pl.when(fresh)
        def _():
            lax.fori_loop(jnp.where(g >= 0, 1, 0), jnp.where(s < n_late, 2, 3), rest, 0)
        return 0

    lax.fori_loop(0, n_groups + 1 + lag + n_late, slot_body, 0)

    result(0).wait()

    @pl.when(me < n_seq - 1)
    def _():
        hand_on(0).wait_send()


def solution(mesh):
    n_seq = mesh.shape["seq"]

    def per_device(tokens, theta_q, theta_k, theta_v, w_out, w_init, inner_lr):
        n_batch, tok_dev, width_d = tokens.shape
        n_heads, head_dim, _ = w_init.shape
        n_groups = n_heads // HEADS_PER_GROUP
        n_rows, width = n_batch * tok_dev, n_heads * head_dim
        flat = tokens.reshape(n_rows, width_d)
        w_start = w_init.reshape(n_groups, HEADS_PER_GROUP, head_dim, head_dim).transpose(0, 2, 1, 3).reshape(n_groups, head_dim, 4 * head_dim)
        eta = jnp.repeat((2.0 / MINI_BATCH) * inner_lr, head_dim).reshape(n_groups, 1, 4 * head_dim)
        hbm, vmem = pl.BlockSpec(memory_space=pl.ANY), pl.BlockSpec(memory_space=pltpu.VMEM)
        o = pl.pallas_call(
            functools.partial(fused_kernel, n_seq, n_batch, tok_dev, n_groups),
            out_shape=jax.ShapeDtypeStruct((n_rows, width), bf16),
            in_specs=[hbm] * 5 + [vmem], out_specs=hbm,
            scratch_shapes=[pltpu.VMEM((n_rows, width_d), bf16), pltpu.VMEM((3, n_groups, n_rows, 256), bf16),
                            pltpu.VMEM((2, width_d, 256), bf16), pltpu.VMEM((n_rows, 256), bf16), pltpu.VMEM((n_rows, 256), bf16), pltpu.VMEM((n_batch, MINI_BATCH, 256), f32),
                            pltpu.VMEM((n_groups, n_batch, head_dim, 4 * head_dim), f32),
                            pltpu.VMEM((n_batch, head_dim, 4 * head_dim), f32), pltpu.VMEM((n_batch, head_dim, 4 * head_dim), f32),
                            pltpu.SemaphoreType.DMA((2,)), pltpu.SemaphoreType.DMA((2,)), pltpu.SemaphoreType.DMA,
                            pltpu.SemaphoreType.DMA((n_groups,)), pltpu.SemaphoreType.DMA, pltpu.SemaphoreType.DMA((n_groups,))],
            compiler_params=pltpu.CompilerParams(collective_id=0, has_side_effects=True, vmem_limit_bytes=67043328),
            name="fused",
        )(flat, theta_k, theta_v, theta_q, w_start, eta)
        result = jnp.dot(o, w_out, preferred_element_type=f32).astype(bf16)
        return result.reshape(n_batch, tok_dev, width_d)

    tok_spec = P("data", "seq", None)
    return jax.shard_map(per_device, mesh=mesh, in_specs=(tok_spec, P(), P(), P(), P(), P(), P()), out_specs=tok_spec, check_vma=False)
```

```python
import functools

import jax
import jax.numpy as jnp
from jax import lax
from jax.experimental import pallas as pl
from jax.experimental.pallas import tpu as pltpu
from jax.sharding import PartitionSpec as P

MINI_BATCH = 16
HEADS_PER_GROUP = 4
STEPS_PER_TRIP = 15
SCHEDULE = ((0, 7, 0), (1, 6, 0), (2, 4, 0), (3, 1, 0), (3, 0, 1), (3, 0, 1), (5, 0, 1), (7, 0, 1))
N_FIRST = 8
bf16, f32 = jnp.bfloat16, jnp.float32


def split3(x):
    a = x.astype(bf16)
    rest = x - a.astype(f32)
    b = rest.astype(bf16)
    return a, b, (rest - b.astype(f32)).astype(bf16)


def per_head_rows(x, low):
    rows = []
    for half in range(2):
        y = x[:, half * 128:(half + 1) * 128]
        turned = pltpu.roll(y, 64, 1)
        rows += [jnp.where(low, y, turned), jnp.where(low, turned, y)]
    return rows


def own_columns(z, low, first):
    t = MINI_BATCH
    return jnp.concatenate([
        jnp.where(low, z[first:first + t, :128], z[first + t:first + 2 * t, :128]),
        jnp.where(low, z[first + 2 * t:first + 3 * t, 128:], z[first + 3 * t:first + 4 * t, 128:])], axis=1)


def times_w(rows, w):
    m = jnp.concatenate(rows, axis=0)
    lhs = jnp.concatenate([m, m], axis=1)
    rhs = jnp.concatenate([*split3(w), jnp.zeros(w.shape, bf16)], axis=0)
    return jnp.dot(lhs, rhs, preferred_element_type=f32)


def k_transposed_times(k_rows, r, low):
    zero = jnp.zeros((MINI_BATCH, 128), bf16)
    rows = []
    for part in split3(r):
        a, b = part[:, :128], part[:, 128:]
        rows += [jnp.concatenate([jnp.where(low, a, zero), zero], axis=1), jnp.concatenate([jnp.where(low, zero, a), zero], axis=1),
                 jnp.concatenate([zero, jnp.where(low, b, zero)], axis=1), jnp.concatenate([zero, jnp.where(low, zero, b)], axis=1)]
    rhs = jnp.concatenate([*rows, jnp.zeros((4 * MINI_BATCH, 256), bf16)], axis=0)
    k_mat = jnp.concatenate(k_rows, axis=0)
    turned = jnp.concatenate([k_mat, k_mat], axis=0).T[:64]
    lhs = jnp.concatenate([turned, turned], axis=1)
    return jnp.dot(lhs, rhs, preferred_element_type=f32)


def fused_kernel(n_seq, n_batch, tok_dev, n_groups, x_hbm, theta_k_hbm, theta_v_hbm, theta_q_hbm, w_out_hbm, w_init_hbm, eta_ref, o_hbm, sum_hbm,
                 x_buf, kvq_buf, theta_buf, tile_buf, o_buf, z_buf, w_buf, w_now, w_send, init_buf, x_sem, theta_sem, out_sem, sum_sem, init_sem, send_sem, recv_sem):
    me = lax.axis_index("seq")
    lag, n_late, early_out = jnp.int32(0), jnp.int32(0), jnp.int32(0)
    for place, (ahead, late, early) in enumerate(SCHEDULE):
        lag = jnp.where(me == place, ahead, lag)
        n_late = jnp.where(me == place, late, n_late)
        early_out = jnp.where(me == place, early, early_out)
    n_tiles = 3 * n_groups
    n_out_tiles = sum_hbm.shape[-1] // 256
    first_depth = N_FIRST * 256
    outs_per_slot = n_out_tiles // (n_groups - N_FIRST)
    n_rows = n_batch * tok_dev
    n_steps = tok_dev // MINI_BATCH
    chunk = n_rows // n_steps
    depth = x_buf.shape[1]
    thetas = (theta_k_hbm, theta_v_hbm, theta_q_hbm)
    barrier = pltpu.get_barrier_semaphore()

    def columns(g):
        return pl.ds(pl.multiple_of(g * 256, 256), 256)

    def tile_at(c):
        early, body = 2 * n_late, c - 2 * n_late
        kind = jnp.where(c < early, lax.rem(c, 2), jnp.where(c < n_tiles - n_late, lax.rem(body, 3), 2))
        g = jnp.where(c < early, c // 2, jnp.where(c < n_tiles - n_late, n_late + body // 3, c - (n_tiles - n_late)))
        return kind, g

    def start_theta(c):
        kind, g = tile_at(c)
        for i in range(3):
            @pl.when((kind == i) & (c < n_tiles))
            def _():
                pltpu.make_async_copy(thetas[i].at[:, columns(g)], theta_buf.at[lax.rem(c, 2)], theta_sem.at[lax.rem(c, 2)]).start()

        @pl.when((c >= n_tiles) & (c < n_tiles + n_out_tiles))
        def _():
            w_out_copy(c - n_tiles, lax.rem(c, 2)).start()

    def w_out_copy(n, slot):
        return pltpu.make_async_copy(w_out_hbm.at[pl.ds(0, first_depth), columns(n)], theta_buf.at[slot, pl.ds(0, first_depth)], theta_sem.at[slot])

    def wait_theta(c):
        slot = lax.rem(c, 2)
        pltpu.make_async_copy(theta_k_hbm.at[:, pl.ds(0, 256)], theta_buf.at[slot], theta_sem.at[slot]).wait()

    def result(g):
        return pltpu.make_async_copy(o_buf, o_hbm.at[:, columns(g - N_FIRST)], out_sem)

    def sum_copy(n):
        part = lax.rem(n, 2)
        return pltpu.make_async_copy(w_buf.at[pl.ds(part * sum_slots, sum_slots)], sum_hbm.at[:, :, :, columns(n)], sum_sem.at[part])

    def hand_on(g):
        return pltpu.make_async_remote_copy(w_send, w_buf.at[g], send_sem, recv_sem.at[g],
                                            device_id={"seq": lax.rem(me + 1, n_seq)}, device_id_type=pl.DeviceIdType.MESH)

    sum_slots = sum_hbm.shape[0]

    def first_w(g):
        return pltpu.make_async_copy(w_init_hbm.at[pl.ds(g * HEADS_PER_GROUP, HEADS_PER_GROUP)], init_buf, init_sem)

    def x_copy(i):
        rows = pl.ds(i * (n_rows // 2), n_rows // 2)
        return pltpu.make_async_copy(x_hbm.at[rows], x_buf.at[rows], x_sem.at[i])

    start_theta(jnp.int32(0))
    for i in range(2):
        x_copy(i).start()

    @pl.when(me == 0)
    def _():
        first_w(0).start()

    for peer in (lax.rem(me + 1, n_seq), lax.rem(me + n_seq - 1, n_seq)):
        pl.semaphore_signal(barrier, inc=1, device_id={"seq": peer}, device_id_type=pl.DeviceIdType.MESH)
    pl.semaphore_wait(barrier, 2)
    for i in range(2):
        x_copy(i).wait()

    low = lax.broadcasted_iota(jnp.int32, (MINI_BATCH, 128), 1) < 64

    def whole_tile(c):
        kind, g = tile_at(c)
        slot = lax.rem(c, 2)
        wait_theta(c)
        start_theta(c + 1)
        for i in range(2):
            rows = pl.ds(i * (n_rows // 2), n_rows // 2)
            kvq_buf[kind, g, rows, :] = jnp.dot(x_buf[rows, :], theta_buf[slot], preferred_element_type=f32).astype(bf16)

    def out_tile(n):
        c = n_tiles + n
        slot = lax.rem(c, 2)
        w_out_copy(n, slot).wait()
        start_theta(c + 1)

        @pl.when(n >= 2)
        def _():
            sum_copy(n - 2).wait()

        for i in range(2):
            rows = pl.ds(i * (n_rows // 2), n_rows // 2)
            lhs = jnp.concatenate([kvq_buf[2, g, rows, :] for g in range(N_FIRST)], axis=1)
            part = jnp.dot(lhs, theta_buf[slot, :first_depth, :], preferred_element_type=f32)
            w_buf[pl.ds(lax.rem(n, 2) * sum_slots + i * (sum_slots // 2), sum_slots // 2)] = part.reshape(sum_slots // 2, *w_buf.shape[1:])
        sum_copy(n).start()

    def inner(g, first_time, c):
        slot = lax.rem(jnp.where(c < n_tiles, c, c - 1), 2)
        has_q = jnp.logical_not(first_time) | (g >= n_late)

        @pl.when(c < n_tiles)
        def _():
            wait_theta(c)
            start_theta(c + 1)

        @pl.when((me == 0) & first_time)
        def _():
            first_w(g).wait()
            start = jnp.concatenate([init_buf[h] for h in range(HEADS_PER_GROUP)], axis=1)
            for b in range(n_batch):
                w_buf[g, b] = start

        @pl.when((me == 0) & first_time & (g + 1 < n_groups))
        def _():
            first_w(g + 1).start()

        @pl.when((me > 0) & first_time)
        def _():
            hand_on(g).wait_recv()

        @pl.when(jnp.where(first_time, g > N_FIRST, g == 0))
        def _():
            result(N_FIRST).wait()

        w_now[...] = w_buf[g]
        eta = eta_ref[g]

        def rows_of(b, j):
            start = b * tok_dev + j * MINI_BATCH
            return pl.ds(start if isinstance(start, int) else pl.multiple_of(start, MINI_BATCH), MINI_BATCH)

        half = n_batch // 2

        def multiply(b, j, with_k, with_q):
            rows = per_head_rows(kvq_buf[0, g, rows_of(b, j), :], low) if with_k else []
            if with_q:
                rows = rows + per_head_rows(kvq_buf[2, g, rows_of(b, j - 1), :], low)
            prod = times_w(rows, w_now[b])
            if with_k:
                z_buf[b] = own_columns(prod, low, 0)
            if with_q:
                o_buf[rows_of(b, j - 1), :] = own_columns(prod, low, 4 * MINI_BATCH if with_k else 0).astype(bf16)

        def update(b, j):
            r = (z_buf[b] - kvq_buf[1, g, rows_of(b, j), :].astype(f32)) * eta
            w_now[b] -= k_transposed_times(per_head_rows(kvq_buf[0, g, rows_of(b, j), :], low), r, low)

        def step(j, first=False):
            part = pl.ds(j * chunk if isinstance(j, int) else pl.multiple_of(j * chunk, chunk), chunk)
            tile_part = jnp.dot(x_buf[part, :], theta_buf[slot], preferred_element_type=f32)
            for b in range(half):
                multiply(b, j, True, not first)
                if not first:
                    update(half + b, j - 1)
            for b in range(half):
                multiply(half + b, j, True, not first)
                update(b, j)
            tile_buf[part, :] = tile_part.astype(bf16)

        step(0, True)

        def trip(i, _):
            for s in range(STEPS_PER_TRIP):
                step(1 + i * STEPS_PER_TRIP + s)
            return 0

        lax.fori_loop(0, (n_steps - 1) // STEPS_PER_TRIP, trip, 0)
        for b in range(half):
            update(half + b, n_steps - 1)

        @pl.when((me < n_seq - 1) & first_time & (g > 0))
        def _():
            hand_on(0).wait_send()

        @pl.when((me < n_seq - 1) & first_time)
        def _():
            w_send[...] = w_now[...]
            hand_on(g).start()

        for b in range(n_batch):
            multiply(b, n_steps, False, True)

        @pl.when(has_q & (g >= N_FIRST))
        def _():
            result(g).start()

        @pl.when(has_q & (g < N_FIRST))
        def _():
            kvq_buf[2, g] = o_buf[...]

        @pl.when(c < n_tiles)
        def _():
            kind, of = tile_at(c)
            kvq_buf[kind, of] = tile_buf[...]

    def slot_body(s, _):
        first_time = s <= n_groups + lag
        g = jnp.where(first_time, s - 1 - lag, s - (n_groups + 1 + lag))
        fresh = s < n_groups
        c = jnp.where(fresh, 2 * s + jnp.maximum(s - n_late, 0), jnp.minimum(n_tiles - n_late + s - n_groups, n_tiles))
        out_now = (early_out > 0) & first_time & (g >= N_FIRST)
        n_out = jnp.where(out_now, outs_per_slot * (g - N_FIRST), 0)

        def outs(n, _):
            out_tile(n)
            return 0

        lax.fori_loop(n_out, jnp.where(out_now, n_out + outs_per_slot, n_out), outs, 0)
        c_inner = jnp.where(out_now, n_tiles + n_out + outs_per_slot, c)

        @pl.when(g >= 0)
        def _():
            inner(g, first_time, c_inner)

        def rest(i, _):
            whole_tile(c + i)
            return 0

        @pl.when(fresh)
        def _():
            lax.fori_loop(jnp.where(g >= 0, 1, 0), jnp.where(s < n_late, 2, 3), rest, 0)
        return 0

    lax.fori_loop(0, n_groups + 1 + lag + n_late, slot_body, 0)

    def outs(n, _):
        out_tile(n)
        return 0

    lax.fori_loop(jnp.where(early_out > 0, n_out_tiles, 0), n_out_tiles, outs, 0)
    for n in range(2):
        sum_copy(n_out_tiles - 2 + n).wait()

    @pl.when(n_late == 0)
    def _():
        result(N_FIRST).wait()

    @pl.when(me < n_seq - 1)
    def _():
        hand_on(0).wait_send()


def solution(mesh):
    n_seq = mesh.shape["seq"]

    def per_device(tokens, theta_q, theta_k, theta_v, w_out, w_init, inner_lr):
        n_batch, tok_dev, width_d = tokens.shape
        n_heads, head_dim, _ = w_init.shape
        n_groups = n_heads // HEADS_PER_GROUP
        n_rows, width = n_batch * tok_dev, n_heads * head_dim
        flat = tokens.reshape(n_rows, width_d)
        eta = jnp.repeat((2.0 / MINI_BATCH) * inner_lr, head_dim).reshape(n_groups, 1, 4 * head_dim)
        hbm, vmem = pl.BlockSpec(memory_space=pl.ANY), pl.BlockSpec(memory_space=pltpu.VMEM)
        sum_slots = n_rows // (n_batch * head_dim)
        o, first_sum = pl.pallas_call(
            functools.partial(fused_kernel, n_seq, n_batch, tok_dev, n_groups),
            out_shape=(jax.ShapeDtypeStruct((n_rows, width - 256 * N_FIRST), bf16), jax.ShapeDtypeStruct((sum_slots, n_batch, head_dim, width_d), f32)),
            in_specs=[hbm] * 6 + [vmem], out_specs=(hbm, hbm),
            scratch_shapes=[pltpu.VMEM((n_rows, width_d), bf16), pltpu.VMEM((3, n_groups, n_rows, 256), bf16),
                            pltpu.VMEM((2, width_d, 256), bf16), pltpu.VMEM((n_rows, 256), bf16), pltpu.VMEM((n_rows, 256), bf16), pltpu.VMEM((n_batch, MINI_BATCH, 256), f32),
                            pltpu.VMEM((n_groups, n_batch, head_dim, 4 * head_dim), f32),
                            pltpu.VMEM((n_batch, head_dim, 4 * head_dim), f32), pltpu.VMEM((n_batch, head_dim, 4 * head_dim), f32),
                            pltpu.VMEM((HEADS_PER_GROUP, head_dim, head_dim), f32),
                            pltpu.SemaphoreType.DMA((2,)), pltpu.SemaphoreType.DMA((2,)), pltpu.SemaphoreType.DMA, pltpu.SemaphoreType.DMA((2,)),
                            pltpu.SemaphoreType.DMA, pltpu.SemaphoreType.DMA, pltpu.SemaphoreType.DMA((n_groups,))],
            compiler_params=pltpu.CompilerParams(collective_id=0, has_side_effects=True, vmem_limit_bytes=67043328),
            name="fused",
        )(flat, theta_k, theta_v, theta_q, w_out, w_init, eta)
        rest = jnp.dot(o, w_out[256 * N_FIRST:], preferred_element_type=f32)
        result = (rest + first_sum.reshape(n_rows, width_d)).astype(bf16)
        return result.reshape(n_batch, tok_dev, width_d)

    tok_spec = P("data", "seq", None)
    return jax.shard_map(per_device, mesh=mesh, in_specs=(tok_spec, P(), P(), P(), P(), P(), P()), out_specs=tok_spec, check_vma=False)
```

```python
import functools

import jax
import jax.numpy as jnp
from jax import lax
from jax.experimental import pallas as pl
from jax.experimental.pallas import tpu as pltpu
from jax.sharding import PartitionSpec as P

MINI_BATCH = 16
HEADS_PER_GROUP = 4
SCHEDULE = ((0, 3, (0, 0, 0, 0)), (1, 2, (0, 0, 0, 0)), (1, 1, (0, 0, 0, 0)), (2, 1, (0, 0, 0, 0)),
            (4, 0, (4, 7, 10, 10)), (5, 0, (6, 10, 10, 10)), (7, 0, (11, 11, 11, 11)), (8, 0, (11, 11, 11, 11)))
N_FIRST = 8
FILL = 768
bf16, f32 = jnp.bfloat16, jnp.float32


def split3(x):
    a = x.astype(bf16)
    rest = x - a.astype(f32)
    b = rest.astype(bf16)
    return a, b, (rest - b.astype(f32)).astype(bf16)


def per_head_rows(x, low):
    rows = []
    for half in range(2):
        y = x[:, half * 128:(half + 1) * 128]
        turned = pltpu.roll(y, 64, 1)
        rows += [jnp.where(low, y, turned), jnp.where(low, turned, y)]
    return rows


def own_columns(z, low, first):
    t = MINI_BATCH
    return jnp.concatenate([
        jnp.where(low, z[first:first + t, :128], z[first + t:first + 2 * t, :128]),
        jnp.where(low, z[first + 2 * t:first + 3 * t, 128:], z[first + 3 * t:first + 4 * t, 128:])], axis=1)


def times_w(rows, w):
    m = jnp.concatenate(rows, axis=0)
    lhs = jnp.concatenate([m, m], axis=1)
    rhs = jnp.concatenate([*split3(w), jnp.zeros(w.shape, bf16)], axis=0)
    return jnp.dot(lhs, rhs, preferred_element_type=f32)


def k_transposed_times(k_rows, r, low):
    zero = jnp.zeros((MINI_BATCH, 128), bf16)
    rows = []
    for part in split3(r):
        a, b = part[:, :128], part[:, 128:]
        rows += [jnp.concatenate([jnp.where(low, a, zero), zero], axis=1), jnp.concatenate([jnp.where(low, zero, a), zero], axis=1),
                 jnp.concatenate([zero, jnp.where(low, b, zero)], axis=1), jnp.concatenate([zero, jnp.where(low, zero, b)], axis=1)]
    rhs = jnp.concatenate([*rows, jnp.zeros((4 * MINI_BATCH, 256), bf16)], axis=0)
    k_mat = jnp.concatenate(k_rows, axis=0)
    turned = jnp.concatenate([k_mat, k_mat], axis=0).T[:64]
    lhs = jnp.concatenate([turned, turned], axis=1)
    return jnp.dot(lhs, rhs, preferred_element_type=f32)


def fused_kernel(n_seq, n_batch, tok_dev, n_groups, x_hbm, theta_k_hbm, theta_v_hbm, theta_q_hbm, w_out_hbm, w_init_hbm, eta_ref, o_hbm, sum_hbm,
                 x_buf, kvq_buf, theta_buf, tile_buf, o_buf, z_buf, w_buf, w_now, w_send, init_buf, x_sem, theta_sem, out_sem, sum_sem, init_sem, send_sem, recv_sem):
    me = lax.axis_index("seq")
    lag, n_late = jnp.int32(0), jnp.int32(0)
    for place, (ahead, late, _) in enumerate(SCHEDULE):
        lag = jnp.where(me == place, ahead, lag)
        n_late = jnp.where(me == place, late, n_late)

    def outs_before(g):
        n = jnp.int32(0)
        for place, (_, _, counts) in enumerate(SCHEDULE):
            for i, count in enumerate(counts):
                n = jnp.where((me == place) & (g >= N_FIRST + i), count, n)
        return n

    n_tiles = 3 * n_groups
    n_out_tiles = sum_hbm.shape[-1] // 256
    first_depth = N_FIRST * 256
    n_rows = n_batch * tok_dev
    n_steps = tok_dev // MINI_BATCH
    chunk = n_rows // n_steps
    depth = x_buf.shape[1]
    thetas = (theta_k_hbm, theta_v_hbm, theta_q_hbm)
    barrier = pltpu.get_barrier_semaphore()

    def columns(g):
        return pl.ds(pl.multiple_of(g * 256, 256), 256)

    def tile_at(c):
        early, body = 2 * n_late, c - 2 * n_late
        kind = jnp.where(c < early, lax.rem(c, 2), jnp.where(c < n_tiles - n_late, lax.rem(body, 3), 2))
        g = jnp.where(c < early, c // 2, jnp.where(c < n_tiles - n_late, n_late + body // 3, c - (n_tiles - n_late)))
        return kind, g

    def start_theta(c):
        kind, g = tile_at(c)
        for i in range(3):
            @pl.when((kind == i) & (c < n_tiles))
            def _():
                pltpu.make_async_copy(thetas[i].at[:, columns(g)], theta_buf.at[lax.rem(c, 2)], theta_sem.at[lax.rem(c, 2)]).start()

        @pl.when((c >= n_tiles) & (c < n_tiles + n_out_tiles))
        def _():
            w_out_copy(c - n_tiles, lax.rem(c, 2)).start()

    def w_out_copy(n, slot):
        return pltpu.make_async_copy(w_out_hbm.at[pl.ds(0, first_depth), columns(n)], theta_buf.at[slot, pl.ds(0, first_depth)], theta_sem.at[slot])

    def wait_theta(c):
        slot = lax.rem(c, 2)
        pltpu.make_async_copy(theta_k_hbm.at[:, pl.ds(0, 256)], theta_buf.at[slot], theta_sem.at[slot]).wait()

    def result(g):
        return pltpu.make_async_copy(o_buf, o_hbm.at[:, columns(g - N_FIRST)], out_sem)

    def sum_copy(n):
        part = lax.rem(n, 2)
        return pltpu.make_async_copy(w_buf.at[pl.ds(part * sum_slots, sum_slots)], sum_hbm.at[:, :, :, columns(n)], sum_sem.at[part])

    def hand_on(g):
        return pltpu.make_async_remote_copy(w_send, w_buf.at[g], send_sem, recv_sem.at[g],
                                            device_id={"seq": lax.rem(me + 1, n_seq)}, device_id_type=pl.DeviceIdType.MESH)

    sum_slots = sum_hbm.shape[0]

    def first_w(g):
        return pltpu.make_async_copy(w_init_hbm.at[pl.ds(g * HEADS_PER_GROUP, HEADS_PER_GROUP)], init_buf, init_sem)

    def x_copy(i):
        rows = pl.ds(i * (n_rows // 2), n_rows // 2)
        return pltpu.make_async_copy(x_hbm.at[rows], x_buf.at[rows], x_sem.at[i])

    start_theta(jnp.int32(0))
    for i in range(2):
        x_copy(i).start()

    @pl.when(me == 0)
    def _():
        first_w(0).start()

    for peer in (lax.rem(me + 1, n_seq), lax.rem(me + n_seq - 1, n_seq)):
        pl.semaphore_signal(barrier, inc=1, device_id={"seq": peer}, device_id_type=pl.DeviceIdType.MESH)
    pl.semaphore_wait(barrier, 2)
    for i in range(2):
        x_copy(i).wait()

    low = lax.broadcasted_iota(jnp.int32, (MINI_BATCH, 128), 1) < 64

    def whole_tile(c):
        kind, g = tile_at(c)
        slot = lax.rem(c, 2)
        wait_theta(c)
        start_theta(c + 1)
        for i in range(2):
            rows = pl.ds(i * (n_rows // 2), n_rows // 2)
            kvq_buf[kind, g, rows, :] = jnp.dot(x_buf[rows, :], theta_buf[slot], preferred_element_type=f32).astype(bf16)

    def out_tile(n):
        c = n_tiles + n
        slot = lax.rem(c, 2)
        w_out_copy(n, slot).wait()
        start_theta(c + 1)

        @pl.when(n >= 2)
        def _():
            sum_copy(n - 2).wait()

        for i in range(2):
            rows = pl.ds(i * (n_rows // 2), n_rows // 2)
            lhs = jnp.concatenate([kvq_buf[2, g, rows, :] for g in range(N_FIRST)], axis=1)
            part = jnp.dot(lhs, theta_buf[slot, :first_depth, :], preferred_element_type=f32)
            w_buf[pl.ds(lax.rem(n, 2) * sum_slots + i * (sum_slots // 2), sum_slots // 2)] = part.reshape(sum_slots // 2, *w_buf.shape[1:])
        sum_copy(n).start()

    def inner(g, first_time, c, fill):
        slot = lax.rem(jnp.where(c < n_tiles, c, c - 1), 2)
        has_q = jnp.logical_not(first_time) | (g >= n_late)

        @pl.when(c < n_tiles)
        def _():
            wait_theta(c)
            start_theta(c + 1)

        @pl.when((me == 0) & first_time)
        def _():
            first_w(g).wait()
            start = jnp.concatenate([init_buf[h] for h in range(HEADS_PER_GROUP)], axis=1)
            for b in range(n_batch):
                w_buf[g, b] = start

        @pl.when((me == 0) & first_time & (g + 1 < n_groups))
        def _():
            first_w(g + 1).start()

        @pl.when((me > 0) & first_time)
        def _():
            hand_on(g).wait_recv()

        @pl.when(jnp.where(first_time, g > N_FIRST, g == 0))
        def _():
            result(N_FIRST).wait()

        eta = eta_ref[g]

        def rows_of(b, j):
            start = b * tok_dev + j * MINI_BATCH
            return pl.ds(start if isinstance(start, int) else pl.multiple_of(start, MINI_BATCH), MINI_BATCH)

        half = n_batch // 2

        def multiply(b, j, with_k, with_q):
            rows = per_head_rows(kvq_buf[0, g, rows_of(b, j), :], low) if with_k else []
            if with_q:
                rows = rows + per_head_rows(kvq_buf[2, g, rows_of(b, j - 1), :], low)
            prod = times_w(rows, w_now[b] if with_k and with_q or not with_k else w_buf[g, b])
            if with_k:
                z_buf[b] = own_columns(prod, low, 0)
            if with_q:
                o_buf[rows_of(b, j - 1), :] = own_columns(prod, low, 4 * MINI_BATCH if with_k else 0).astype(bf16)

        def update(b, j, first=False):
            r = (z_buf[b] - kvq_buf[1, g, rows_of(b, j), :].astype(f32)) * eta
            w_now[b] = (w_buf[g, b] if first else w_now[b]) - k_transposed_times(per_head_rows(kvq_buf[0, g, rows_of(b, j), :], low), r, low)

        def step(j, first=False, second=False):
            part = pl.ds(j * chunk if isinstance(j, int) else pl.multiple_of(j * chunk, chunk), chunk)
            tile_part = jnp.dot(x_buf[part, :fill], theta_buf[slot, :fill, :], preferred_element_type=f32)
            for b in range(half):
                multiply(b, j, True, not first)
                if not first:
                    update(half + b, j - 1, second)
            for b in range(half):
                multiply(half + b, j, True, not first)
                update(b, j, first)
            tile_buf[part, :] = tile_part.astype(bf16)

        step(0, first=True)
        step(1, second=True)

        def later_step(j, _):
            step(j)
            return 0

        lax.fori_loop(2, n_steps, later_step, 0)
        for b in range(half):
            update(half + b, n_steps - 1)

        @pl.when((me < n_seq - 1) & first_time & (g > 0))
        def _():
            hand_on(0).wait_send()

        @pl.when((me < n_seq - 1) & first_time)
        def _():
            w_send[...] = w_now[...]
            hand_on(g).start()

        for b in range(n_batch):
            multiply(b, n_steps, False, True)

        @pl.when(has_q & (g >= N_FIRST))
        def _():
            result(g).start()

        @pl.when(has_q & (g < N_FIRST))
        def _():
            kvq_buf[2, g] = o_buf[...]

        @pl.when(c < n_tiles)
        def _():
            kind, of = tile_at(c)
            kvq_buf[kind, of] = tile_buf[...]

    def slot_body(s, _):
        first_time = s <= n_groups + lag
        g = jnp.where(first_time, s - 1 - lag, s - (n_groups + 1 + lag))
        fresh = s < n_groups
        c = jnp.where(fresh, 2 * s + jnp.maximum(s - n_late, 0), jnp.minimum(n_tiles - n_late + s - n_groups, n_tiles))
        n_out = jnp.where(first_time, outs_before(g), 0)

        def outs(n, _):
            out_tile(n)
            return 0

        lax.fori_loop(jnp.where(first_time, outs_before(g - 1), 0), n_out, outs, 0)

        @pl.when((g >= 0) & (c < n_tiles))
        def _():
            inner(g, first_time, c + n_out, depth)

        @pl.when((g >= 0) & (c >= n_tiles))
        def _():
            inner(g, first_time, c + n_out, FILL)

        def rest(i, _):
            whole_tile(c + i)
            return 0

        @pl.when(fresh)
        def _():
            lax.fori_loop(jnp.where(g >= 0, 1, 0), jnp.where(s < n_late, 2, 3), rest, 0)
        return 0

    lax.fori_loop(0, n_groups + 1 + lag + n_late, slot_body, 0)

    def outs(n, _):
        out_tile(n)
        return 0

    lax.fori_loop(outs_before(n_groups), n_out_tiles, outs, 0)
    for n in range(2):
        sum_copy(n_out_tiles - 2 + n).wait()

    @pl.when(n_late == 0)
    def _():
        result(N_FIRST).wait()

    @pl.when(me < n_seq - 1)
    def _():
        hand_on(0).wait_send()


def solution(mesh):
    n_seq = mesh.shape["seq"]

    def per_device(tokens, theta_q, theta_k, theta_v, w_out, w_init, inner_lr):
        n_batch, tok_dev, width_d = tokens.shape
        n_heads, head_dim, _ = w_init.shape
        n_groups = n_heads // HEADS_PER_GROUP
        n_rows, width = n_batch * tok_dev, n_heads * head_dim
        flat = tokens.reshape(n_rows, width_d)
        eta = jnp.repeat((2.0 / MINI_BATCH) * inner_lr, head_dim).reshape(n_groups, 1, 4 * head_dim)
        hbm, vmem = pl.BlockSpec(memory_space=pl.ANY), pl.BlockSpec(memory_space=pltpu.VMEM)
        sum_slots = n_rows // (n_batch * head_dim)
        o, first_sum = pl.pallas_call(
            functools.partial(fused_kernel, n_seq, n_batch, tok_dev, n_groups),
            out_shape=(jax.ShapeDtypeStruct((n_rows, width - 256 * N_FIRST), bf16), jax.ShapeDtypeStruct((sum_slots, n_batch, head_dim, width_d), f32)),
            in_specs=[hbm] * 6 + [vmem], out_specs=(hbm, hbm),
            scratch_shapes=[pltpu.VMEM((n_rows, width_d), bf16), pltpu.VMEM((3, n_groups, n_rows, 256), bf16),
                            pltpu.VMEM((2, width_d, 256), bf16), pltpu.VMEM((n_rows, 256), bf16), pltpu.VMEM((n_rows, 256), bf16), pltpu.VMEM((n_batch, MINI_BATCH, 256), f32),
                            pltpu.VMEM((n_groups, n_batch, head_dim, 4 * head_dim), f32),
                            pltpu.VMEM((n_batch, head_dim, 4 * head_dim), f32), pltpu.VMEM((n_batch, head_dim, 4 * head_dim), f32),
                            pltpu.VMEM((HEADS_PER_GROUP, head_dim, head_dim), f32),
                            pltpu.SemaphoreType.DMA((2,)), pltpu.SemaphoreType.DMA((2,)), pltpu.SemaphoreType.DMA, pltpu.SemaphoreType.DMA((2,)),
                            pltpu.SemaphoreType.DMA, pltpu.SemaphoreType.DMA, pltpu.SemaphoreType.DMA((n_groups,))],
            compiler_params=pltpu.CompilerParams(collective_id=0, has_side_effects=True, vmem_limit_bytes=67043328),
            name="fused",
        )(flat, theta_k, theta_v, theta_q, w_out, w_init, eta)
        rest = jnp.dot(o, w_out[256 * N_FIRST:], preferred_element_type=f32)
        result = (rest + first_sum.reshape(n_rows, width_d)).astype(bf16)
        return result.reshape(n_batch, tok_dev, width_d)

    tok_spec = P("data", "seq", None)
    return jax.shard_map(per_device, mesh=mesh, in_specs=(tok_spec, P(), P(), P(), P(), P(), P()), out_specs=tok_spec, check_vma=False)
```

```python
import functools

import jax
import jax.numpy as jnp
from jax import lax
from jax.experimental import pallas as pl
from jax.experimental.pallas import tpu as pltpu
from jax.sharding import PartitionSpec as P

MINI_BATCH = 16
HEADS_PER_GROUP = 4
SCHEDULE = ((0, 3, (0, 0, 0, 0)), (1, 2, (0, 0, 0, 0)), (1, 1, (0, 0, 0, 0)), (2, 1, (0, 0, 0, 0)),
            (4, 0, (4, 7, 10, 10)), (5, 0, (6, 10, 10, 10)), (7, 0, (11, 11, 11, 11)), (8, 0, (11, 11, 11, 11)))
N_FIRST = 8
FILL = 768
bf16, f32 = jnp.bfloat16, jnp.float32


def split3(x):
    a = x.astype(bf16)
    rest = x - a.astype(f32)
    b = rest.astype(bf16)
    return a, b, (rest - b.astype(f32)).astype(bf16)


def per_head_rows(x, low):
    rows = []
    for half in range(2):
        y = x[:, half * 128:(half + 1) * 128]
        turned = pltpu.roll(y, 64, 1)
        rows += [jnp.where(low, y, turned), jnp.where(low, turned, y)]
    return rows


def own_columns(z, low, first):
    t = MINI_BATCH
    return jnp.concatenate([
        jnp.where(low, z[first:first + t, :128], z[first + t:first + 2 * t, :128]),
        jnp.where(low, z[first + 2 * t:first + 3 * t, 128:], z[first + 3 * t:first + 4 * t, 128:])], axis=1)


def times_w(rows, w):
    m = jnp.concatenate(rows, axis=0)
    lhs = jnp.concatenate([m, m], axis=1)
    rhs = jnp.concatenate([*split3(w), jnp.zeros(w.shape, bf16)], axis=0)
    return jnp.dot(lhs, rhs, preferred_element_type=f32)


def k_transposed_times(k_rows, r, low):
    zero = jnp.zeros((MINI_BATCH, 128), bf16)
    rows = []
    for part in split3(r):
        a, b = part[:, :128], part[:, 128:]
        rows += [jnp.concatenate([jnp.where(low, a, zero), zero], axis=1), jnp.concatenate([jnp.where(low, zero, a), zero], axis=1),
                 jnp.concatenate([zero, jnp.where(low, b, zero)], axis=1), jnp.concatenate([zero, jnp.where(low, zero, b)], axis=1)]
    rhs = jnp.concatenate([*rows, jnp.zeros((4 * MINI_BATCH, 256), bf16)], axis=0)
    k_mat = jnp.concatenate(k_rows, axis=0)
    turned = jnp.concatenate([k_mat, k_mat], axis=0).T[:64]
    lhs = jnp.concatenate([turned, turned], axis=1)
    return jnp.dot(lhs, rhs, preferred_element_type=f32)


def fused_kernel(n_seq, n_batch, tok_dev, n_groups, x_hbm, theta_k_hbm, theta_v_hbm, theta_q_hbm, w_out_hbm, w_init_hbm, eta_ref, o_hbm, sum_hbm,
                 x_buf, kvq_buf, theta_buf, tile_buf, o_buf, z_buf, w_buf, w_now, w_send, init_buf, x_sem, theta_sem, out_sem, sum_sem, init_sem, send_sem, recv_sem):
    me = lax.axis_index("seq")
    lag, n_late = jnp.int32(0), jnp.int32(0)
    for place, (ahead, late, _) in enumerate(SCHEDULE):
        lag = jnp.where(me == place, ahead, lag)
        n_late = jnp.where(me == place, late, n_late)

    def outs_before(g):
        n = jnp.int32(0)
        for place, (_, _, counts) in enumerate(SCHEDULE):
            for i, count in enumerate(counts):
                n = jnp.where((me == place) & (g >= N_FIRST + i), count, n)
        return n

    n_tiles = 3 * n_groups
    n_out_tiles = sum_hbm.shape[-1] // 256
    first_depth = N_FIRST * 256
    n_rows = n_batch * tok_dev
    n_steps = tok_dev // MINI_BATCH
    chunk = n_rows // n_steps
    depth = x_buf.shape[1]
    thetas = (theta_k_hbm, theta_v_hbm, theta_q_hbm)
    barrier = pltpu.get_barrier_semaphore()

    def columns(g):
        return pl.ds(pl.multiple_of(g * 256, 256), 256)

    def tile_at(c):
        early, body = 2 * n_late, c - 2 * n_late
        kind = jnp.where(c < early, lax.rem(c, 2), jnp.where(c < n_tiles - n_late, lax.rem(body, 3), 2))
        g = jnp.where(c < early, c // 2, jnp.where(c < n_tiles - n_late, n_late + body // 3, c - (n_tiles - n_late)))
        return kind, g

    def start_theta(c):
        kind, g = tile_at(c)
        for i in range(3):
            @pl.when((kind == i) & (c < n_tiles))
            def _():
                pltpu.make_async_copy(thetas[i].at[:, columns(g)], theta_buf.at[lax.rem(c, 2)], theta_sem.at[lax.rem(c, 2)]).start()

        @pl.when((c >= n_tiles) & (c < n_tiles + n_out_tiles))
        def _():
            w_out_copy(c - n_tiles, lax.rem(c, 2)).start()

    def w_out_copy(n, slot):
        return pltpu.make_async_copy(w_out_hbm.at[pl.ds(0, first_depth), columns(n)], theta_buf.at[slot, pl.ds(0, first_depth)], theta_sem.at[slot])

    def wait_theta(c):
        slot = lax.rem(c, 2)
        pltpu.make_async_copy(theta_k_hbm.at[:, pl.ds(0, 256)], theta_buf.at[slot], theta_sem.at[slot]).wait()

    def result(g):
        return pltpu.make_async_copy(o_buf, o_hbm.at[:, columns(g - N_FIRST)], out_sem)

    def sum_copy(n):
        part = lax.rem(n, 2)
        return pltpu.make_async_copy(w_buf.at[pl.ds(part * sum_slots, sum_slots)], sum_hbm.at[:, :, :, columns(n)], sum_sem.at[part])

    def hand_on(g):
        return pltpu.make_async_remote_copy(w_send, w_buf.at[g], send_sem, recv_sem.at[g],
                                            device_id={"seq": lax.rem(me + 1, n_seq)}, device_id_type=pl.DeviceIdType.MESH)

    sum_slots = sum_hbm.shape[0]

    def first_w(g):
        return pltpu.make_async_copy(w_init_hbm.at[pl.ds(g * HEADS_PER_GROUP, HEADS_PER_GROUP)], init_buf, init_sem)

    def x_copy(i):
        rows = pl.ds(i * (n_rows // 2), n_rows // 2)
        return pltpu.make_async_copy(x_hbm.at[rows], x_buf.at[rows], x_sem.at[i])

    start_theta(jnp.int32(0))
    for i in range(2):
        x_copy(i).start()

    @pl.when(me == 0)
    def _():
        first_w(0).start()

    for peer in (lax.rem(me + 1, n_seq), lax.rem(me + n_seq - 1, n_seq)):
        pl.semaphore_signal(barrier, inc=1, device_id={"seq": peer}, device_id_type=pl.DeviceIdType.MESH)
    pl.semaphore_wait(barrier, 2)
    for i in range(2):
        x_copy(i).wait()

    low = lax.broadcasted_iota(jnp.int32, (MINI_BATCH, 128), 1) < 64

    def whole_tile(c):
        kind, g = tile_at(c)
        slot = lax.rem(c, 2)
        wait_theta(c)
        start_theta(c + 1)
        for i in range(2):
            rows = pl.ds(i * (n_rows // 2), n_rows // 2)
            kvq_buf[kind, g, rows, :] = jnp.dot(x_buf[rows, :], theta_buf[slot], preferred_element_type=f32).astype(bf16)

    def out_tile(n):
        c = n_tiles + n
        slot = lax.rem(c, 2)
        w_out_copy(n, slot).wait()
        start_theta(c + 1)

        @pl.when(n >= 2)
        def _():
            sum_copy(n - 2).wait()

        for i in range(2):
            rows = pl.ds(i * (n_rows // 2), n_rows // 2)
            lhs = jnp.concatenate([kvq_buf[2, g, rows, :] for g in range(N_FIRST)], axis=1)
            part = jnp.dot(lhs, theta_buf[slot, :first_depth, :], preferred_element_type=f32)
            w_buf[pl.ds(lax.rem(n, 2) * sum_slots + i * (sum_slots // 2), sum_slots // 2)] = part.reshape(sum_slots // 2, *w_buf.shape[1:])
        sum_copy(n).start()

    def inner(g, first_time, c, fill, per_trip):
        slot = lax.rem(jnp.where(c < n_tiles, c, c - 1), 2)
        has_q = jnp.logical_not(first_time) | (g >= n_late)

        @pl.when(c < n_tiles)
        def _():
            wait_theta(c)
            start_theta(c + 1)

        @pl.when((me == 0) & first_time)
        def _():
            first_w(g).wait()
            start = jnp.concatenate([init_buf[h] for h in range(HEADS_PER_GROUP)], axis=1)
            for b in range(n_batch):
                w_buf[g, b] = start

        @pl.when((me == 0) & first_time & (g + 1 < n_groups))
        def _():
            first_w(g + 1).start()

        @pl.when((me > 0) & first_time)
        def _():
            hand_on(g).wait_recv()

        @pl.when(jnp.where(first_time, g > N_FIRST, g == 0))
        def _():
            result(N_FIRST).wait()

        eta = eta_ref[g]

        def rows_of(b, j):
            start = b * tok_dev + j * MINI_BATCH
            return pl.ds(start if isinstance(start, int) else pl.multiple_of(start, MINI_BATCH), MINI_BATCH)

        half = n_batch // 2

        def multiply(b, j, with_k, with_q):
            k_rows = rows = per_head_rows(kvq_buf[0, g, rows_of(b, j), :], low) if with_k else []
            if with_q:
                rows = rows + per_head_rows(kvq_buf[2, g, rows_of(b, j - 1), :], low)
            prod = times_w(rows, w_now[b] if with_k and with_q or not with_k else w_buf[g, b])
            if with_k:
                z_buf[b] = own_columns(prod, low, 0)
            if with_q:
                o_buf[rows_of(b, j - 1), :] = own_columns(prod, low, 4 * MINI_BATCH if with_k else 0).astype(bf16)
            return k_rows

        def update(b, j, k_rows=None, first=False):
            k_rows = k_rows or per_head_rows(kvq_buf[0, g, rows_of(b, j), :], low)
            r = (z_buf[b] - kvq_buf[1, g, rows_of(b, j), :].astype(f32)) * eta
            w_now[b] = (w_buf[g, b] if first else w_now[b]) - k_transposed_times(k_rows, r, low)

        def step(j, first=False, second=False):
            part = pl.ds(j * chunk if isinstance(j, int) else pl.multiple_of(j * chunk, chunk), chunk)
            tile_part = jnp.dot(x_buf[part, :fill], theta_buf[slot, :fill, :], preferred_element_type=f32)
            k_rows = {}
            for b in range(half):
                k_rows[b] = multiply(b, j, True, not first)
                if not first:
                    update(half + b, j - 1, first=second)
            for b in range(half):
                multiply(half + b, j, True, not first)
                update(b, j, k_rows[b], first)
            tile_buf[part, :] = tile_part.astype(bf16)

        step(0, first=True)
        step(1, second=True)

        def later_steps(i, _):
            for s in range(per_trip):
                step(2 + i * per_trip + s)
            return 0

        lax.fori_loop(0, (n_steps - 2) // per_trip, later_steps, 0)
        for b in range(half):
            update(half + b, n_steps - 1)

        @pl.when((me < n_seq - 1) & first_time & (g > 0))
        def _():
            hand_on(0).wait_send()

        @pl.when((me < n_seq - 1) & first_time)
        def _():
            w_send[...] = w_now[...]
            hand_on(g).start()

        for b in range(n_batch):
            multiply(b, n_steps, False, True)

        @pl.when(has_q & (g >= N_FIRST))
        def _():
            result(g).start()

        @pl.when(has_q & (g < N_FIRST))
        def _():
            kvq_buf[2, g] = o_buf[...]

        @pl.when(c < n_tiles)
        def _():
            kind, of = tile_at(c)
            kvq_buf[kind, of] = tile_buf[...]

    def slot_body(s, _):
        first_time = s <= n_groups + lag
        g = jnp.where(first_time, s - 1 - lag, s - (n_groups + 1 + lag))
        fresh = s < n_groups
        c = jnp.where(fresh, 2 * s + jnp.maximum(s - n_late, 0), jnp.minimum(n_tiles - n_late + s - n_groups, n_tiles))
        n_out = jnp.where(first_time, outs_before(g), 0)

        def outs(n, _):
            out_tile(n)
            return 0

        lax.fori_loop(jnp.where(first_time, outs_before(g - 1), 0), n_out, outs, 0)

        @pl.when((g >= 0) & (c < n_tiles))
        def _():
            inner(g, first_time, c + n_out, depth, (n_steps - 2) // 2)

        @pl.when((g >= 0) & (c >= n_tiles))
        def _():
            inner(g, first_time, c + n_out, FILL, (n_steps - 2) // 2)

        def rest(i, _):
            whole_tile(c + i)
            return 0

        @pl.when(fresh)
        def _():
            lax.fori_loop(jnp.where(g >= 0, 1, 0), jnp.where(s < n_late, 2, 3), rest, 0)
        return 0

    lax.fori_loop(0, n_groups + 1 + lag + n_late, slot_body, 0)

    def outs(n, _):
        out_tile(n)
        return 0

    lax.fori_loop(outs_before(n_groups), n_out_tiles, outs, 0)
    for n in range(2):
        sum_copy(n_out_tiles - 2 + n).wait()

    @pl.when(n_late == 0)
    def _():
        result(N_FIRST).wait()

    @pl.when(me < n_seq - 1)
    def _():
        hand_on(0).wait_send()


def solution(mesh):
    n_seq = mesh.shape["seq"]

    def per_device(tokens, theta_q, theta_k, theta_v, w_out, w_init, inner_lr):
        n_batch, tok_dev, width_d = tokens.shape
        n_heads, head_dim, _ = w_init.shape
        n_groups = n_heads // HEADS_PER_GROUP
        n_rows, width = n_batch * tok_dev, n_heads * head_dim
        flat = tokens.reshape(n_rows, width_d)
        eta = jnp.repeat((2.0 / MINI_BATCH) * inner_lr, head_dim).reshape(n_groups, 1, 4 * head_dim)
        hbm, vmem = pl.BlockSpec(memory_space=pl.ANY), pl.BlockSpec(memory_space=pltpu.VMEM)
        sum_slots = n_rows // (n_batch * head_dim)
        o, first_sum = pl.pallas_call(
            functools.partial(fused_kernel, n_seq, n_batch, tok_dev, n_groups),
            out_shape=(jax.ShapeDtypeStruct((n_rows, width - 256 * N_FIRST), bf16), jax.ShapeDtypeStruct((sum_slots, n_batch, head_dim, width_d), f32)),
            in_specs=[hbm] * 6 + [vmem], out_specs=(hbm, hbm),
            scratch_shapes=[pltpu.VMEM((n_rows, width_d), bf16), pltpu.VMEM((3, n_groups, n_rows, 256), bf16),
                            pltpu.VMEM((2, width_d, 256), bf16), pltpu.VMEM((n_rows, 256), bf16), pltpu.VMEM((n_rows, 256), bf16), pltpu.VMEM((n_batch, MINI_BATCH, 256), f32),
                            pltpu.VMEM((n_groups, n_batch, head_dim, 4 * head_dim), f32),
                            pltpu.VMEM((n_batch, head_dim, 4 * head_dim), f32), pltpu.VMEM((n_batch, head_dim, 4 * head_dim), f32),
                            pltpu.VMEM((HEADS_PER_GROUP, head_dim, head_dim), f32),
                            pltpu.SemaphoreType.DMA((2,)), pltpu.SemaphoreType.DMA((2,)), pltpu.SemaphoreType.DMA, pltpu.SemaphoreType.DMA((2,)),
                            pltpu.SemaphoreType.DMA, pltpu.SemaphoreType.DMA, pltpu.SemaphoreType.DMA((n_groups,))],
            compiler_params=pltpu.CompilerParams(collective_id=0, has_side_effects=True, vmem_limit_bytes=67043328),
            name="fused",
        )(flat, theta_k, theta_v, theta_q, w_out, w_init, eta)
        rest = jnp.dot(o, w_out[256 * N_FIRST:], preferred_element_type=f32)
        result = (rest + first_sum.reshape(n_rows, width_d)).astype(bf16)
        return result.reshape(n_batch, tok_dev, width_d)

    tok_spec = P("data", "seq", None)
    return jax.shard_map(per_device, mesh=mesh, in_specs=(tok_spec, P(), P(), P(), P(), P(), P()), out_specs=tok_spec, check_vma=False)
```

```python
import functools

import jax
import jax.numpy as jnp
from jax import lax
from jax.experimental import pallas as pl
from jax.experimental.pallas import tpu as pltpu
from jax.sharding import PartitionSpec as P

MINI_BATCH = 16
HEADS_PER_GROUP = 4
SCHEDULE = ((0, 6, (0, 0, 0, 0)), (1, 5, (0, 0, 0, 0)), (2, 4, (0, 0, 0, 0)), (2, 4, (0, 0, 0, 0)),
            (5, 2, (0, 0, 0, 0)), (5, 0, (4, 8, 8, 9)), (7, 0, (8, 8, 11, 11)), (7, 0, (10, 11, 11, 11)))
N_FIRST = 8
REST_COLUMNS = 512
bf16, f32 = jnp.bfloat16, jnp.float32


def split3(x):
    a = x.astype(bf16)
    rest = x - a.astype(f32)
    b = rest.astype(bf16)
    return a, b, (rest - b.astype(f32)).astype(bf16)


def per_head_rows(x, low):
    rows = []
    for half in range(2):
        y = x[:, half * 128:(half + 1) * 128]
        turned = pltpu.roll(y, 64, 1)
        rows += [jnp.where(low, y, turned), jnp.where(low, turned, y)]
    return rows


def own_columns(z, low, first):
    t = MINI_BATCH
    return jnp.concatenate([
        jnp.where(low, z[first:first + t, :128], z[first + t:first + 2 * t, :128]),
        jnp.where(low, z[first + 2 * t:first + 3 * t, 128:], z[first + 3 * t:first + 4 * t, 128:])], axis=1)


def times_w(rows, w):
    m = jnp.concatenate(rows, axis=0)
    lhs = jnp.concatenate([m, m], axis=1)
    rhs = jnp.concatenate([*split3(w), jnp.zeros(w.shape, bf16)], axis=0)
    return jnp.dot(lhs, rhs, preferred_element_type=f32)


def k_transposed_times(k_rows, r, low):
    zero = jnp.zeros((MINI_BATCH, 128), bf16)
    rows = []
    for part in split3(r):
        a, b = part[:, :128], part[:, 128:]
        rows += [jnp.concatenate([jnp.where(low, a, zero), zero], axis=1), jnp.concatenate([jnp.where(low, zero, a), zero], axis=1),
                 jnp.concatenate([zero, jnp.where(low, b, zero)], axis=1), jnp.concatenate([zero, jnp.where(low, zero, b)], axis=1)]
    rhs = jnp.concatenate([*rows, jnp.zeros((4 * MINI_BATCH, 256), bf16)], axis=0)
    k_mat = jnp.concatenate(k_rows, axis=0)
    turned = jnp.concatenate([k_mat, k_mat], axis=0).T[:64]
    lhs = jnp.concatenate([turned, turned], axis=1)
    return jnp.dot(lhs, rhs, preferred_element_type=f32)


def fused_kernel(n_seq, n_batch, tok_dev, n_groups, x_hbm, theta_k_hbm, theta_v_hbm, theta_q_hbm, w_out_hbm, w_init_hbm, eta_ref, o_hbm, sum_hbm,
                 x_buf, kvq_buf, theta_buf, tile_buf, o_buf, z_buf, w_buf, w_now, w_send, init_buf, x_sem, theta_sem, out_sem, sum_sem, init_sem, send_sem, recv_sem):
    me = lax.axis_index("seq")
    lag, n_late = jnp.int32(0), jnp.int32(0)
    for place, (ahead, late, _) in enumerate(SCHEDULE):
        lag = jnp.where(me == place, ahead, lag)
        n_late = jnp.where(me == place, late, n_late)

    def outs_before(g):
        n = jnp.int32(0)
        for place, (_, _, counts) in enumerate(SCHEDULE):
            for i, count in enumerate(counts):
                n = jnp.where((me == place) & (g >= N_FIRST + i), count, n)
        return n

    n_tiles = 3 * n_groups
    n_out_tiles = sum_hbm.shape[-1] // 256
    first_depth = N_FIRST * 256
    n_rows = n_batch * tok_dev
    n_steps = tok_dev // MINI_BATCH
    chunk = n_rows // n_steps
    depth = x_buf.shape[1]
    thetas = (theta_k_hbm, theta_v_hbm, theta_q_hbm)
    barrier = pltpu.get_barrier_semaphore()

    def columns(g):
        return pl.ds(pl.multiple_of(g * 256, 256), 256)

    def tile_at(c):
        early, body = 2 * n_late, c - 2 * n_late
        kind = jnp.where(c < early, lax.rem(c, 2), jnp.where(c < n_tiles - n_late, lax.rem(body, 3), 2))
        g = jnp.where(c < early, c // 2, jnp.where(c < n_tiles - n_late, n_late + body // 3, c - (n_tiles - n_late)))
        return kind, g

    def start_theta(c):
        kind, g = tile_at(c)
        for i in range(3):
            @pl.when((kind == i) & (c < n_tiles))
            def _():
                pltpu.make_async_copy(thetas[i].at[:, columns(g)], theta_buf.at[lax.rem(c, 2)], theta_sem.at[lax.rem(c, 2)]).start()

        @pl.when((c >= n_tiles) & (c < n_tiles + n_out_tiles))
        def _():
            w_out_copy(c - n_tiles, lax.rem(c, 2)).start()

    def w_out_copy(n, slot):
        return pltpu.make_async_copy(w_out_hbm.at[pl.ds(0, first_depth), columns(n)], theta_buf.at[slot, pl.ds(0, first_depth)], theta_sem.at[slot])

    def wait_theta(c):
        slot = lax.rem(c, 2)
        pltpu.make_async_copy(theta_k_hbm.at[:, pl.ds(0, 256)], theta_buf.at[slot], theta_sem.at[slot]).wait()

    def result(g):
        return pltpu.make_async_copy(o_buf, o_hbm.at[:, columns(g - N_FIRST)], out_sem)

    def sum_copy(n):
        part = lax.rem(n, 2)
        return pltpu.make_async_copy(w_buf.at[pl.ds(part * sum_slots, sum_slots)], sum_hbm.at[:, :, :, columns(n)], sum_sem.at[part])

    def hand_on(g):
        return pltpu.make_async_remote_copy(w_send, w_buf.at[g], send_sem, recv_sem.at[g],
                                            device_id={"seq": lax.rem(me + 1, n_seq)}, device_id_type=pl.DeviceIdType.MESH)

    sum_slots = sum_hbm.shape[0]

    def first_w(g):
        return pltpu.make_async_copy(w_init_hbm.at[pl.ds(g * HEADS_PER_GROUP, HEADS_PER_GROUP)], init_buf, init_sem)

    def x_copy(i):
        rows = pl.ds(i * (n_rows // 2), n_rows // 2)
        return pltpu.make_async_copy(x_hbm.at[rows], x_buf.at[rows], x_sem.at[i])

    start_theta(jnp.int32(0))
    for i in range(2):
        x_copy(i).start()

    @pl.when(me == 0)
    def _():
        first_w(0).start()

    for peer in (lax.rem(me + 1, n_seq), lax.rem(me + n_seq - 1, n_seq)):
        pl.semaphore_signal(barrier, inc=1, device_id={"seq": peer}, device_id_type=pl.DeviceIdType.MESH)
    for i in range(2):
        x_copy(i).wait()

    low = lax.broadcasted_iota(jnp.int32, (MINI_BATCH, 128), 1) < 64

    def rows_of(b, j):
        start = b * tok_dev + j * MINI_BATCH
        return pl.ds(start if isinstance(start, int) else pl.multiple_of(start, MINI_BATCH), MINI_BATCH)

    def multiply(g, b, j, with_k, with_q):
        k_rows = rows = per_head_rows(kvq_buf[0, g, rows_of(b, j), :], low) if with_k else []
        if with_q:
            rows = rows + per_head_rows(kvq_buf[2, g, rows_of(b, j - 1), :], low)
        prod = times_w(rows, w_now[b] if with_k and with_q or not with_k else w_buf[g, b])
        if with_k:
            z_buf[b] = own_columns(prod, low, 0)
        if with_q:
            o_buf[rows_of(b, j - 1), :] = own_columns(prod, low, 4 * MINI_BATCH if with_k else 0).astype(bf16)
        return k_rows

    def whole_tile(c, group=None):
        kind, g = tile_at(c)
        slot = lax.rem(c, 2)
        wait_theta(c)
        start_theta(c + 1)
        for i in range(2):
            rows = pl.ds(i * (n_rows // 2), n_rows // 2)
            part = jnp.dot(x_buf[rows, :], theta_buf[slot], preferred_element_type=f32).astype(bf16)
            if group is not None and i == 0:
                last_results(group)
                before = tile_at(c - 1)
                kvq_buf[before[0], before[1]] = tile_buf[...]
            kvq_buf[kind, g, rows, :] = part

    def out_tile(n):
        c = n_tiles + n
        slot = lax.rem(c, 2)
        w_out_copy(n, slot).wait()
        start_theta(c + 1)

        @pl.when(n >= 2)
        def _():
            sum_copy(n - 2).wait()

        for i in range(2):
            rows = pl.ds(i * (n_rows // 2), n_rows // 2)
            lhs = jnp.concatenate([kvq_buf[2, g, rows, :] for g in range(N_FIRST)], axis=1)
            part = jnp.dot(lhs, theta_buf[slot, :first_depth, :], preferred_element_type=f32)
            w_buf[pl.ds(lax.rem(n, 2) * sum_slots + i * (sum_slots // 2), sum_slots // 2)] = part.reshape(sum_slots // 2, *w_buf.shape[1:])
        sum_copy(n).start()

    def inner(g, first_time, c):
        slot = lax.rem(jnp.where(c < n_tiles, c, c - 1), 2)

        @pl.when(c < n_tiles)
        def _():
            wait_theta(c)
            start_theta(c + 1)

        @pl.when((me == 0) & first_time)
        def _():
            first_w(g).wait()
            start = jnp.concatenate([init_buf[h] for h in range(HEADS_PER_GROUP)], axis=1)
            for b in range(n_batch):
                w_buf[g, b] = start

        @pl.when((me == 0) & first_time & (g + 1 < n_groups))
        def _():
            first_w(g + 1).start()

        @pl.when((me > 0) & first_time)
        def _():
            hand_on(g).wait_recv()

        @pl.when(jnp.where(first_time, g > N_FIRST, g == 0))
        def _():
            result(N_FIRST).wait()

        eta = eta_ref[g]

        half = n_batch // 2

        def update(b, j, k_rows=None, first=False):
            k_rows = k_rows or per_head_rows(kvq_buf[0, g, rows_of(b, j), :], low)
            r = (z_buf[b] - kvq_buf[1, g, rows_of(b, j), :].astype(f32)) * eta
            w_now[b] = (w_buf[g, b] if first else w_now[b]) - k_transposed_times(k_rows, r, low)

        def step(j, first=False, second=False):
            part = pl.ds(j * chunk if isinstance(j, int) else pl.multiple_of(j * chunk, chunk), chunk)
            tile_part = jnp.dot(x_buf[part, :], theta_buf[slot], preferred_element_type=f32)
            k_rows = {}
            for b in range(half):
                k_rows[b] = multiply(g, b, j, True, not first)
                if not first:
                    update(half + b, j - 1, first=second)
            for b in range(half):
                multiply(g, half + b, j, True, not first)
                update(b, j, k_rows[b], first)
            tile_buf[part, :] = tile_part.astype(bf16)

        step(0, first=True)
        step(1, second=True)

        for j in range(2, n_steps):
            step(j)
        for b in range(half):
            update(half + b, n_steps - 1)

        @pl.when((me < n_seq - 1) & first_time & (g > 0))
        def _():
            hand_on(0).wait_send()

        @pl.when((me < n_seq - 1) & first_time)
        def _():
            w_send[...] = w_now[...]
            hand_on(g).start()

    def last_results(g):
        for b in range(n_batch):
            multiply(g, b, n_steps, False, True)
        kvq_buf[2, g] = o_buf[...]

    def send_result(g, first_time):
        @pl.when((g >= N_FIRST) & (jnp.logical_not(first_time) | (g >= n_late)))
        def _():
            result(g).start()

    def slot_body(s, _):
        @pl.when(s == 1)
        def _():
            pl.semaphore_wait(barrier, 2)

        first_time = s <= n_groups + lag
        g = jnp.where(first_time, s - 1 - lag, s - (n_groups + 1 + lag))
        fresh = s < n_groups
        c = jnp.where(fresh, 2 * s + jnp.maximum(s - n_late, 0), jnp.minimum(n_tiles - n_late + s - n_groups, n_tiles))
        n_out = jnp.where(first_time, outs_before(g), 0)

        def outs(n, _):
            out_tile(n)
            return 0

        lax.fori_loop(jnp.where(first_time, outs_before(g - 1), 0), n_out, outs, 0)

        @pl.when(g >= 0)
        def _():
            inner(g, first_time, c + n_out)

        @pl.when((g >= 0) & fresh)
        def _():
            whole_tile(c + 1, g)
            send_result(g, first_time)

        @pl.when((g >= 0) & jnp.logical_not(fresh))
        def _():
            last_results(g)
            send_result(g, first_time)

            @pl.when(c < n_tiles)
            def _():
                kind, of = tile_at(c)
                kvq_buf[kind, of] = tile_buf[...]

        def rest(i, _):
            whole_tile(c + i)
            return 0

        @pl.when(fresh)
        def _():
            lax.fori_loop(jnp.where(g >= 0, 2, 0), jnp.where(s < n_late, 2, 3), rest, 0)
        return 0

    lax.fori_loop(0, n_groups + 1 + lag + n_late, slot_body, 0)

    def outs(n, _):
        out_tile(n)
        return 0

    lax.fori_loop(outs_before(n_groups), n_out_tiles, outs, 0)
    for n in range(2):
        sum_copy(n_out_tiles - 2 + n).wait()

    @pl.when(n_late == 0)
    def _():
        result(N_FIRST).wait()

    @pl.when(me < n_seq - 1)
    def _():
        hand_on(0).wait_send()


def rest_kernel(o_ref, w_ref, sum_ref, out_ref):
    n_rows = o_ref.shape[0]
    slots = sum_ref.shape[0] // 2
    for i in range(2):
        rows = pl.ds(i * (n_rows // 2), n_rows // 2)
        first = sum_ref[pl.ds(i * slots, slots)].reshape(n_rows // 2, out_ref.shape[1])
        out_ref[rows, :] = (jnp.dot(o_ref[rows, :], w_ref[...], preferred_element_type=f32) + first).astype(bf16)


def solution(mesh):
    n_seq = mesh.shape["seq"]

    def per_device(tokens, theta_q, theta_k, theta_v, w_out, w_init, inner_lr):
        n_batch, tok_dev, width_d = tokens.shape
        n_heads, head_dim, _ = w_init.shape
        n_groups = n_heads // HEADS_PER_GROUP
        n_rows, width = n_batch * tok_dev, n_heads * head_dim
        flat = tokens.reshape(n_rows, width_d)
        eta = jnp.repeat((2.0 / MINI_BATCH) * inner_lr, head_dim).reshape(n_groups, 1, 4 * head_dim)
        hbm, vmem = pl.BlockSpec(memory_space=pl.ANY), pl.BlockSpec(memory_space=pltpu.VMEM)
        sum_slots = n_rows // (n_batch * head_dim)
        o, first_sum = pl.pallas_call(
            functools.partial(fused_kernel, n_seq, n_batch, tok_dev, n_groups),
            out_shape=(jax.ShapeDtypeStruct((n_rows, width - 256 * N_FIRST), bf16), jax.ShapeDtypeStruct((sum_slots, n_batch, head_dim, width_d), f32)),
            in_specs=[hbm] * 6 + [vmem], out_specs=(hbm, hbm),
            scratch_shapes=[pltpu.VMEM((n_rows, width_d), bf16), pltpu.VMEM((3, n_groups, n_rows, 256), bf16),
                            pltpu.VMEM((2, width_d, 256), bf16), pltpu.VMEM((n_rows, 256), bf16), pltpu.VMEM((n_rows, 256), bf16), pltpu.VMEM((n_batch, MINI_BATCH, 256), f32),
                            pltpu.VMEM((n_groups, n_batch, head_dim, 4 * head_dim), f32),
                            pltpu.VMEM((n_batch, head_dim, 4 * head_dim), f32), pltpu.VMEM((n_batch, head_dim, 4 * head_dim), f32),
                            pltpu.VMEM((HEADS_PER_GROUP, head_dim, head_dim), f32),
                            pltpu.SemaphoreType.DMA((2,)), pltpu.SemaphoreType.DMA((2,)), pltpu.SemaphoreType.DMA, pltpu.SemaphoreType.DMA((2,)),
                            pltpu.SemaphoreType.DMA, pltpu.SemaphoreType.DMA, pltpu.SemaphoreType.DMA((n_groups,))],
            compiler_params=pltpu.CompilerParams(collective_id=0, has_side_effects=True, vmem_limit_bytes=67043328),
            name="fused",
        )(flat, theta_k, theta_v, theta_q, w_out, w_init, eta)
        depth = width - 256 * N_FIRST
        result = pl.pallas_call(
            rest_kernel,
            out_shape=jax.ShapeDtypeStruct((n_rows, width_d), bf16),
            grid=(width_d // REST_COLUMNS,),
            in_specs=[pl.BlockSpec((n_rows, depth), lambda n: (0, 0), pipeline_mode=pl.Buffered(1)),
                      pl.BlockSpec((depth, REST_COLUMNS), lambda n: (256 * N_FIRST // depth, n)),
                      pl.BlockSpec((sum_slots, n_batch, head_dim, REST_COLUMNS), lambda n: (0, 0, 0, n))],
            out_specs=pl.BlockSpec((n_rows, REST_COLUMNS), lambda n: (0, n)),
            compiler_params=pltpu.CompilerParams(vmem_limit_bytes=48 * 1024 * 1024),
            name="rest",
        )(o, w_out, first_sum)
        return result.reshape(n_batch, tok_dev, width_d)

    tok_spec = P("data", "seq", None)
    return jax.shard_map(per_device, mesh=mesh, in_specs=(tok_spec, P(), P(), P(), P(), P(), P()), out_specs=tok_spec, check_vma=False)
```

```python
import functools

import jax
import jax.numpy as jnp
from jax import lax
from jax.experimental import pallas as pl
from jax.experimental.pallas import tpu as pltpu
from jax.sharding import PartitionSpec as P

MINI_BATCH = 16
HEADS_PER_GROUP = 4
SCHEDULE = ((0, 6, (0, 0, 0, 0)), (1, 5, (0, 0, 0, 0)), (2, 4, (0, 0, 0, 0)), (2, 4, (0, 0, 0, 0)),
            (5, 2, (0, 0, 0, 0)), (5, 0, (4, 8, 8, 9)), (7, 0, (8, 8, 11, 11)), (7, 0, (10, 11, 11, 11)))
N_FIRST = 8
REST_COLUMNS = 512
bf16, f32 = jnp.bfloat16, jnp.float32


def split3(x):
    a = x.astype(bf16)
    rest = x - a.astype(f32)
    b = rest.astype(bf16)
    return a, b, (rest - b.astype(f32)).astype(bf16)


def per_head_rows(x, low):
    rows = []
    for half in range(2):
        y = x[:, half * 128:(half + 1) * 128]
        turned = pltpu.roll(y, 64, 1)
        rows += [jnp.where(low, y, turned), jnp.where(low, turned, y)]
    return rows


def own_columns(z, low, first):
    t = MINI_BATCH
    return jnp.concatenate([
        jnp.where(low, z[first:first + t, :128], z[first + t:first + 2 * t, :128]),
        jnp.where(low, z[first + 2 * t:first + 3 * t, 128:], z[first + 3 * t:first + 4 * t, 128:])], axis=1)


def times_w(rows, w):
    m = jnp.concatenate(rows, axis=0)
    lhs = jnp.concatenate([m, m], axis=1)
    rhs = jnp.concatenate([*split3(w), jnp.zeros(w.shape, bf16)], axis=0)
    return jnp.dot(lhs, rhs, preferred_element_type=f32)


def k_transposed_times(k_rows, r, low):
    zero = jnp.zeros((MINI_BATCH, 128), bf16)
    rows = []
    for part in split3(r):
        a, b = part[:, :128], part[:, 128:]
        rows += [jnp.concatenate([jnp.where(low, a, zero), zero], axis=1), jnp.concatenate([jnp.where(low, zero, a), zero], axis=1),
                 jnp.concatenate([zero, jnp.where(low, b, zero)], axis=1), jnp.concatenate([zero, jnp.where(low, zero, b)], axis=1)]
    rhs = jnp.concatenate([*rows, jnp.zeros((4 * MINI_BATCH, 256), bf16)], axis=0)
    k_mat = jnp.concatenate(k_rows, axis=0)
    turned = jnp.concatenate([k_mat, k_mat], axis=0).T[:64]
    lhs = jnp.concatenate([turned, turned], axis=1)
    return jnp.dot(lhs, rhs, preferred_element_type=f32)


def fused_kernel(n_seq, n_batch, tok_dev, n_groups, x_hbm, theta_k_hbm, theta_v_hbm, theta_q_hbm, w_out_hbm, w_init_hbm, lr_ref, o_hbm, sum_hbm,
                 x_buf, kvq_buf, theta_buf, tile_buf, o_buf, z_buf, w_buf, w_now, w_send, init_buf, x_sem, theta_sem, out_sem, sum_sem, init_sem, send_sem, recv_sem):
    me = lax.axis_index("seq")
    lag, n_late = jnp.int32(0), jnp.int32(0)
    for place, (ahead, late, _) in enumerate(SCHEDULE):
        lag = jnp.where(me == place, ahead, lag)
        n_late = jnp.where(me == place, late, n_late)

    def outs_before(g):
        n = jnp.int32(0)
        for place, (_, _, counts) in enumerate(SCHEDULE):
            for i, count in enumerate(counts):
                n = jnp.where((me == place) & (g >= N_FIRST + i), count, n)
        return n

    n_tiles = 3 * n_groups
    n_out_tiles = sum_hbm.shape[-1] // 256
    first_depth = N_FIRST * 256
    n_rows = n_batch * tok_dev
    n_steps = tok_dev // MINI_BATCH
    chunk = n_rows // n_steps
    depth = x_buf.shape[1]
    thetas = (theta_k_hbm, theta_v_hbm, theta_q_hbm)
    barrier = pltpu.get_barrier_semaphore()

    def columns(g):
        return pl.ds(pl.multiple_of(g * 256, 256), 256)

    def tile_at(c):
        early, body = 2 * n_late, c - 2 * n_late
        kind = jnp.where(c < early, lax.rem(c, 2), jnp.where(c < n_tiles - n_late, lax.rem(body, 3), 2))
        g = jnp.where(c < early, c // 2, jnp.where(c < n_tiles - n_late, n_late + body // 3, c - (n_tiles - n_late)))
        return kind, g

    def start_theta(c):
        kind, g = tile_at(c)
        for i in range(3):
            @pl.when((kind == i) & (c < n_tiles))
            def _():
                pltpu.make_async_copy(thetas[i].at[:, columns(g)], theta_buf.at[lax.rem(c, 2)], theta_sem.at[lax.rem(c, 2)]).start()

        @pl.when((c >= n_tiles) & (c < n_tiles + n_out_tiles))
        def _():
            w_out_copy(c - n_tiles, lax.rem(c, 2)).start()

    def w_out_copy(n, slot):
        return pltpu.make_async_copy(w_out_hbm.at[pl.ds(0, first_depth), columns(n)], theta_buf.at[slot, pl.ds(0, first_depth)], theta_sem.at[slot])

    def wait_theta(c):
        slot = lax.rem(c, 2)
        pltpu.make_async_copy(theta_k_hbm.at[:, pl.ds(0, 256)], theta_buf.at[slot], theta_sem.at[slot]).wait()

    def result(g):
        return pltpu.make_async_copy(o_buf, o_hbm.at[:, columns(g - N_FIRST)], out_sem)

    def sum_copy(n):
        part = lax.rem(n, 2)
        return pltpu.make_async_copy(w_buf.at[pl.ds(part * sum_slots, sum_slots)], sum_hbm.at[:, :, :, columns(n)], sum_sem.at[part])

    def hand_on(g):
        return pltpu.make_async_remote_copy(w_send, w_buf.at[g], send_sem, recv_sem.at[g],
                                            device_id={"seq": lax.rem(me + 1, n_seq)}, device_id_type=pl.DeviceIdType.MESH)

    sum_slots = sum_hbm.shape[0]

    def first_w(g):
        return pltpu.make_async_copy(w_init_hbm.at[pl.ds(g * HEADS_PER_GROUP, HEADS_PER_GROUP)], init_buf, init_sem)

    def x_copy(i):
        rows = pl.ds(i * (n_rows // 2), n_rows // 2)
        return pltpu.make_async_copy(x_hbm.at[rows], x_buf.at[rows], x_sem.at[i])

    start_theta(jnp.int32(0))
    for i in range(2):
        x_copy(i).start()

    @pl.when(me == 0)
    def _():
        first_w(0).start()

    for peer in (lax.rem(me + 1, n_seq), lax.rem(me + n_seq - 1, n_seq)):
        pl.semaphore_signal(barrier, inc=1, device_id={"seq": peer}, device_id_type=pl.DeviceIdType.MESH)
    for i in range(2):
        x_copy(i).wait()

    low = lax.broadcasted_iota(jnp.int32, (MINI_BATCH, 128), 1) < 64
    head = lax.broadcasted_iota(jnp.int32, (1, 256), 1) // 64

    def rows_of(b, j):
        start = b * tok_dev + j * MINI_BATCH
        return pl.ds(start if isinstance(start, int) else pl.multiple_of(start, MINI_BATCH), MINI_BATCH)

    def multiply(g, b, j, with_k, with_q):
        k_rows = rows = per_head_rows(kvq_buf[0, g, rows_of(b, j), :], low) if with_k else []
        if with_q:
            rows = rows + per_head_rows(kvq_buf[2, g, rows_of(b, j - 1), :], low)
        prod = times_w(rows, w_now[b] if with_k and with_q or not with_k else w_buf[g, b])
        if with_k:
            z_buf[b] = own_columns(prod, low, 0)
        if with_q:
            o_buf[rows_of(b, j - 1), :] = own_columns(prod, low, 4 * MINI_BATCH if with_k else 0).astype(bf16)
        return k_rows

    def whole_tile(c, group=None):
        kind, g = tile_at(c)
        slot = lax.rem(c, 2)
        wait_theta(c)
        start_theta(c + 1)
        for i in range(2):
            rows = pl.ds(i * (n_rows // 2), n_rows // 2)
            part = jnp.dot(x_buf[rows, :], theta_buf[slot], preferred_element_type=f32).astype(bf16)
            if group is not None and i == 0:
                last_results(group)
                before = tile_at(c - 1)
                kvq_buf[before[0], before[1]] = tile_buf[...]
            kvq_buf[kind, g, rows, :] = part

    def out_tile(n):
        c = n_tiles + n
        slot = lax.rem(c, 2)
        w_out_copy(n, slot).wait()
        start_theta(c + 1)

        @pl.when(n >= 2)
        def _():
            sum_copy(n - 2).wait()

        for i in range(2):
            rows = pl.ds(i * (n_rows // 2), n_rows // 2)
            lhs = jnp.concatenate([kvq_buf[2, g, rows, :] for g in range(N_FIRST)], axis=1)
            part = jnp.dot(lhs, theta_buf[slot, :first_depth, :], preferred_element_type=f32)
            w_buf[pl.ds(lax.rem(n, 2) * sum_slots + i * (sum_slots // 2), sum_slots // 2)] = part.reshape(sum_slots // 2, *w_buf.shape[1:])
        sum_copy(n).start()

    def inner(g, first_time, c):
        slot = lax.rem(jnp.where(c < n_tiles, c, c - 1), 2)

        @pl.when(c < n_tiles)
        def _():
            wait_theta(c)
            start_theta(c + 1)

        @pl.when((me == 0) & first_time)
        def _():
            first_w(g).wait()
            start = jnp.concatenate([init_buf[h] for h in range(HEADS_PER_GROUP)], axis=1)
            for b in range(n_batch):
                w_buf[g, b] = start

        @pl.when((me == 0) & first_time & (g + 1 < n_groups))
        def _():
            first_w(g + 1).start()

        @pl.when((me > 0) & first_time)
        def _():
            hand_on(g).wait_recv()

        @pl.when(jnp.where(first_time, g > N_FIRST, g == 0))
        def _():
            result(N_FIRST).wait()

        eta = jnp.zeros((1, 256), f32)
        for h in range(HEADS_PER_GROUP):
            eta = jnp.where(head == h, (2.0 / MINI_BATCH) * lr_ref[g * HEADS_PER_GROUP + h], eta)

        half = n_batch // 2

        def update(b, j, k_rows=None, first=False):
            k_rows = k_rows or per_head_rows(kvq_buf[0, g, rows_of(b, j), :], low)
            r = (z_buf[b] - kvq_buf[1, g, rows_of(b, j), :].astype(f32)) * eta
            w_now[b] = (w_buf[g, b] if first else w_now[b]) - k_transposed_times(k_rows, r, low)

        def step(j, first=False, second=False):
            part = pl.ds(j * chunk if isinstance(j, int) else pl.multiple_of(j * chunk, chunk), chunk)
            tile_part = jnp.dot(x_buf[part, :], theta_buf[slot], preferred_element_type=f32)
            k_rows = {}
            for b in range(half):
                k_rows[b] = multiply(g, b, j, True, not first)
                if not first:
                    update(half + b, j - 1, first=second)
            for b in range(half):
                multiply(g, half + b, j, True, not first)
                update(b, j, k_rows[b], first)
            tile_buf[part, :] = tile_part.astype(bf16)

        step(0, first=True)
        step(1, second=True)

        for j in range(2, n_steps):
            step(j)
        for b in range(half):
            update(half + b, n_steps - 1)

        @pl.when((me < n_seq - 1) & first_time & (g > 0))
        def _():
            hand_on(0).wait_send()

        @pl.when((me < n_seq - 1) & first_time)
        def _():
            w_send[...] = w_now[...]
            hand_on(g).start()

    def last_results(g):
        for b in range(n_batch):
            multiply(g, b, n_steps, False, True)
        kvq_buf[2, g] = o_buf[...]

    def send_result(g, first_time):
        @pl.when((g >= N_FIRST) & (jnp.logical_not(first_time) | (g >= n_late)))
        def _():
            result(g).start()

    def slot_body(s, _):
        @pl.when(s == 1)
        def _():
            pl.semaphore_wait(barrier, 2)

        first_time = s <= n_groups + lag
        g = jnp.where(first_time, s - 1 - lag, s - (n_groups + 1 + lag))
        fresh = s < n_groups
        c = jnp.where(fresh, 2 * s + jnp.maximum(s - n_late, 0), jnp.minimum(n_tiles - n_late + s - n_groups, n_tiles))
        n_out = jnp.where(first_time, outs_before(g), 0)

        def outs(n, _):
            out_tile(n)
            return 0

        lax.fori_loop(jnp.where(first_time, outs_before(g - 1), 0), n_out, outs, 0)

        @pl.when(g >= 0)
        def _():
            inner(g, first_time, c + n_out)

        @pl.when((g >= 0) & fresh)
        def _():
            whole_tile(c + 1, g)
            send_result(g, first_time)

        @pl.when((g >= 0) & jnp.logical_not(fresh))
        def _():
            last_results(g)
            send_result(g, first_time)

            @pl.when(c < n_tiles)
            def _():
                kind, of = tile_at(c)
                kvq_buf[kind, of] = tile_buf[...]

        def rest(i, _):
            whole_tile(c + i)
            return 0

        @pl.when(fresh)
        def _():
            lax.fori_loop(jnp.where(g >= 0, 2, 0), jnp.where(s < n_late, 2, 3), rest, 0)
        return 0

    lax.fori_loop(0, n_groups + 1 + lag + n_late, slot_body, 0)

    def outs(n, _):
        out_tile(n)
        return 0

    lax.fori_loop(outs_before(n_groups), n_out_tiles, outs, 0)
    for n in range(2):
        sum_copy(n_out_tiles - 2 + n).wait()

    @pl.when(n_late == 0)
    def _():
        result(N_FIRST).wait()

    @pl.when(me < n_seq - 1)
    def _():
        hand_on(0).wait_send()


def rest_kernel(o_hbm, w_hbm, sum_hbm, out_hbm, o_buf, w_buf, sum_buf, out_buf, o_sem, w_sem, sum_sem, out_sem):
    n_rows, depth = o_buf.shape
    half, slots = n_rows // 2, sum_buf.shape[1] // 2
    n_parts = out_hbm.shape[1] // REST_COLUMNS

    def columns(n):
        return pl.ds(pl.multiple_of(n * REST_COLUMNS, REST_COLUMNS), REST_COLUMNS)

    def o_copy(i):
        rows = pl.ds(i * half, half)
        return pltpu.make_async_copy(o_hbm.at[rows], o_buf.at[rows], o_sem.at[i])

    def w_copy(n):
        slot = lax.rem(n, 2)
        return pltpu.make_async_copy(w_hbm.at[pl.ds(w_hbm.shape[0] - depth, depth), columns(n)], w_buf.at[slot], w_sem.at[slot])

    def sum_copy(n, i):
        slot, part = lax.rem(n, 2), pl.ds(i * slots, slots)
        return pltpu.make_async_copy(sum_hbm.at[part, :, :, columns(n)], sum_buf.at[slot, part], sum_sem.at[slot, i])

    def out_copy(n, i):
        slot, rows = lax.rem(n, 2), pl.ds(i * half, half)
        return pltpu.make_async_copy(out_buf.at[slot, rows], out_hbm.at[rows, columns(n)], out_sem.at[slot, i])

    first = jnp.int32(0)
    w_copy(first).start()
    for i in range(2):
        o_copy(i).start()
        sum_copy(first, i).start()
    w_copy(first + 1).start()

    def part(n, _):
        slot = lax.rem(n, 2)
        w_copy(n).wait()

        @pl.when(n + 1 < n_parts)
        def _():
            for i in range(2):
                sum_copy(n + 1, i).start()

        for i in range(2):
            @pl.when(n == 0)
            def _():
                o_copy(i).wait()

            @pl.when(n >= 2)
            def _():
                out_copy(n - 2, i).wait()

            sum_copy(n, i).wait()
            rows = pl.ds(i * half, half)
            so_far = sum_buf[slot, pl.ds(i * slots, slots)].reshape(half, REST_COLUMNS)
            out_buf[slot, rows, :] = (jnp.dot(o_buf[rows, :], w_buf[slot], preferred_element_type=f32) + so_far).astype(bf16)
            out_copy(n, i).start()

        @pl.when(n + 2 < n_parts)
        def _():
            w_copy(n + 2).start()
        return 0

    lax.fori_loop(0, n_parts, part, 0)
    for n in range(n_parts - 2, n_parts):
        for i in range(2):
            out_copy(n, i).wait()


def solution(mesh):
    n_seq = mesh.shape["seq"]

    def per_device(tokens, theta_q, theta_k, theta_v, w_out, w_init, inner_lr):
        n_batch, tok_dev, width_d = tokens.shape
        n_heads, head_dim, _ = w_init.shape
        n_groups = n_heads // HEADS_PER_GROUP
        n_rows, width = n_batch * tok_dev, n_heads * head_dim
        flat = tokens.reshape(n_rows, width_d)
        hbm, smem = pl.BlockSpec(memory_space=pl.ANY), pl.BlockSpec(memory_space=pltpu.SMEM)
        sum_slots = n_rows // (n_batch * head_dim)
        o, first_sum = pl.pallas_call(
            functools.partial(fused_kernel, n_seq, n_batch, tok_dev, n_groups),
            out_shape=(jax.ShapeDtypeStruct((n_rows, width - 256 * N_FIRST), bf16), jax.ShapeDtypeStruct((sum_slots, n_batch, head_dim, width_d), f32)),
            in_specs=[hbm] * 6 + [smem], out_specs=(hbm, hbm),
            scratch_shapes=[pltpu.VMEM((n_rows, width_d), bf16), pltpu.VMEM((3, n_groups, n_rows, 256), bf16),
                            pltpu.VMEM((2, width_d, 256), bf16), pltpu.VMEM((n_rows, 256), bf16), pltpu.VMEM((n_rows, 256), bf16), pltpu.VMEM((n_batch, MINI_BATCH, 256), f32),
                            pltpu.VMEM((n_groups, n_batch, head_dim, 4 * head_dim), f32),
                            pltpu.VMEM((n_batch, head_dim, 4 * head_dim), f32), pltpu.VMEM((n_batch, head_dim, 4 * head_dim), f32),
                            pltpu.VMEM((HEADS_PER_GROUP, head_dim, head_dim), f32),
                            pltpu.SemaphoreType.DMA((2,)), pltpu.SemaphoreType.DMA((2,)), pltpu.SemaphoreType.DMA, pltpu.SemaphoreType.DMA((2,)),
                            pltpu.SemaphoreType.DMA, pltpu.SemaphoreType.DMA, pltpu.SemaphoreType.DMA((n_groups,))],
            compiler_params=pltpu.CompilerParams(collective_id=0, has_side_effects=True, vmem_limit_bytes=67043328),
            name="fused",
        )(flat, theta_k, theta_v, theta_q, w_out, w_init, inner_lr)
        depth = width - 256 * N_FIRST
        result = pl.pallas_call(
            rest_kernel,
            out_shape=jax.ShapeDtypeStruct((n_rows, width_d), bf16),
            in_specs=[hbm] * 3, out_specs=hbm,
            scratch_shapes=[pltpu.VMEM((n_rows, depth), bf16), pltpu.VMEM((2, depth, REST_COLUMNS), bf16),
                            pltpu.VMEM((2, sum_slots, n_batch, head_dim, REST_COLUMNS), f32), pltpu.VMEM((2, n_rows, REST_COLUMNS), bf16),
                            pltpu.SemaphoreType.DMA((2,)), pltpu.SemaphoreType.DMA((2,)), pltpu.SemaphoreType.DMA((2, 2)), pltpu.SemaphoreType.DMA((2, 2))],
            compiler_params=pltpu.CompilerParams(vmem_limit_bytes=67043328),
            name="rest",
        )(o, w_out, first_sum)
        return result.reshape(n_batch, tok_dev, width_d)

    tok_spec = P("data", "seq", None)
    return jax.shard_map(per_device, mesh=mesh, in_specs=(tok_spec, P(), P(), P(), P(), P(), P()), out_specs=tok_spec, check_vma=False)
```

```python
import functools

import jax
import jax.numpy as jnp
from jax import lax
from jax.experimental import pallas as pl
from jax.experimental.pallas import tpu as pltpu
from jax.sharding import PartitionSpec as P

MINI_BATCH = 16
HEADS_PER_GROUP = 4
SCHEDULE = ((0, 5, (0, 0, 0, 0)), (1, 4, (0, 0, 0, 0)), (2, 1, (0, 0, 0, 0)), (2, 0, (0, 0, 0, 0)),
            (4, 0, (3, 6, 6, 6)), (5, 0, (3, 6, 6, 6)), (5, 0, (4, 6, 6, 6)), (8, 0, (6, 6, 6, 6)))
N_FIRST = 8
REST_COLUMNS = 512
bf16, f32 = jnp.bfloat16, jnp.float32


def split3(x):
    a = x.astype(bf16)
    rest = x - a.astype(f32)
    b = rest.astype(bf16)
    return a, b, (rest - b.astype(f32)).astype(bf16)


def per_head_rows(x):
    rows = []
    for half in range(2):
        y = x[:, :, half * 128:(half + 1) * 128]
        turned, low = pltpu.roll(y, 64, 2), low_lanes(y.shape)
        rows += [jnp.where(low, y, turned), jnp.where(low, turned, y)]
    return rows


def low_lanes(shape):
    return lax.broadcasted_iota(jnp.int32, shape, 2) < 64


def under(rows):
    n, t, width = rows[0].shape
    return jnp.concatenate([r.reshape(n, 1, t, width) for r in rows], axis=1).reshape(n, t * len(rows), width)


def own_columns(z, first):
    a, b, c, d = (z[:, first + i * MINI_BATCH:first + (i + 1) * MINI_BATCH, (i // 2) * 128:(i // 2 + 1) * 128] for i in range(4))
    low = low_lanes(a.shape)
    return jnp.concatenate([jnp.where(low, a, b), jnp.where(low, c, d)], axis=2)


def times_w(rows, w):
    m = under(rows)
    return jnp.concatenate([m, m], axis=2), jnp.concatenate([*split3(w), jnp.zeros(w.shape, bf16)], axis=1)


def k_transposed_times(k_rows, r):
    zero = jnp.zeros((*r.shape[:2], 128), bf16)
    low = low_lanes(zero.shape)
    rows = []
    for part in split3(r):
        a, b = part[:, :, :128], part[:, :, 128:]
        rows += [jnp.concatenate(pair, axis=2) for pair in (
            (jnp.where(low, a, zero), zero), (jnp.where(low, zero, a), zero), (zero, jnp.where(low, b, zero)), (zero, jnp.where(low, zero, b)))]
    rhs = jnp.concatenate([under(rows), jnp.zeros((r.shape[0], 4 * MINI_BATCH, 256), bf16)], axis=1)
    twice = under(k_rows + k_rows)
    turned = [twice[i].T[:64] for i in range(r.shape[0])]
    return [jnp.concatenate([t, t], axis=1) for t in turned], rhs


def fused_kernel(n_seq, n_batch, tok_dev, n_groups, x_hbm, theta_k_hbm, theta_v_hbm, theta_q_hbm, w_out_hbm, w_init_hbm, lr_ref, o_hbm, sum_hbm,
                 x_buf, kvq_buf, theta_buf, tile_buf, o_buf, w_buf, w_now, w_send, init_buf, x_sem, theta_sem, out_sem, sum_sem, init_sem, send_sem, recv_sem):
    me = lax.axis_index("seq")
    lag, n_late = jnp.int32(0), jnp.int32(0)
    for place, (ahead, late, _) in enumerate(SCHEDULE):
        lag = jnp.where(me == place, ahead, lag)
        n_late = jnp.where(me == place, late, n_late)

    outs_beside = (n_late == 0) & (lag > 2)

    def outs_before(g):
        n = jnp.int32(0)
        for place, (_, _, counts) in enumerate(SCHEDULE):
            for i, count in enumerate(counts):
                n = jnp.where((me == place) & (g >= N_FIRST + i), count, n)
        return n

    n_tiles = 3 * n_groups
    n_out_tiles = sum_hbm.shape[-1] // 256
    first_depth = N_FIRST * 256
    n_rows = n_batch * tok_dev
    n_steps = tok_dev // MINI_BATCH
    chunk = n_rows // n_steps
    depth = x_buf.shape[1]
    thetas = (theta_k_hbm, theta_v_hbm, theta_q_hbm)
    barrier = pltpu.get_barrier_semaphore()

    def columns(g):
        return pl.ds(pl.multiple_of(g * 256, 256), 256)

    def tile_at(c):
        early, body = 2 * n_late, c - 2 * n_late
        kind = jnp.where(c < early, lax.rem(c, 2), jnp.where(c < n_tiles - n_late, lax.rem(body, 3), 2))
        g = jnp.where(c < early, c // 2, jnp.where(c < n_tiles - n_late, n_late + body // 3, c - (n_tiles - n_late)))
        return kind, g

    def start_theta(c):
        kind, g = tile_at(c)
        for i in range(3):
            @pl.when((kind == i) & (c < n_tiles))
            def _():
                pltpu.make_async_copy(thetas[i].at[:, columns(g)], theta_buf.at[lax.rem(c, 2)], theta_sem.at[lax.rem(c, 2)]).start()

        @pl.when((c >= n_tiles) & (c < n_tiles + n_out_tiles))
        def _():
            w_out_copy(c - n_tiles, lax.rem(c, 2)).start()

    def w_out_copy(n, slot):
        return pltpu.make_async_copy(w_out_hbm.at[pl.ds(0, first_depth), columns(n)], theta_buf.at[slot, pl.ds(0, first_depth)], theta_sem.at[slot])

    def wait_theta(c):
        slot = lax.rem(c, 2)
        pltpu.make_async_copy(theta_k_hbm.at[:, pl.ds(0, 256)], theta_buf.at[slot], theta_sem.at[slot]).wait()

    def result(g):
        return pltpu.make_async_copy(o_buf, o_hbm.at[:, :, columns(g - N_FIRST)], out_sem)

    def sum_copy(n):
        part = lax.rem(n, 2)
        return pltpu.make_async_copy(w_buf.at[pl.ds(part * sum_slots, sum_slots)], sum_hbm.at[:, :, :, columns(n)], sum_sem.at[part])

    def hand_on(g):
        return pltpu.make_async_remote_copy(w_send, w_buf.at[g], send_sem, recv_sem.at[g],
                                            device_id={"seq": lax.rem(me + 1, n_seq)}, device_id_type=pl.DeviceIdType.MESH)

    sum_slots = sum_hbm.shape[0]

    def first_w(g):
        return pltpu.make_async_copy(w_init_hbm.at[pl.ds(g * HEADS_PER_GROUP, HEADS_PER_GROUP)], init_buf, init_sem)

    def x_copy(i):
        rows = pl.ds(i * (n_rows // 2), n_rows // 2)
        return pltpu.make_async_copy(x_hbm.at[rows], x_buf.at[rows], x_sem.at[i])

    start_theta(jnp.int32(0))
    for i in range(2):
        x_copy(i).start()

    @pl.when(me == 0)
    def _():
        first_w(0).start()

    for peer in (lax.rem(me + 1, n_seq), lax.rem(me + n_seq - 1, n_seq)):
        pl.semaphore_signal(barrier, inc=1, device_id={"seq": peer}, device_id_type=pl.DeviceIdType.MESH)

    head = lax.broadcasted_iota(jnp.int32, (1, 256), 1) // 64

    half = n_batch // 2

    def tokens(kind, g, units, j):
        return kvq_buf[kind, g, units, pl.ds(j * MINI_BATCH, MINI_BATCH), :]

    def chain_step(g, eta, j, now, before):
        k_rows = z = None
        if now is not None:
            k_rows = per_head_rows(tokens(0, g, now, j)) if j < n_steps else []
            rows = k_rows + (per_head_rows(tokens(2, g, now, j - 1)) if j > 0 else [])
            lhs, rhs = times_w(rows, w_now[now])
        if before is not None:
            units, step, keys, inputs = before
            r = (inputs - tokens(1, g, units, step).astype(f32)) * eta
            lhs_u, rhs_u = k_transposed_times(keys, r)
        prod, change = [], []
        for i in range(half):
            if now is not None:
                prod.append(jnp.dot(lhs[i], rhs[i], preferred_element_type=f32))
            if before is not None:
                change.append(jnp.dot(lhs_u[i], rhs_u[i], preferred_element_type=f32))
        if now is not None:
            prod = jnp.stack(prod)
            if j < n_steps:
                z = own_columns(prod, 0)
            if j > 0:
                o_buf[now, pl.ds((j - 1) * MINI_BATCH, MINI_BATCH), :] = own_columns(prod, 4 * MINI_BATCH if j < n_steps else 0).astype(bf16)
        if before is not None:
            w_now[units] = w_now[units] - jnp.stack(change)
        return k_rows, z

    def chain(g, eta, fill):
        one, two = pl.ds(0, half), pl.ds(half, half)
        open_two = None
        for j in range(n_steps):
            put = fill(j)
            open_one = (one, j, *chain_step(g, eta, j, one, open_two))
            open_two = (two, j, *chain_step(g, eta, j, two, open_one))
            put()
        chain_step(g, eta, n_steps, None, open_two)

    def whole_tile(c, group=None):
        kind, g = tile_at(c)
        slot = lax.rem(c, 2)
        wait_theta(c)
        start_theta(c + 1)
        for i in range(2):
            rows = pl.ds(i * (n_rows // 2), n_rows // 2)
            if isinstance(c, int):
                x_copy(i).wait()
            part = jnp.dot(x_buf[rows, :], theta_buf[slot], preferred_element_type=f32).astype(bf16)
            if group is not None and i == 0:
                last_results(group)
                before = tile_at(c - 1)
                kvq_buf[before[0], before[1]] = tile_buf[...].reshape(n_batch, tok_dev, 256)
            kvq_buf[kind, g, pl.ds(i * half, half)] = part.reshape(half, tok_dev, 256)

    def out_tile(n):
        c = n_tiles + n
        slot = lax.rem(c, 2)
        w_out_copy(n, slot).wait()
        start_theta(c + 1)

        @pl.when(n >= 2)
        def _():
            sum_copy(n - 2).wait()

        for i in range(2):
            rows = pl.ds(i * (n_rows // 2), n_rows // 2)
            lhs = jnp.concatenate([kvq_buf[2, g, pl.ds(i * half, half)].reshape(n_rows // 2, 256) for g in range(N_FIRST)], axis=1)
            part = jnp.dot(lhs, theta_buf[slot, :first_depth, :], preferred_element_type=f32)
            w_buf[pl.ds(lax.rem(n, 2) * sum_slots + i * (sum_slots // 2), sum_slots // 2)] = part.reshape(sum_slots // 2, *w_buf.shape[1:])
        sum_copy(n).start()

    def inner(g, first_time, c, n=None):
        slot = lax.rem(jnp.where(c < n_tiles, c, c - 1), 2) if n is None else lax.rem(c, 2)

        if n is None:
            @pl.when(c < n_tiles)
            def _():
                wait_theta(c)
                start_theta(c + 1)
        else:
            w_out_copy(n, slot).wait()
            start_theta(c + 1)

            @pl.when(n >= 2)
            def _():
                sum_copy(n - 2).wait()

        @pl.when((me == 0) & first_time)
        def _():
            first_w(g).wait()
            start = jnp.concatenate([init_buf[h] for h in range(HEADS_PER_GROUP)], axis=1)
            for b in range(n_batch):
                w_buf[g, b] = start

        @pl.when((me == 0) & first_time & (g + 1 < n_groups))
        def _():
            first_w(g + 1).start()

        @pl.when((me > 0) & first_time)
        def _():
            hand_on(g).wait_recv()

        @pl.when(jnp.where(first_time, g > N_FIRST, g == 0))
        def _():
            result(N_FIRST).wait()

        eta = jnp.zeros((1, 256), f32)
        for h in range(HEADS_PER_GROUP):
            eta = jnp.where(head == h, (2.0 / MINI_BATCH) * lr_ref[g * HEADS_PER_GROUP + h], eta)

        w_now[...] = w_buf[g]

        if n is None:
            def fill(j):
                part = pl.ds(j * chunk, chunk)
                tile_part = jnp.dot(x_buf[part, :], theta_buf[slot], preferred_element_type=f32)

                def put():
                    tile_buf[part, :] = tile_part.astype(bf16)
                return put
        else:
            def fill(j):
                b, first = j * chunk // tok_dev, j * chunk % tok_dev
                lhs = jnp.concatenate([kvq_buf[2, i, b, pl.ds(first, chunk), :] for i in range(N_FIRST)], axis=1)
                part = jnp.dot(lhs, theta_buf[slot, :first_depth, :], preferred_element_type=f32)
                rows = n_batch * w_buf.shape[2]
                at, within = j * chunk // rows, j * chunk % rows // w_buf.shape[2]

                def put():
                    w_buf[lax.rem(n, 2) * sum_slots + at, pl.ds(within, chunk // w_buf.shape[2])] = part.reshape(chunk // w_buf.shape[2], *w_buf.shape[2:])
                return put

        chain(g, eta, fill)

        if n is not None:
            sum_copy(n).start()

        @pl.when((me < n_seq - 1) & first_time & (g > 0))
        def _():
            hand_on(0).wait_send()

        @pl.when((me < n_seq - 1) & first_time)
        def _():
            w_send[...] = w_now[...]
            hand_on(g).start()

    def last_results(g):
        for units in (pl.ds(0, half), pl.ds(half, half)):
            chain_step(g, None, n_steps, units, None)
        kvq_buf[2, g] = o_buf[...]

    def send_result(g, first_time):
        @pl.when((g >= N_FIRST) & (jnp.logical_not(first_time) | (g >= n_late)))
        def _():
            result(g).start()

    def slot_body(s, _):
        @pl.when(s == 1)
        def _():
            pl.semaphore_wait(barrier, 2)

        first_time = s <= n_groups + lag
        g = jnp.where(first_time, s - 1 - lag, s - (n_groups + 1 + lag))
        fresh = s < n_groups
        c = jnp.where(fresh, 2 * s + jnp.maximum(s - n_late, 0), jnp.minimum(n_tiles - n_late + s - n_groups, n_tiles))
        beside_out = outs_beside & first_time & (g >= N_FIRST)
        n_out = jnp.where(beside_out, outs_before(g) + g - N_FIRST, 0)

        def outs(n, _):
            out_tile(n)
            return 0

        lax.fori_loop(jnp.where(beside_out, outs_before(g - 1) + g - N_FIRST, 0), n_out, outs, 0)

        @pl.when((g >= 0) & jnp.logical_not(beside_out))
        def _():
            inner(g, first_time, c)

        @pl.when(beside_out)
        def _():
            inner(g, first_time, n_tiles + n_out, n_out)

        @pl.when((g >= 0) & fresh)
        def _():
            whole_tile(c + 1, g)
            send_result(g, first_time)

        @pl.when((g >= 0) & jnp.logical_not(fresh))
        def _():
            last_results(g)
            send_result(g, first_time)

            @pl.when(c < n_tiles)
            def _():
                kind, of = tile_at(c)
                kvq_buf[kind, of] = tile_buf[...].reshape(n_batch, tok_dev, 256)

        def rest(i, _):
            whole_tile(c + i)
            return 0

        @pl.when(fresh)
        def _():
            lax.fori_loop(jnp.where(g >= 0, 2, jnp.where(s == 0, 1, 0)), jnp.where(s < n_late, 2, 3), rest, 0)
        return 0

    whole_tile(0)
    lax.fori_loop(0, n_groups + 1 + lag + n_late, slot_body, 0)

    def outs(n, _):
        out_tile(n)
        return 0

    lax.fori_loop(jnp.where(outs_beside, outs_before(n_groups) + n_groups - N_FIRST, 0), n_out_tiles, outs, 0)
    for n in range(2):
        sum_copy(n_out_tiles - 2 + n).wait()

    @pl.when(n_late == 0)
    def _():
        result(N_FIRST).wait()

    @pl.when(me < n_seq - 1)
    def _():
        hand_on(0).wait_send()


def rest_kernel(o_hbm, w_hbm, sum_hbm, out_hbm, o_buf, w_buf, sum_buf, out_buf, o_sem, w_sem, sum_sem, out_sem):
    n_rows, depth = o_buf.shape
    half, slots = n_rows // 2, sum_buf.shape[1] // 2
    n_parts = out_hbm.shape[1] // REST_COLUMNS

    def columns(n):
        return pl.ds(pl.multiple_of(n * REST_COLUMNS, REST_COLUMNS), REST_COLUMNS)

    def o_copy(i):
        rows = pl.ds(i * half, half)
        return pltpu.make_async_copy(o_hbm.at[rows], o_buf.at[rows], o_sem.at[i])

    def w_copy(n):
        slot = lax.rem(n, 2)
        return pltpu.make_async_copy(w_hbm.at[pl.ds(w_hbm.shape[0] - depth, depth), columns(n)], w_buf.at[slot], w_sem.at[slot])

    def sum_copy(n, i):
        slot, part = lax.rem(n, 2), pl.ds(i * slots, slots)
        return pltpu.make_async_copy(sum_hbm.at[part, :, :, columns(n)], sum_buf.at[slot, part], sum_sem.at[slot, i])

    def out_copy(n, i):
        slot, rows = lax.rem(n, 2), pl.ds(i * half, half)
        return pltpu.make_async_copy(out_buf.at[slot, rows], out_hbm.at[rows, columns(n)], out_sem.at[slot, i])

    first = jnp.int32(0)
    w_copy(first).start()
    for i in range(2):
        o_copy(i).start()
        sum_copy(first, i).start()
    w_copy(first + 1).start()

    def part(n, _):
        slot = lax.rem(n, 2)
        w_copy(n).wait()

        @pl.when(n + 1 < n_parts)
        def _():
            for i in range(2):
                sum_copy(n + 1, i).start()

        for i in range(2):
            @pl.when(n == 0)
            def _():
                o_copy(i).wait()

            @pl.when(n >= 2)
            def _():
                out_copy(n - 2, i).wait()

            sum_copy(n, i).wait()
            rows = pl.ds(i * half, half)
            so_far = sum_buf[slot, pl.ds(i * slots, slots)].reshape(half, REST_COLUMNS)
            out_buf[slot, rows, :] = (jnp.dot(o_buf[rows, :], w_buf[slot], preferred_element_type=f32) + so_far).astype(bf16)
            out_copy(n, i).start()

        @pl.when(n + 2 < n_parts)
        def _():
            w_copy(n + 2).start()
        return 0

    lax.fori_loop(0, n_parts, part, 0)
    for n in range(n_parts - 2, n_parts):
        for i in range(2):
            out_copy(n, i).wait()


def solution(mesh):
    n_seq = mesh.shape["seq"]

    def per_device(tokens, theta_q, theta_k, theta_v, w_out, w_init, inner_lr):
        n_batch, tok_dev, width_d = tokens.shape
        n_heads, head_dim, _ = w_init.shape
        n_groups = n_heads // HEADS_PER_GROUP
        n_rows, width = n_batch * tok_dev, n_heads * head_dim
        flat = tokens.reshape(n_rows, width_d)
        hbm, smem = pl.BlockSpec(memory_space=pl.ANY), pl.BlockSpec(memory_space=pltpu.SMEM)
        sum_slots = n_rows // (n_batch * head_dim)
        o, first_sum = pl.pallas_call(
            functools.partial(fused_kernel, n_seq, n_batch, tok_dev, n_groups),
            out_shape=(jax.ShapeDtypeStruct((n_batch, tok_dev, width - 256 * N_FIRST), bf16), jax.ShapeDtypeStruct((sum_slots, n_batch, head_dim, width_d), f32)),
            in_specs=[hbm] * 6 + [smem], out_specs=(hbm, hbm),
            scratch_shapes=[pltpu.VMEM((n_rows, width_d), bf16), pltpu.VMEM((3, n_groups, n_batch, tok_dev, 256), bf16),
                            pltpu.VMEM((2, width_d, 256), bf16), pltpu.VMEM((n_rows, 256), bf16), pltpu.VMEM((n_batch, tok_dev, 256), bf16),
                            pltpu.VMEM((n_groups, n_batch, head_dim, 4 * head_dim), f32),
                            pltpu.VMEM((n_batch, head_dim, 4 * head_dim), f32), pltpu.VMEM((n_batch, head_dim, 4 * head_dim), f32),
                            pltpu.VMEM((HEADS_PER_GROUP, head_dim, head_dim), f32),
                            pltpu.SemaphoreType.DMA((2,)), pltpu.SemaphoreType.DMA((2,)), pltpu.SemaphoreType.DMA, pltpu.SemaphoreType.DMA((2,)),
                            pltpu.SemaphoreType.DMA, pltpu.SemaphoreType.DMA, pltpu.SemaphoreType.DMA((n_groups,))],
            compiler_params=pltpu.CompilerParams(collective_id=0, has_side_effects=True, vmem_limit_bytes=67043328),
            name="fused",
        )(flat, theta_k, theta_v, theta_q, w_out, w_init, inner_lr)
        depth = width - 256 * N_FIRST
        result = pl.pallas_call(
            rest_kernel,
            out_shape=jax.ShapeDtypeStruct((n_rows, width_d), bf16),
            in_specs=[hbm] * 3, out_specs=hbm,
            scratch_shapes=[pltpu.VMEM((n_rows, depth), bf16), pltpu.VMEM((2, depth, REST_COLUMNS), bf16),
                            pltpu.VMEM((2, sum_slots, n_batch, head_dim, REST_COLUMNS), f32), pltpu.VMEM((2, n_rows, REST_COLUMNS), bf16),
                            pltpu.SemaphoreType.DMA((2,)), pltpu.SemaphoreType.DMA((2,)), pltpu.SemaphoreType.DMA((2, 2)), pltpu.SemaphoreType.DMA((2, 2))],
            compiler_params=pltpu.CompilerParams(vmem_limit_bytes=67043328),
            name="rest",
        )(o.reshape(n_rows, depth), w_out, first_sum)
        return result.reshape(n_batch, tok_dev, width_d)

    tok_spec = P("data", "seq", None)
    return jax.shard_map(per_device, mesh=mesh, in_specs=(tok_spec, P(), P(), P(), P(), P(), P()), out_specs=tok_spec, check_vma=False)
```

```python
import functools

import jax
import jax.numpy as jnp
from jax import lax
from jax.experimental import pallas as pl
from jax.experimental.pallas import tpu as pltpu
from jax.sharding import PartitionSpec as P

MINI_BATCH = 16
HEADS_PER_GROUP = 4
SCHEDULE = ((0, 6, (0, 0, 0, 0, 0)), (1, 5, (0, 0, 0, 0, 0)), (3, 3, (0, 0, 0, 0, 0)), (3, 1, (0, 0, 0, 0, 0)),
            (4, 0, (0, 3, 3, 3, 3)), (5, 0, (3, 6, 6, 6, 6)), (5, 0, (3, 6, 6, 6, 6)), (5, 0, (3, 6, 6, 7, 7)))
N_FIRST = 7
REST_COLUMNS = 512
bf16, f32 = jnp.bfloat16, jnp.float32


def split3(x):
    a = x.astype(bf16)
    rest = x - a.astype(f32)
    b = rest.astype(bf16)
    return a, b, (rest - b.astype(f32)).astype(bf16)


def per_head_rows(x):
    rows = []
    for half in range(2):
        y = x[:, :, half * 128:(half + 1) * 128]
        turned, low = pltpu.roll(y, 64, 2), low_lanes(y.shape)
        rows += [jnp.where(low, y, turned), jnp.where(low, turned, y)]
    return rows


def low_lanes(shape):
    return lax.broadcasted_iota(jnp.int32, shape, 2) < 64


def under(rows):
    n, t, width = rows[0].shape
    return jnp.concatenate([r.reshape(n, 1, t, width) for r in rows], axis=1).reshape(n, t * len(rows), width)


def own_columns(z, first):
    a, b, c, d = (z[:, first + i * MINI_BATCH:first + (i + 1) * MINI_BATCH, (i // 2) * 128:(i // 2 + 1) * 128] for i in range(4))
    low = low_lanes(a.shape)
    return jnp.concatenate([jnp.where(low, a, b), jnp.where(low, c, d)], axis=2)


def times_w(rows, w):
    m = under(rows)
    return jnp.concatenate([m, m], axis=2), jnp.concatenate([*split3(w), jnp.zeros(w.shape, bf16)], axis=1)


def k_transposed_times(k_rows, r):
    zero = jnp.zeros((*r.shape[:2], 128), bf16)
    low = low_lanes(zero.shape)
    rows = []
    for part in split3(r):
        a, b = part[:, :, :128], part[:, :, 128:]
        rows += [jnp.concatenate(pair, axis=2) for pair in (
            (jnp.where(low, a, zero), zero), (jnp.where(low, zero, a), zero), (zero, jnp.where(low, b, zero)), (zero, jnp.where(low, zero, b)))]
    rhs = jnp.concatenate([under(rows), jnp.zeros((r.shape[0], 4 * MINI_BATCH, 256), bf16)], axis=1)
    twice = under(k_rows + k_rows)
    turned = [twice[i].T[:64] for i in range(r.shape[0])]
    return [jnp.concatenate([t, t], axis=1) for t in turned], rhs


def fused_kernel(n_seq, n_batch, tok_dev, n_groups, x_hbm, theta_k_hbm, theta_v_hbm, theta_q_hbm, w_out_hbm, w_init_hbm, lr_ref, o_hbm, sum_hbm,
                 x_buf, kvq_buf, theta_buf, tile_buf, o_buf, w_buf, w_now, w_send, init_buf, x_sem, theta_sem, out_sem, sum_sem, init_sem, send_sem, recv_sem):
    me = lax.axis_index("seq")
    lag, n_late = jnp.int32(0), jnp.int32(0)
    for place, (ahead, late, _) in enumerate(SCHEDULE):
        lag = jnp.where(me == place, ahead, lag)
        n_late = jnp.where(me == place, late, n_late)

    outs_beside = (n_late == 0) & (lag + 1 + N_FIRST >= n_groups)

    def outs_before(g):
        n = jnp.int32(0)
        for place, (_, _, counts) in enumerate(SCHEDULE):
            for i, count in enumerate(counts):
                n = jnp.where((me == place) & (g >= N_FIRST + i), count, n)
        return n

    n_tiles = 3 * n_groups
    n_out_tiles = sum_hbm.shape[-1] // 256
    w_first = w_buf.shape[0] - n_groups
    first_depth = N_FIRST * 256
    n_rows = n_batch * tok_dev
    n_steps = tok_dev // MINI_BATCH
    chunk = n_rows // n_steps
    depth = x_buf.shape[1]
    thetas = (theta_k_hbm, theta_v_hbm, theta_q_hbm)
    barrier = pltpu.get_barrier_semaphore()

    def columns(g):
        return pl.ds(pl.multiple_of(g * 256, 256), 256)

    def tile_at(c):
        early, body = 2 * n_late, c - 2 * n_late
        kind = jnp.where(c < early, lax.rem(c, 2), jnp.where(c < n_tiles - n_late, lax.rem(body, 3), 2))
        g = jnp.where(c < early, c // 2, jnp.where(c < n_tiles - n_late, n_late + body // 3, c - (n_tiles - n_late)))
        return kind, g

    def start_theta(c):
        kind, g = tile_at(c)
        for i in range(3):
            @pl.when((kind == i) & (c < n_tiles))
            def _():
                pltpu.make_async_copy(thetas[i].at[:, columns(g)], theta_buf.at[lax.rem(c, 2)], theta_sem.at[lax.rem(c, 2)]).start()

        @pl.when((c >= n_tiles) & (c < n_tiles + n_out_tiles))
        def _():
            w_out_copy(c - n_tiles, lax.rem(c, 2)).start()

    def w_out_copy(n, slot):
        return pltpu.make_async_copy(w_out_hbm.at[pl.ds(0, first_depth), columns(n)], theta_buf.at[slot, pl.ds(0, first_depth)], theta_sem.at[slot])

    def wait_theta(c):
        slot = lax.rem(c, 2)
        pltpu.make_async_copy(theta_k_hbm.at[:, pl.ds(0, 256)], theta_buf.at[slot], theta_sem.at[slot]).wait()

    def result(g):
        return pltpu.make_async_copy(o_buf, o_hbm.at[:, :, columns(g - N_FIRST)], out_sem)

    def sum_copy(n):
        part = lax.rem(n, 2)
        return pltpu.make_async_copy(w_buf.at[pl.ds(part * sum_slots, sum_slots)], sum_hbm.at[:, :, :, columns(n)], sum_sem.at[part])

    def hand_on(g):
        return pltpu.make_async_remote_copy(w_send, w_buf.at[w_first + g], send_sem, recv_sem.at[g],
                                            device_id={"seq": lax.rem(me + 1, n_seq)}, device_id_type=pl.DeviceIdType.MESH)

    sum_slots = sum_hbm.shape[0]

    def first_w(g):
        return pltpu.make_async_copy(w_init_hbm.at[pl.ds(g * HEADS_PER_GROUP, HEADS_PER_GROUP)], init_buf, init_sem)

    def x_copy(i):
        rows = pl.ds(i * (n_rows // 2), n_rows // 2)
        return pltpu.make_async_copy(x_hbm.at[rows], x_buf.at[rows], x_sem.at[i])

    start_theta(jnp.int32(0))
    for i in range(2):
        x_copy(i).start()

    @pl.when(me == 0)
    def _():
        first_w(0).start()

    for peer in (lax.rem(me + 1, n_seq), lax.rem(me + n_seq - 1, n_seq)):
        pl.semaphore_signal(barrier, inc=1, device_id={"seq": peer}, device_id_type=pl.DeviceIdType.MESH)

    head = lax.broadcasted_iota(jnp.int32, (1, 256), 1) // 64

    half = n_batch // 2

    def tokens(kind, g, units, j):
        return kvq_buf[kind, g, units, pl.ds(j * MINI_BATCH, MINI_BATCH), :]

    def chain_step(g, eta, j, now, before):
        k_rows = z = None
        if now is not None:
            k_rows = per_head_rows(tokens(0, g, now, j)) if j < n_steps else []
            rows = k_rows + (per_head_rows(tokens(2, g, now, j - 1)) if j > 0 else [])
            lhs, rhs = times_w(rows, w_now[now])
        if before is not None:
            units, step, keys, inputs = before
            r = (inputs - tokens(1, g, units, step).astype(f32)) * eta
            lhs_u, rhs_u = k_transposed_times(keys, r)
        prod, change = [], []
        for i in range(half):
            if now is not None:
                prod.append(jnp.dot(lhs[i], rhs[i], preferred_element_type=f32))
            if before is not None:
                change.append(jnp.dot(lhs_u[i], rhs_u[i], preferred_element_type=f32))
        if now is not None:
            prod = jnp.stack(prod)
            if j < n_steps:
                z = own_columns(prod, 0)
            if j > 0:
                o_buf[now, pl.ds((j - 1) * MINI_BATCH, MINI_BATCH), :] = own_columns(prod, 4 * MINI_BATCH if j < n_steps else 0).astype(bf16)
        if before is not None:
            w_now[units] = w_now[units] - jnp.stack(change)
        return k_rows, z

    def chain(g, eta, fill):
        one, two = pl.ds(0, half), pl.ds(half, half)
        open_two = None
        for j in range(n_steps):
            put = fill(j)
            open_one = (one, j, *chain_step(g, eta, j, one, open_two))
            open_two = (two, j, *chain_step(g, eta, j, two, open_one))
            put()
        chain_step(g, eta, n_steps, None, open_two)

    def whole_tile(c, group=None):
        kind, g = tile_at(c)
        slot = lax.rem(c, 2)
        wait_theta(c)
        start_theta(c + 1)
        for i in range(2):
            rows = pl.ds(i * (n_rows // 2), n_rows // 2)
            if isinstance(c, int):
                x_copy(i).wait()
            part = jnp.dot(x_buf[rows, :], theta_buf[slot], preferred_element_type=f32).astype(bf16)
            if group is not None and i == 0:
                last_results(group)
                before = tile_at(c - 1)
                kvq_buf[before[0], before[1]] = tile_buf[...].reshape(n_batch, tok_dev, 256)
            kvq_buf[kind, g, pl.ds(i * half, half)] = part.reshape(half, tok_dev, 256)

    def out_tile(n):
        c = n_tiles + n
        slot = lax.rem(c, 2)
        w_out_copy(n, slot).wait()
        start_theta(c + 1)

        @pl.when(n >= 2)
        def _():
            sum_copy(n - 2).wait()

        for i in range(2):
            rows = pl.ds(i * (n_rows // 2), n_rows // 2)
            lhs = jnp.concatenate([kvq_buf[2, g, pl.ds(i * half, half)].reshape(n_rows // 2, 256) for g in range(N_FIRST)], axis=1)
            part = jnp.dot(lhs, theta_buf[slot, :first_depth, :], preferred_element_type=f32)
            w_buf[pl.ds(lax.rem(n, 2) * sum_slots + i * (sum_slots // 2), sum_slots // 2)] = part.reshape(sum_slots // 2, *w_buf.shape[1:])
        sum_copy(n).start()

    def inner(g, first_time, c, n=None):
        slot = lax.rem(jnp.where(c < n_tiles, c, c - 1), 2) if n is None else lax.rem(c, 2)

        if n is None:
            @pl.when(c < n_tiles)
            def _():
                wait_theta(c)
                start_theta(c + 1)
        else:
            w_out_copy(n, slot).wait()
            start_theta(c + 1)

            @pl.when(n >= 2)
            def _():
                sum_copy(n - 2).wait()

        @pl.when((me == 0) & first_time)
        def _():
            first_w(g).wait()
            start = jnp.concatenate([init_buf[h] for h in range(HEADS_PER_GROUP)], axis=1)
            for b in range(n_batch):
                w_buf[w_first + g, b] = start

        @pl.when((me == 0) & first_time & (g + 1 < n_groups))
        def _():
            first_w(g + 1).start()

        @pl.when((me > 0) & first_time)
        def _():
            hand_on(g).wait_recv()

        @pl.when(jnp.where(first_time, g > N_FIRST, g == 0))
        def _():
            result(N_FIRST).wait()

        eta = jnp.zeros((1, 256), f32)
        for h in range(HEADS_PER_GROUP):
            eta = jnp.where(head == h, (2.0 / MINI_BATCH) * lr_ref[g * HEADS_PER_GROUP + h], eta)

        w_now[...] = w_buf[w_first + g]

        if n is None:
            def fill(j):
                part = pl.ds(j * chunk, chunk)
                tile_part = jnp.dot(x_buf[part, :], theta_buf[slot], preferred_element_type=f32)

                def put():
                    tile_buf[part, :] = tile_part.astype(bf16)
                return put
        else:
            def fill(j):
                b, first = j * chunk // tok_dev, j * chunk % tok_dev
                lhs = jnp.concatenate([kvq_buf[2, i, b, pl.ds(first, chunk), :] for i in range(N_FIRST)], axis=1)
                part = jnp.dot(lhs, theta_buf[slot, :first_depth, :], preferred_element_type=f32)
                spare = pl.ds(j * chunk, chunk)
                even = jnp.dot(x_buf[spare, :depth - first_depth], theta_buf[slot, first_depth:, :], preferred_element_type=f32)
                rows = n_batch * w_buf.shape[2]
                at, within = j * chunk // rows, j * chunk % rows // w_buf.shape[2]

                def put():
                    w_buf[lax.rem(n, 2) * sum_slots + at, pl.ds(within, chunk // w_buf.shape[2])] = part.reshape(chunk // w_buf.shape[2], *w_buf.shape[2:])
                    tile_buf[spare, :] = even.astype(bf16)
                return put

        chain(g, eta, fill)

        if n is not None:
            sum_copy(n).start()

        @pl.when((me < n_seq - 1) & first_time & (g > 0))
        def _():
            hand_on(0).wait_send()

        @pl.when((me < n_seq - 1) & first_time)
        def _():
            w_send[...] = w_now[...]
            hand_on(g).start()

    def last_results(g):
        for units in (pl.ds(0, half), pl.ds(half, half)):
            chain_step(g, None, n_steps, units, None)
        kvq_buf[2, g] = o_buf[...]

    def send_result(g, first_time):
        @pl.when((g >= N_FIRST) & (jnp.logical_not(first_time) | (g >= n_late)))
        def _():
            result(g).start()

    def slot_body(s, _):
        @pl.when(s == 1)
        def _():
            pl.semaphore_wait(barrier, 2)

        first_time = s <= n_groups + lag
        g = jnp.where(first_time, s - 1 - lag, s - (n_groups + 1 + lag))
        fresh = s < n_groups
        c = jnp.where(fresh, 2 * s + jnp.maximum(s - n_late, 0), jnp.minimum(n_tiles - n_late + s - n_groups, n_tiles))
        beside_out = outs_beside & first_time & (g >= N_FIRST)
        n_out = jnp.where(beside_out, outs_before(g) + g - N_FIRST, 0)

        def outs(n, _):
            out_tile(n)
            return 0

        lax.fori_loop(jnp.where(beside_out, outs_before(g - 1) + g - N_FIRST, 0), n_out, outs, 0)

        @pl.when((g >= 0) & jnp.logical_not(beside_out))
        def _():
            inner(g, first_time, c)

        @pl.when(beside_out)
        def _():
            inner(g, first_time, n_tiles + n_out, n_out)

        @pl.when((g >= 0) & fresh)
        def _():
            whole_tile(c + 1, g)
            send_result(g, first_time)

        @pl.when((g >= 0) & jnp.logical_not(fresh))
        def _():
            last_results(g)
            send_result(g, first_time)

            @pl.when(c < n_tiles)
            def _():
                kind, of = tile_at(c)
                kvq_buf[kind, of] = tile_buf[...].reshape(n_batch, tok_dev, 256)

        def rest(i, _):
            whole_tile(c + i)
            return 0

        @pl.when(fresh)
        def _():
            lax.fori_loop(jnp.where(g >= 0, 2, jnp.where(s == 0, 1, 0)), jnp.where(s < n_late, 2, 3), rest, 0)
        return 0

    whole_tile(0)
    lax.fori_loop(0, n_groups + 1 + lag + n_late, slot_body, 0)

    def outs(n, _):
        out_tile(n)
        return 0

    lax.fori_loop(jnp.where(outs_beside, outs_before(n_groups) + n_groups - N_FIRST, 0), n_out_tiles, outs, 0)
    for n in range(2):
        sum_copy(n_out_tiles - 2 + n).wait()

    @pl.when(n_late == 0)
    def _():
        result(N_FIRST).wait()

    @pl.when(me < n_seq - 1)
    def _():
        hand_on(0).wait_send()


def rest_kernel(o_hbm, w_hbm, sum_hbm, out_hbm, o_buf, w_buf, sum_buf, out_buf, o_sem, w_sem, sum_sem, out_sem):
    n_rows, depth = o_buf.shape
    half, slots = n_rows // 2, sum_buf.shape[1] // 2
    n_parts = out_hbm.shape[1] // REST_COLUMNS

    def columns(n):
        return pl.ds(pl.multiple_of(n * REST_COLUMNS, REST_COLUMNS), REST_COLUMNS)

    def o_copy(i):
        rows = pl.ds(i * half, half)
        return pltpu.make_async_copy(o_hbm.at[rows], o_buf.at[rows], o_sem.at[i])

    def w_copy(n):
        slot = lax.rem(n, 2)
        return pltpu.make_async_copy(w_hbm.at[pl.ds(w_hbm.shape[0] - depth, depth), columns(n)], w_buf.at[slot], w_sem.at[slot])

    def sum_copy(n, i):
        slot, part = lax.rem(n, 2), pl.ds(i * slots, slots)
        return pltpu.make_async_copy(sum_hbm.at[part, :, :, columns(n)], sum_buf.at[slot, part], sum_sem.at[slot, i])

    def out_copy(n, i):
        slot, rows = lax.rem(n, 2), pl.ds(i * half, half)
        return pltpu.make_async_copy(out_buf.at[slot, rows], out_hbm.at[rows, columns(n)], out_sem.at[slot, i])

    first = jnp.int32(0)
    w_copy(first).start()
    for i in range(2):
        o_copy(i).start()
        sum_copy(first, i).start()
    w_copy(first + 1).start()

    def part(n, _):
        slot = lax.rem(n, 2)
        w_copy(n).wait()

        @pl.when(n + 1 < n_parts)
        def _():
            for i in range(2):
                sum_copy(n + 1, i).start()

        for i in range(2):
            @pl.when(n == 0)
            def _():
                o_copy(i).wait()

            @pl.when(n >= 2)
            def _():
                out_copy(n - 2, i).wait()

            sum_copy(n, i).wait()
            rows = pl.ds(i * half, half)
            so_far = sum_buf[slot, pl.ds(i * slots, slots)].reshape(half, REST_COLUMNS)
            out_buf[slot, rows, :] = (jnp.dot(o_buf[rows, :], w_buf[slot], preferred_element_type=f32) + so_far).astype(bf16)
            out_copy(n, i).start()

        @pl.when(n + 2 < n_parts)
        def _():
            w_copy(n + 2).start()
        return 0

    lax.fori_loop(0, n_parts, part, 0)
    for n in range(n_parts - 2, n_parts):
        for i in range(2):
            out_copy(n, i).wait()


def solution(mesh):
    n_seq = mesh.shape["seq"]

    def per_device(tokens, theta_q, theta_k, theta_v, w_out, w_init, inner_lr):
        n_batch, tok_dev, width_d = tokens.shape
        n_heads, head_dim, _ = w_init.shape
        n_groups = n_heads // HEADS_PER_GROUP
        n_rows, width = n_batch * tok_dev, n_heads * head_dim
        flat = tokens.reshape(n_rows, width_d)
        hbm, smem = pl.BlockSpec(memory_space=pl.ANY), pl.BlockSpec(memory_space=pltpu.SMEM)
        sum_slots = n_rows // (n_batch * head_dim)
        o, first_sum = pl.pallas_call(
            functools.partial(fused_kernel, n_seq, n_batch, tok_dev, n_groups),
            out_shape=(jax.ShapeDtypeStruct((n_batch, tok_dev, width - 256 * N_FIRST), bf16), jax.ShapeDtypeStruct((sum_slots, n_batch, head_dim, width_d), f32)),
            in_specs=[hbm] * 6 + [smem], out_specs=(hbm, hbm),
            scratch_shapes=[pltpu.VMEM((n_rows, width_d), bf16), pltpu.VMEM((3, n_groups, n_batch, tok_dev, 256), bf16),
                            pltpu.VMEM((2, width_d, 256), bf16), pltpu.VMEM((n_rows, 256), bf16), pltpu.VMEM((n_batch, tok_dev, 256), bf16),
                            pltpu.VMEM((n_groups + max(0, 2 * sum_slots - N_FIRST), n_batch, head_dim, 4 * head_dim), f32),
                            pltpu.VMEM((n_batch, head_dim, 4 * head_dim), f32), pltpu.VMEM((n_batch, head_dim, 4 * head_dim), f32),
                            pltpu.VMEM((HEADS_PER_GROUP, head_dim, head_dim), f32),
                            pltpu.SemaphoreType.DMA((2,)), pltpu.SemaphoreType.DMA((2,)), pltpu.SemaphoreType.DMA, pltpu.SemaphoreType.DMA((2,)),
                            pltpu.SemaphoreType.DMA, pltpu.SemaphoreType.DMA, pltpu.SemaphoreType.DMA((n_groups,))],
            compiler_params=pltpu.CompilerParams(collective_id=0, has_side_effects=True, vmem_limit_bytes=67043328),
            name="fused",
        )(flat, theta_k, theta_v, theta_q, w_out, w_init, inner_lr)
        depth = width - 256 * N_FIRST
        result = pl.pallas_call(
            rest_kernel,
            out_shape=jax.ShapeDtypeStruct((n_rows, width_d), bf16),
            in_specs=[hbm] * 3, out_specs=hbm,
            scratch_shapes=[pltpu.VMEM((n_rows, depth), bf16), pltpu.VMEM((2, depth, REST_COLUMNS), bf16),
                            pltpu.VMEM((2, sum_slots, n_batch, head_dim, REST_COLUMNS), f32), pltpu.VMEM((2, n_rows, REST_COLUMNS), bf16),
                            pltpu.SemaphoreType.DMA((2,)), pltpu.SemaphoreType.DMA((2,)), pltpu.SemaphoreType.DMA((2, 2)), pltpu.SemaphoreType.DMA((2, 2))],
            compiler_params=pltpu.CompilerParams(vmem_limit_bytes=67043328),
            name="rest",
        )(o.reshape(n_rows, depth), w_out, first_sum)
        return result.reshape(n_batch, tok_dev, width_d)

    tok_spec = P("data", "seq", None)
    return jax.shard_map(per_device, mesh=mesh, in_specs=(tok_spec, P(), P(), P(), P(), P(), P()), out_specs=tok_spec, check_vma=False)
```

```python
import functools

import jax
import jax.numpy as jnp
from jax import lax
from jax.experimental import pallas as pl
from jax.experimental.pallas import tpu as pltpu
from jax.sharding import PartitionSpec as P

MINI_BATCH = 16
HEADS_PER_GROUP = 4
SCHEDULE = ((0, 6, (0, 0, 0, 0, 0)), (1, 5, (0, 0, 0, 0, 0)), (3, 3, (0, 0, 0, 0, 0)), (3, 1, (0, 0, 0, 0, 0)),
            (4, 0, (0, 3, 3, 3, 3)), (5, 0, (3, 6, 6, 6, 6)), (5, 0, (3, 6, 6, 6, 6)), (5, 0, (4, 7, 7, 7, 7)))
N_FIRST = 7
REST_COLUMNS = 512
bf16, f32 = jnp.bfloat16, jnp.float32


def split3(x):
    a = x.astype(bf16)
    rest = x - a.astype(f32)
    b = rest.astype(bf16)
    return a, b, (rest - b.astype(f32)).astype(bf16)


def per_head_rows(x):
    rows = []
    for half in range(2):
        y = x[:, :, half * 128:(half + 1) * 128]
        turned, low = pltpu.roll(y, 64, 2), low_lanes(y.shape)
        rows += [jnp.where(low, y, turned), jnp.where(low, turned, y)]
    return rows


def low_lanes(shape):
    return lax.broadcasted_iota(jnp.int32, shape, 2) < 64


def under(rows):
    n, t, width = rows[0].shape
    return jnp.concatenate([r.reshape(n, 1, t, width) for r in rows], axis=1).reshape(n, t * len(rows), width)


def own_columns(z, first):
    a, b, c, d = (z[:, first + i * MINI_BATCH:first + (i + 1) * MINI_BATCH, (i // 2) * 128:(i // 2 + 1) * 128] for i in range(4))
    low = low_lanes(a.shape)
    return jnp.concatenate([jnp.where(low, a, b), jnp.where(low, c, d)], axis=2)


def times_w(rows, w):
    m = under(rows)
    return jnp.concatenate([m, m], axis=2), jnp.concatenate([*split3(w), jnp.zeros(w.shape, bf16)], axis=1)


def k_transposed_times(k_rows, r):
    zero = jnp.zeros((*r.shape[:2], 128), bf16)
    low = low_lanes(zero.shape)
    rows = []
    for part in split3(r):
        a, b = part[:, :, :128], part[:, :, 128:]
        rows += [jnp.concatenate(pair, axis=2) for pair in (
            (jnp.where(low, a, zero), zero), (jnp.where(low, zero, a), zero), (zero, jnp.where(low, b, zero)), (zero, jnp.where(low, zero, b)))]
    rhs = jnp.concatenate([under(rows), jnp.zeros((r.shape[0], 4 * MINI_BATCH, 256), bf16)], axis=1)
    twice = under(k_rows + k_rows)
    turned = [twice[i].T[:64] for i in range(r.shape[0])]
    return [jnp.concatenate([t, t], axis=1) for t in turned], rhs


def fused_kernel(n_seq, n_batch, tok_dev, n_groups, x_hbm, theta_k_hbm, theta_v_hbm, theta_q_hbm, w_out_hbm, w_init_hbm, lr_ref, o_hbm, sum_hbm,
                 x_buf, kvq_buf, theta_buf, tile_buf, o_buf, w_buf, w_now, w_send, init_buf, x_sem, theta_sem, out_sem, sum_sem, init_sem, send_sem, recv_sem):
    me = lax.axis_index("seq")
    lag, n_late = jnp.int32(0), jnp.int32(0)
    for place, (ahead, late, _) in enumerate(SCHEDULE):
        lag = jnp.where(me == place, ahead, lag)
        n_late = jnp.where(me == place, late, n_late)

    outs_beside = (n_late == 0) & (lag + 1 + N_FIRST >= n_groups)

    def outs_before(g):
        n = jnp.int32(0)
        for place, (_, _, counts) in enumerate(SCHEDULE):
            for i, count in enumerate(counts):
                n = jnp.where((me == place) & (g >= N_FIRST + i), count, n)
        return n

    n_tiles = 3 * n_groups
    n_out_tiles = sum_hbm.shape[-1] // 256
    w_first = w_buf.shape[0] - n_groups
    first_depth = N_FIRST * 256
    n_rows = n_batch * tok_dev
    n_steps = tok_dev // MINI_BATCH
    chunk = n_rows // n_steps
    depth = x_buf.shape[1]
    thetas = (theta_k_hbm, theta_v_hbm, theta_q_hbm)
    barrier = pltpu.get_barrier_semaphore()

    def columns(g):
        return pl.ds(pl.multiple_of(g * 256, 256), 256)

    def tile_at(c):
        early, body = 2 * n_late, c - 2 * n_late
        kind = jnp.where(c < early, lax.rem(c, 2), jnp.where(c < n_tiles - n_late, lax.rem(body, 3), 2))
        g = jnp.where(c < early, c // 2, jnp.where(c < n_tiles - n_late, n_late + body // 3, c - (n_tiles - n_late)))
        return kind, g

    def start_theta(c):
        kind, g = tile_at(c)
        for i in range(3):
            @pl.when((kind == i) & (c < n_tiles))
            def _():
                pltpu.make_async_copy(thetas[i].at[:, columns(g)], theta_buf.at[lax.rem(c, 2)], theta_sem.at[lax.rem(c, 2)]).start()

        @pl.when((c >= n_tiles) & (c < n_tiles + n_out_tiles))
        def _():
            w_out_copy(c - n_tiles, lax.rem(c, 2)).start()

    def w_out_copy(n, slot):
        return pltpu.make_async_copy(w_out_hbm.at[pl.ds(0, first_depth), columns(n)], theta_buf.at[slot, pl.ds(0, first_depth)], theta_sem.at[slot])

    def wait_theta(c):
        slot = lax.rem(c, 2)
        pltpu.make_async_copy(theta_k_hbm.at[:, pl.ds(0, 256)], theta_buf.at[slot], theta_sem.at[slot]).wait()

    def result(g):
        return pltpu.make_async_copy(o_buf, o_hbm.at[:, :, columns(g - N_FIRST)], out_sem)

    def sum_copy(n):
        part = lax.rem(n, 2)
        return pltpu.make_async_copy(w_buf.at[pl.ds(part * sum_slots, sum_slots)], sum_hbm.at[:, :, :, columns(n)], sum_sem.at[part])

    def hand_on(g):
        return pltpu.make_async_remote_copy(w_send, w_buf.at[w_first + g], send_sem, recv_sem.at[g],
                                            device_id={"seq": lax.rem(me + 1, n_seq)}, device_id_type=pl.DeviceIdType.MESH)

    sum_slots = sum_hbm.shape[0]

    def first_w(g):
        return pltpu.make_async_copy(w_init_hbm.at[pl.ds(g * HEADS_PER_GROUP, HEADS_PER_GROUP)], init_buf, init_sem)

    def x_copy(i):
        rows = pl.ds(i * (n_rows // 2), n_rows // 2)
        return pltpu.make_async_copy(x_hbm.at[rows], x_buf.at[rows], x_sem.at[i])

    start_theta(jnp.int32(0))
    for i in range(2):
        x_copy(i).start()

    @pl.when(me == 0)
    def _():
        first_w(0).start()

    for peer in (lax.rem(me + 1, n_seq), lax.rem(me + n_seq - 1, n_seq)):
        pl.semaphore_signal(barrier, inc=1, device_id={"seq": peer}, device_id_type=pl.DeviceIdType.MESH)

    head = lax.broadcasted_iota(jnp.int32, (1, 256), 1) // 64

    half = n_batch // 2

    def tokens(kind, g, units, j):
        return kvq_buf[kind, g, units, pl.ds(j * MINI_BATCH, MINI_BATCH), :]

    def chain_step(g, eta, j, now, before):
        k_rows = z = None
        if now is not None:
            k_rows = per_head_rows(tokens(0, g, now, j)) if j < n_steps else []
            rows = k_rows + (per_head_rows(tokens(2, g, now, j - 1)) if j > 0 else [])
            lhs, rhs = times_w(rows, w_now[now])
        if before is not None:
            units, step, keys, inputs = before
            r = (inputs - tokens(1, g, units, step).astype(f32)) * eta
            lhs_u, rhs_u = k_transposed_times(keys, r)
        prod, change = [], []
        for i in range(half):
            if now is not None:
                prod.append(jnp.dot(lhs[i], rhs[i], preferred_element_type=f32))
            if before is not None:
                change.append(jnp.dot(lhs_u[i], rhs_u[i], preferred_element_type=f32))
        if now is not None:
            prod = jnp.stack(prod)
            if j < n_steps:
                z = own_columns(prod, 0)
            if j > 0:
                o_buf[now, pl.ds((j - 1) * MINI_BATCH, MINI_BATCH), :] = own_columns(prod, 4 * MINI_BATCH if j < n_steps else 0).astype(bf16)
        if before is not None:
            w_now[units] = w_now[units] - jnp.stack(change)
        return k_rows, z

    def chain(g, eta, fill):
        one, two = pl.ds(0, half), pl.ds(half, half)
        open_two = None
        for j in range(n_steps):
            put = fill(j)
            open_one = (one, j, *chain_step(g, eta, j, one, open_two))
            open_two = (two, j, *chain_step(g, eta, j, two, open_one))
            put()
        chain_step(g, eta, n_steps, None, open_two)

    def whole_tile(c, group=None):
        kind, g = tile_at(c)
        slot = lax.rem(c, 2)
        wait_theta(c)
        start_theta(c + 1)
        for i in range(2):
            rows = pl.ds(i * (n_rows // 2), n_rows // 2)
            if isinstance(c, int):
                x_copy(i).wait()
            pieces = [pl.ds(i * (n_rows // 2) + p * (n_rows // 4), n_rows // 4) for p in range(2)] if isinstance(c, int) else [rows]
            part = jnp.concatenate([jnp.dot(x_buf[p, :], theta_buf[slot], preferred_element_type=f32).astype(bf16) for p in pieces], axis=0)
            if group is not None and i == 0:
                last_results(group)
                before = tile_at(c - 1)
                kvq_buf[before[0], before[1]] = tile_buf[...].reshape(n_batch, tok_dev, 256)
            kvq_buf[kind, g, pl.ds(i * half, half)] = part.reshape(half, tok_dev, 256)

    def out_tile(n):
        c = n_tiles + n
        slot = lax.rem(c, 2)
        w_out_copy(n, slot).wait()
        start_theta(c + 1)

        @pl.when(n >= 2)
        def _():
            sum_copy(n - 2).wait()

        for i in range(2):
            rows = pl.ds(i * (n_rows // 2), n_rows // 2)
            lhs = jnp.concatenate([kvq_buf[2, g, pl.ds(i * half, half)].reshape(n_rows // 2, 256) for g in range(N_FIRST)], axis=1)
            part = jnp.dot(lhs, theta_buf[slot, :first_depth, :], preferred_element_type=f32)
            w_buf[pl.ds(lax.rem(n, 2) * sum_slots + i * (sum_slots // 2), sum_slots // 2)] = part.reshape(sum_slots // 2, *w_buf.shape[1:])
        sum_copy(n).start()

    def inner(g, first_time, c, n=None):
        slot = lax.rem(jnp.where(c < n_tiles, c, c - 1), 2) if n is None else lax.rem(c, 2)

        if n is None:
            @pl.when(c < n_tiles)
            def _():
                wait_theta(c)
                start_theta(c + 1)
        else:
            w_out_copy(n, slot).wait()
            start_theta(c + 1)

            @pl.when(n >= 2)
            def _():
                sum_copy(n - 2).wait()

        @pl.when((me == 0) & first_time)
        def _():
            first_w(g).wait()
            start = jnp.concatenate([init_buf[h] for h in range(HEADS_PER_GROUP)], axis=1)
            for b in range(n_batch):
                w_buf[w_first + g, b] = start

        @pl.when((me == 0) & first_time & (g + 1 < n_groups))
        def _():
            first_w(g + 1).start()

        @pl.when((me > 0) & first_time)
        def _():
            hand_on(g).wait_recv()

        @pl.when(jnp.where(first_time, g > N_FIRST, g == 0))
        def _():
            result(N_FIRST).wait()

        eta = jnp.zeros((1, 256), f32)
        for h in range(HEADS_PER_GROUP):
            eta = jnp.where(head == h, (2.0 / MINI_BATCH) * lr_ref[g * HEADS_PER_GROUP + h], eta)

        w_now[...] = w_buf[w_first + g]
        if n is not None:
            theta_buf[slot, first_depth:, :] = jnp.zeros((depth - first_depth, 256), bf16)

        if n is None:
            def fill(j):
                part = pl.ds(j * chunk, chunk)
                tile_part = jnp.dot(x_buf[part, :], theta_buf[slot], preferred_element_type=f32)

                def put():
                    tile_buf[part, :] = tile_part.astype(bf16)
                return put
        else:
            def fill(j):
                b, first = j * chunk // tok_dev, j * chunk % tok_dev
                lhs = jnp.concatenate([kvq_buf[2, i, b, pl.ds(first, chunk), :] for i in range(N_FIRST)], axis=1)
                lhs = jnp.concatenate([lhs, x_buf[pl.ds(j * chunk, chunk), :depth - first_depth]], axis=1)
                part = jnp.dot(lhs, theta_buf[slot], preferred_element_type=f32)
                rows = n_batch * w_buf.shape[2]
                at, within = j * chunk // rows, j * chunk % rows // w_buf.shape[2]

                def put():
                    w_buf[lax.rem(n, 2) * sum_slots + at, pl.ds(within, chunk // w_buf.shape[2])] = part.reshape(chunk // w_buf.shape[2], *w_buf.shape[2:])
                return put

        chain(g, eta, fill)

        @pl.when((me < n_seq - 1) & first_time & (g > 0))
        def _():
            hand_on(0).wait_send()

        @pl.when((me < n_seq - 1) & first_time)
        def _():
            w_send[...] = w_now[...]
            hand_on(g).start()

        if n is not None:
            sum_copy(n).start()

    def last_results(g):
        for units in (pl.ds(0, half), pl.ds(half, half)):
            chain_step(g, None, n_steps, units, None)
        kvq_buf[2, g] = o_buf[...]

    def send_result(g, first_time):
        @pl.when((g >= N_FIRST) & (jnp.logical_not(first_time) | (g >= n_late)))
        def _():
            result(g).start()

    def slot_body(s, _):
        @pl.when(s == 1)
        def _():
            pl.semaphore_wait(barrier, 2)

        first_time = s <= n_groups + lag
        g = jnp.where(first_time, s - 1 - lag, s - (n_groups + 1 + lag))
        fresh = s < n_groups
        c = jnp.where(fresh, 2 * s + jnp.maximum(s - n_late, 0), jnp.minimum(n_tiles - n_late + s - n_groups, n_tiles))
        beside_out = outs_beside & first_time & (g >= N_FIRST)
        n_out = jnp.where(beside_out, outs_before(g) + g - N_FIRST, 0)

        def outs(n, _):
            out_tile(n)
            return 0

        lax.fori_loop(jnp.where(beside_out, outs_before(g - 1) + g - N_FIRST, 0), n_out, outs, 0)

        @pl.when((g >= 0) & jnp.logical_not(beside_out))
        def _():
            inner(g, first_time, c)

        @pl.when(beside_out)
        def _():
            inner(g, first_time, n_tiles + n_out, n_out)

        @pl.when((g >= 0) & fresh)
        def _():
            whole_tile(c + 1, g)
            send_result(g, first_time)

        @pl.when((g >= 0) & jnp.logical_not(fresh))
        def _():
            last_results(g)
            send_result(g, first_time)

            @pl.when(c < n_tiles)
            def _():
                kind, of = tile_at(c)
                kvq_buf[kind, of] = tile_buf[...].reshape(n_batch, tok_dev, 256)

        def rest(i, _):
            whole_tile(c + i)
            return 0

        @pl.when(fresh)
        def _():
            lax.fori_loop(jnp.where(g >= 0, 2, jnp.where(s == 0, 1, 0)), jnp.where(s < n_late, 2, 3), rest, 0)
        return 0

    whole_tile(0)
    lax.fori_loop(0, n_groups + 1 + lag + n_late, slot_body, 0)

    def outs(n, _):
        out_tile(n)
        return 0

    lax.fori_loop(jnp.where(outs_beside, outs_before(n_groups) + n_groups - N_FIRST, 0), n_out_tiles, outs, 0)
    for n in range(2):
        sum_copy(n_out_tiles - 2 + n).wait()

    @pl.when(n_late == 0)
    def _():
        result(N_FIRST).wait()

    @pl.when(me < n_seq - 1)
    def _():
        hand_on(0).wait_send()


def rest_kernel(o_hbm, w_hbm, sum_hbm, out_hbm, o_buf, w_buf, sum_buf, out_buf, o_sem, w_sem, sum_sem, out_sem):
    n_rows, depth = o_buf.shape
    half, slots = n_rows // 2, sum_buf.shape[1] // 2
    n_parts = out_hbm.shape[1] // REST_COLUMNS

    def columns(n):
        return pl.ds(pl.multiple_of(n * REST_COLUMNS, REST_COLUMNS), REST_COLUMNS)

    def o_copy(i):
        rows = pl.ds(i * half, half)
        return pltpu.make_async_copy(o_hbm.at[rows], o_buf.at[rows], o_sem.at[i])

    def w_copy(n):
        slot = lax.rem(n, 3)
        return pltpu.make_async_copy(w_hbm.at[pl.ds(w_hbm.shape[0] - depth, depth), columns(n)], w_buf.at[slot], w_sem.at[slot])

    def sum_copy(n, i):
        slot, part = lax.rem(n, 3), pl.ds(i * slots, slots)
        return pltpu.make_async_copy(sum_hbm.at[part, :, :, columns(n)], sum_buf.at[slot, part], sum_sem.at[slot, i])

    def out_copy(n, i):
        slot, rows = lax.rem(n, 2), pl.ds(i * half, half)
        return pltpu.make_async_copy(out_buf.at[slot, rows], out_hbm.at[rows, columns(n)], out_sem.at[slot, i])

    def start(n):
        w_copy(n).start()
        for i in range(2):
            sum_copy(n, i).start()

    def product(n, i):
        rows = pl.ds(i * half, half)
        so_far = sum_buf[lax.rem(n, 3), pl.ds(i * slots, slots)].reshape(half, REST_COLUMNS)
        part = jnp.dot(o_buf[rows, :], w_buf[lax.rem(n, 3)], preferred_element_type=f32)
        out_buf[lax.rem(n, 2), rows, :] = (part + so_far).astype(bf16)

    first = jnp.int32(0)
    w_copy(first).start()
    for i in range(2):
        o_copy(i).start()
        sum_copy(first, i).start()
    start(first + 1)
    w_copy(first).wait()
    for i in range(2):
        o_copy(i).wait()
        sum_copy(first, i).wait()
        product(first, i)
        out_copy(first, i).start()

    def part(n, _):
        @pl.when((n >= 2) & (n + 1 < n_parts))
        def _():
            start(n + 1)

        @pl.when(n >= 2)
        def _():
            for i in range(2):
                out_copy(n - 2, i).wait()

        w_copy(n).wait()
        for i in range(2):
            sum_copy(n, i).wait()
        for i in range(2):
            product(n, i)
        for i in range(2):
            out_copy(n, i).start()
        return 0

    start(first + 2)
    lax.fori_loop(1, n_parts, part, 0)
    for n in range(n_parts - 2, n_parts):
        for i in range(2):
            out_copy(n, i).wait()


def solution(mesh):
    n_seq = mesh.shape["seq"]

    def per_device(tokens, theta_q, theta_k, theta_v, w_out, w_init, inner_lr):
        n_batch, tok_dev, width_d = tokens.shape
        n_heads, head_dim, _ = w_init.shape
        n_groups = n_heads // HEADS_PER_GROUP
        n_rows, width = n_batch * tok_dev, n_heads * head_dim
        flat = tokens.reshape(n_rows, width_d)
        hbm, smem = pl.BlockSpec(memory_space=pl.ANY), pl.BlockSpec(memory_space=pltpu.SMEM)
        sum_slots = n_rows // (n_batch * head_dim)
        o, first_sum = pl.pallas_call(
            functools.partial(fused_kernel, n_seq, n_batch, tok_dev, n_groups),
            out_shape=(jax.ShapeDtypeStruct((n_batch, tok_dev, width - 256 * N_FIRST), bf16), jax.ShapeDtypeStruct((sum_slots, n_batch, head_dim, width_d), f32)),
            in_specs=[hbm] * 6 + [smem], out_specs=(hbm, hbm),
            scratch_shapes=[pltpu.VMEM((n_rows, width_d), bf16), pltpu.VMEM((3, n_groups, n_batch, tok_dev, 256), bf16),
                            pltpu.VMEM((2, width_d, 256), bf16), pltpu.VMEM((n_rows, 256), bf16), pltpu.VMEM((n_batch, tok_dev, 256), bf16),
                            pltpu.VMEM((n_groups + max(0, 2 * sum_slots - N_FIRST), n_batch, head_dim, 4 * head_dim), f32),
                            pltpu.VMEM((n_batch, head_dim, 4 * head_dim), f32), pltpu.VMEM((n_batch, head_dim, 4 * head_dim), f32),
                            pltpu.VMEM((HEADS_PER_GROUP, head_dim, head_dim), f32),
                            pltpu.SemaphoreType.DMA((2,)), pltpu.SemaphoreType.DMA((2,)), pltpu.SemaphoreType.DMA, pltpu.SemaphoreType.DMA((2,)),
                            pltpu.SemaphoreType.DMA, pltpu.SemaphoreType.DMA, pltpu.SemaphoreType.DMA((n_groups,))],
            compiler_params=pltpu.CompilerParams(collective_id=0, has_side_effects=True, vmem_limit_bytes=67043328),
            name="fused",
        )(flat, theta_k, theta_v, theta_q, w_out, w_init, inner_lr)
        depth = width - 256 * N_FIRST
        result = pl.pallas_call(
            rest_kernel,
            out_shape=jax.ShapeDtypeStruct((n_rows, width_d), bf16),
            in_specs=[hbm] * 3, out_specs=hbm,
            scratch_shapes=[pltpu.VMEM((n_rows, depth), bf16), pltpu.VMEM((3, depth, REST_COLUMNS), bf16),
                            pltpu.VMEM((3, sum_slots, n_batch, head_dim, REST_COLUMNS), f32), pltpu.VMEM((2, n_rows, REST_COLUMNS), bf16),
                            pltpu.SemaphoreType.DMA((2,)), pltpu.SemaphoreType.DMA((3,)), pltpu.SemaphoreType.DMA((3, 2)), pltpu.SemaphoreType.DMA((2, 2))],
            compiler_params=pltpu.CompilerParams(vmem_limit_bytes=67043328),
            name="rest",
        )(o.reshape(n_rows, depth), w_out, first_sum)
        return result.reshape(n_batch, tok_dev, width_d)

    tok_spec = P("data", "seq", None)
    return jax.shard_map(per_device, mesh=mesh, in_specs=(tok_spec, P(), P(), P(), P(), P(), P()), out_specs=tok_spec, check_vma=False)
```

```python
import functools

import jax
import jax.numpy as jnp
from jax import lax
from jax.experimental import pallas as pl
from jax.experimental.pallas import tpu as pltpu
from jax.sharding import PartitionSpec as P

MINI_BATCH = 16
HEADS_PER_GROUP = 4
SCHEDULE = ((0, 7, (0, 0, 0, 0, 0)), (1, 6, (0, 0, 0, 0, 0)), (3, 4, (0, 0, 0, 0, 0)), (3, 1, (0, 0, 0, 0, 0)),
            (4, 0, (0, 3, 3, 3, 3)), (4, 0, (0, 3, 3, 3, 3)), (5, 0, (3, 6, 6, 6, 6)), (5, 0, (4, 7, 7, 7, 7)))
N_FIRST = 7
REST_COLUMNS = 512
bf16, f32 = jnp.bfloat16, jnp.float32


def split3(x):
    a = x.astype(bf16)
    rest = x - a.astype(f32)
    b = rest.astype(bf16)
    return a, b, (rest - b.astype(f32)).astype(bf16)


def per_head_rows(x):
    rows = []
    for half in range(2):
        y = x[:, :, half * 128:(half + 1) * 128]
        turned, low = pltpu.roll(y, 64, 2), low_lanes(y.shape)
        rows += [jnp.where(low, y, turned), jnp.where(low, turned, y)]
    return rows


def low_lanes(shape):
    return lax.broadcasted_iota(jnp.int32, shape, 2) < 64


def under(rows):
    n, t, width = rows[0].shape
    return jnp.concatenate([r.reshape(n, 1, t, width) for r in rows], axis=1).reshape(n, t * len(rows), width)


def own_columns(z, first):
    a, b, c, d = (z[:, first + i * MINI_BATCH:first + (i + 1) * MINI_BATCH, (i // 2) * 128:(i // 2 + 1) * 128] for i in range(4))
    low = low_lanes(a.shape)
    return jnp.concatenate([jnp.where(low, a, b), jnp.where(low, c, d)], axis=2)


def times_w(rows, w):
    m = under(rows)
    return jnp.concatenate([m, m], axis=2), jnp.concatenate([*split3(w), jnp.zeros(w.shape, bf16)], axis=1)


def k_transposed_times(k_rows, r):
    zero = jnp.zeros((*r.shape[:2], 128), bf16)
    low = low_lanes(zero.shape)
    rows = []
    for part in split3(r):
        a, b = part[:, :, :128], part[:, :, 128:]
        rows += [jnp.concatenate(pair, axis=2) for pair in (
            (jnp.where(low, a, zero), zero), (jnp.where(low, zero, a), zero), (zero, jnp.where(low, b, zero)), (zero, jnp.where(low, zero, b)))]
    rhs = jnp.concatenate([under(rows), jnp.zeros((r.shape[0], 4 * MINI_BATCH, 256), bf16)], axis=1)
    twice = under(k_rows + k_rows)
    turned = [twice[i].T[:64] for i in range(r.shape[0])]
    return [jnp.concatenate([t, t], axis=1) for t in turned], rhs


def fused_kernel(n_seq, n_batch, tok_dev, n_groups, x_hbm, theta_k_hbm, theta_v_hbm, theta_q_hbm, w_out_hbm, w_init_hbm, lr_ref, o_hbm, sum_hbm,
                 x_buf, kvq_buf, theta_buf, tile_buf, o_buf, w_buf, w_now, w_send, init_buf, x_sem, theta_sem, out_sem, sum_sem, init_sem, send_sem, recv_sem):
    me = lax.axis_index("seq")
    lag, n_late = jnp.int32(0), jnp.int32(0)
    for place, (ahead, late, _) in enumerate(SCHEDULE):
        lag = jnp.where(me == place, ahead, lag)
        n_late = jnp.where(me == place, late, n_late)

    outs_beside = (n_late == 0) & (lag + 1 + N_FIRST >= n_groups)

    def outs_before(g):
        n = jnp.int32(0)
        for place, (_, _, counts) in enumerate(SCHEDULE):
            for i, count in enumerate(counts):
                n = jnp.where((me == place) & (g >= N_FIRST + i), count, n)
        return n

    n_tiles = 3 * n_groups
    n_out_tiles = sum_hbm.shape[-1] // 256
    w_first = w_buf.shape[0] - n_groups
    first_depth = N_FIRST * 256
    n_rows = n_batch * tok_dev
    n_steps = tok_dev // MINI_BATCH
    chunk = n_rows // n_steps
    depth = x_buf.shape[1]
    thetas = (theta_k_hbm, theta_v_hbm, theta_q_hbm)
    barrier = pltpu.get_barrier_semaphore()

    def columns(g):
        return pl.ds(pl.multiple_of(g * 256, 256), 256)

    def tile_at(c):
        early, body = 2 * n_late, c - 2 * n_late
        kind = jnp.where(c < early, lax.rem(c, 2), jnp.where(c < n_tiles - n_late, lax.rem(body, 3), 2))
        g = jnp.where(c < early, c // 2, jnp.where(c < n_tiles - n_late, n_late + body // 3, c - (n_tiles - n_late)))
        return kind, g

    def start_theta(c):
        kind, g = tile_at(c)
        for i in range(3):
            @pl.when((kind == i) & (c < n_tiles))
            def _():
                pltpu.make_async_copy(thetas[i].at[:, columns(g)], theta_buf.at[lax.rem(c, 2)], theta_sem.at[lax.rem(c, 2)]).start()

        @pl.when((c >= n_tiles) & (c < n_tiles + n_out_tiles))
        def _():
            w_out_copy(c - n_tiles, lax.rem(c, 2)).start()

    def w_out_copy(n, slot):
        return pltpu.make_async_copy(w_out_hbm.at[pl.ds(0, first_depth), columns(n)], theta_buf.at[slot, pl.ds(0, first_depth)], theta_sem.at[slot])

    def wait_theta(c):
        slot = lax.rem(c, 2)
        pltpu.make_async_copy(theta_k_hbm.at[:, pl.ds(0, 256)], theta_buf.at[slot], theta_sem.at[slot]).wait()

    def result(g):
        return pltpu.make_async_copy(o_buf, o_hbm.at[:, :, columns(g - N_FIRST)], out_sem)

    def sum_copy(n):
        part = lax.rem(n, 2)
        return pltpu.make_async_copy(w_buf.at[pl.ds(part * sum_slots, sum_slots)], sum_hbm.at[:, :, :, columns(n)], sum_sem.at[part])

    def hand_on(g):
        return pltpu.make_async_remote_copy(w_send, w_buf.at[w_first + g], send_sem, recv_sem.at[g],
                                            device_id={"seq": lax.rem(me + 1, n_seq)}, device_id_type=pl.DeviceIdType.MESH)

    sum_slots = sum_hbm.shape[0]

    def first_w(g):
        return pltpu.make_async_copy(w_init_hbm.at[pl.ds(g * HEADS_PER_GROUP, HEADS_PER_GROUP)], init_buf, init_sem)

    def x_copy(i):
        rows = pl.ds(i * (n_rows // 2), n_rows // 2)
        return pltpu.make_async_copy(x_hbm.at[rows], x_buf.at[rows], x_sem.at[i])

    start_theta(jnp.int32(0))
    for i in range(2):
        x_copy(i).start()

    @pl.when(me == 0)
    def _():
        first_w(0).start()

    for peer in (lax.rem(me + 1, n_seq), lax.rem(me + n_seq - 1, n_seq)):
        pl.semaphore_signal(barrier, inc=1, device_id={"seq": peer}, device_id_type=pl.DeviceIdType.MESH)

    head = lax.broadcasted_iota(jnp.int32, (1, 256), 1) // 64

    half = n_batch // 2

    def tokens(kind, g, units, j):
        return kvq_buf[kind, g, units, pl.ds(j * MINI_BATCH, MINI_BATCH), :]

    def chain_step(g, eta, j, now, before, w_start=None):
        k_rows = z = None
        if now is not None:
            k_rows = per_head_rows(tokens(0, g, now, j)) if j < n_steps else []
            rows = k_rows + (per_head_rows(tokens(2, g, now, j - 1)) if j > 0 else [])
            lhs, rhs = times_w(rows, w_now[now] if w_start is None or j > 0 else w_start[now])
        if before is not None:
            units, step, keys, inputs = before
            r = (inputs - tokens(1, g, units, step).astype(f32)) * eta
            lhs_u, rhs_u = k_transposed_times(keys, r)
        prod, change = [], []
        for i in range(half):
            if now is not None:
                prod.append(jnp.dot(lhs[i], rhs[i], preferred_element_type=f32))
            if before is not None:
                change.append(jnp.dot(lhs_u[i], rhs_u[i], preferred_element_type=f32))
        if now is not None:
            prod = jnp.stack(prod)
            if j < n_steps:
                z = own_columns(prod, 0)
            if j > 0:
                o_buf[now, pl.ds((j - 1) * MINI_BATCH, MINI_BATCH), :] = own_columns(prod, 4 * MINI_BATCH if j < n_steps else 0).astype(bf16)
        if before is not None:
            w_now[units] = (w_now[units] if w_start is None or step > 0 else w_start[units]) - jnp.stack(change)
        return k_rows, z

    def chain(g, eta, fill, w_start=None):
        one, two = pl.ds(0, half), pl.ds(half, half)
        open_two = None
        for j in range(n_steps):
            put = fill(j)
            open_one = (one, j, *chain_step(g, eta, j, one, open_two, w_start))
            open_two = (two, j, *chain_step(g, eta, j, two, open_one, w_start))
            put()
        chain_step(g, eta, n_steps, None, open_two)

    def whole_tile(c, group=None):
        kind, g = tile_at(c)
        slot = lax.rem(c, 2)
        wait_theta(c)
        start_theta(c + 1)
        for i in range(2):
            rows = pl.ds(i * (n_rows // 2), n_rows // 2)
            if isinstance(c, int):
                x_copy(i).wait()
            pieces = [pl.ds(i * (n_rows // 2) + p * (n_rows // 4), n_rows // 4) for p in range(2)] if isinstance(c, int) else [rows]
            part = jnp.concatenate([jnp.dot(x_buf[p, :], theta_buf[slot], preferred_element_type=f32).astype(bf16) for p in pieces], axis=0)
            if group is not None and i == 0:
                last_results(group)
                before = tile_at(c - 1)
                kvq_buf[before[0], before[1]] = tile_buf[...].reshape(n_batch, tok_dev, 256)
            kvq_buf[kind, g, pl.ds(i * half, half)] = part.reshape(half, tok_dev, 256)

    def out_tile(n):
        c = n_tiles + n
        slot = lax.rem(c, 2)
        w_out_copy(n, slot).wait()
        start_theta(c + 1)

        @pl.when(n >= 2)
        def _():
            sum_copy(n - 2).wait()

        for i in range(2):
            rows = pl.ds(i * (n_rows // 2), n_rows // 2)
            lhs = jnp.concatenate([kvq_buf[2, g, pl.ds(i * half, half)].reshape(n_rows // 2, 256) for g in range(N_FIRST)], axis=1)
            part = jnp.dot(lhs, theta_buf[slot, :first_depth, :], preferred_element_type=f32)
            w_buf[pl.ds(lax.rem(n, 2) * sum_slots + i * (sum_slots // 2), sum_slots // 2)] = part.reshape(sum_slots // 2, *w_buf.shape[1:])
        sum_copy(n).start()

    def inner(g, first_time, c, n=None):
        slot = lax.rem(jnp.where(c < n_tiles, c, c - 1), 2) if n is None else lax.rem(c, 2)

        if n is None:
            @pl.when(c < n_tiles)
            def _():
                wait_theta(c)
                start_theta(c + 1)
        else:
            w_out_copy(n, slot).wait()
            start_theta(c + 1)

            @pl.when(n >= 2)
            def _():
                sum_copy(n - 2).wait()

        @pl.when((me == 0) & first_time)
        def _():
            first_w(g).wait()
            start = jnp.concatenate([init_buf[h] for h in range(HEADS_PER_GROUP)], axis=1)
            for b in range(n_batch):
                w_buf[w_first + g, b] = start

        @pl.when((me == 0) & first_time & (g + 1 < n_groups))
        def _():
            first_w(g + 1).start()

        @pl.when((me > 0) & first_time)
        def _():
            hand_on(g).wait_recv()

        @pl.when(jnp.where(first_time, g > N_FIRST, g == 0))
        def _():
            result(N_FIRST).wait()

        eta = jnp.zeros((1, 256), f32)
        for h in range(HEADS_PER_GROUP):
            eta = jnp.where(head == h, (2.0 / MINI_BATCH) * lr_ref[g * HEADS_PER_GROUP + h], eta)

        if n is not None:
            w_now[...] = w_buf[w_first + g]
            theta_buf[slot, first_depth:, :] = jnp.zeros((depth - first_depth, 256), bf16)

        if n is None:
            def fill(j):
                part = pl.ds(j * chunk, chunk)
                tile_part = jnp.dot(x_buf[part, :], theta_buf[slot], preferred_element_type=f32)

                def put():
                    tile_buf[part, :] = tile_part.astype(bf16)
                return put
        else:
            def fill(j):
                b, first = j * chunk // tok_dev, j * chunk % tok_dev
                lhs = jnp.concatenate([kvq_buf[2, i, b, pl.ds(first, chunk), :] for i in range(N_FIRST)], axis=1)
                lhs = jnp.concatenate([lhs, x_buf[pl.ds(j * chunk, chunk), :depth - first_depth]], axis=1)
                part = jnp.dot(lhs, theta_buf[slot], preferred_element_type=f32)
                rows = n_batch * w_buf.shape[2]
                at, within = j * chunk // rows, j * chunk % rows // w_buf.shape[2]

                def put():
                    w_buf[lax.rem(n, 2) * sum_slots + at, pl.ds(within, chunk // w_buf.shape[2])] = part.reshape(chunk // w_buf.shape[2], *w_buf.shape[2:])
                return put

        chain(g, eta, fill, w_buf.at[w_first + g] if n is None else None)

        @pl.when((me < n_seq - 1) & first_time & (g > 0))
        def _():
            hand_on(0).wait_send()

        @pl.when((me < n_seq - 1) & first_time)
        def _():
            w_send[...] = w_now[...]
            hand_on(g).start()

        if n is not None:
            sum_copy(n).start()

    def last_results(g):
        for units in (pl.ds(0, half), pl.ds(half, half)):
            chain_step(g, None, n_steps, units, None)
        kvq_buf[2, g] = o_buf[...]

    def send_result(g, first_time):
        @pl.when((g >= N_FIRST) & (jnp.logical_not(first_time) | (g >= n_late)))
        def _():
            result(g).start()

    def slot_body(s, _):
        @pl.when(s == 1)
        def _():
            pl.semaphore_wait(barrier, 2)

        first_time = s <= n_groups + lag
        g = jnp.where(first_time, s - 1 - lag, s - (n_groups + 1 + lag))
        fresh = s < n_groups
        c = jnp.where(fresh, 2 * s + jnp.maximum(s - n_late, 0), jnp.minimum(n_tiles - n_late + s - n_groups, n_tiles))
        beside_out = outs_beside & first_time & (g >= N_FIRST)
        n_out = jnp.where(beside_out, outs_before(g) + g - N_FIRST, 0)

        def outs(n, _):
            out_tile(n)
            return 0

        lax.fori_loop(jnp.where(beside_out, outs_before(g - 1) + g - N_FIRST, 0), n_out, outs, 0)

        @pl.when((g >= 0) & jnp.logical_not(beside_out))
        def _():
            inner(g, first_time, c)

        @pl.when(beside_out)
        def _():
            inner(g, first_time, n_tiles + n_out, n_out)

        @pl.when((g >= 0) & fresh)
        def _():
            whole_tile(c + 1, g)
            send_result(g, first_time)

        @pl.when((g >= 0) & jnp.logical_not(fresh))
        def _():
            last_results(g)
            send_result(g, first_time)

            @pl.when(c < n_tiles)
            def _():
                kind, of = tile_at(c)
                kvq_buf[kind, of] = tile_buf[...].reshape(n_batch, tok_dev, 256)

        def rest(i, _):
            whole_tile(c + i)
            return 0

        @pl.when(fresh)
        def _():
            lax.fori_loop(jnp.where(g >= 0, 2, jnp.where(s == 0, 1, 0)), jnp.where(s < n_late, 2, 3), rest, 0)
        return 0

    whole_tile(0)
    lax.fori_loop(0, n_groups + 1 + lag + n_late, slot_body, 0)

    def outs(n, _):
        out_tile(n)
        return 0

    lax.fori_loop(jnp.where(outs_beside, outs_before(n_groups) + n_groups - N_FIRST, 0), n_out_tiles, outs, 0)
    for n in range(2):
        sum_copy(n_out_tiles - 2 + n).wait()

    @pl.when(n_late == 0)
    def _():
        result(N_FIRST).wait()

    @pl.when(me < n_seq - 1)
    def _():
        hand_on(0).wait_send()


def rest_kernel(o_hbm, w_hbm, sum_hbm, out_hbm, o_buf, w_buf, sum_buf, out_buf, o_sem, w_sem, sum_sem, out_sem):
    n_rows, depth = o_buf.shape
    half, slots = n_rows // 2, sum_buf.shape[1] // 2
    n_parts = out_hbm.shape[1] // REST_COLUMNS

    def columns(n):
        return pl.ds(pl.multiple_of(n * REST_COLUMNS, REST_COLUMNS), REST_COLUMNS)

    def o_copy(i):
        rows = pl.ds(i * half, half)
        return pltpu.make_async_copy(o_hbm.at[rows], o_buf.at[rows], o_sem.at[i])

    def w_copy(n):
        slot = lax.rem(n, 3)
        return pltpu.make_async_copy(w_hbm.at[pl.ds(w_hbm.shape[0] - depth, depth), columns(n)], w_buf.at[slot], w_sem.at[slot])

    def sum_copy(n, i):
        slot, part = lax.rem(n, 3), pl.ds(i * slots, slots)
        return pltpu.make_async_copy(sum_hbm.at[part, :, :, columns(n)], sum_buf.at[slot, part], sum_sem.at[slot, i])

    def out_copy(n, i):
        slot, rows = lax.rem(n, 2), pl.ds(i * half, half)
        return pltpu.make_async_copy(out_buf.at[slot, rows], out_hbm.at[rows, columns(n)], out_sem.at[slot, i])

    def start(n):
        w_copy(n).start()
        for i in range(2):
            sum_copy(n, i).start()

    def product(n, i):
        rows = pl.ds(i * half, half)
        so_far = sum_buf[lax.rem(n, 3), pl.ds(i * slots, slots)].reshape(half, REST_COLUMNS)
        part = jnp.dot(o_buf[rows, :], w_buf[lax.rem(n, 3)], preferred_element_type=f32)
        out_buf[lax.rem(n, 2), rows, :] = (part + so_far).astype(bf16)

    first = jnp.int32(0)
    w_copy(first).start()
    for i in range(2):
        o_copy(i).start()
        sum_copy(first, i).start()
    w_copy(first).wait()
    for i in range(2):
        o_copy(i).wait()
        sum_copy(first, i).wait()
        if i == 1:
            start(first + 1)
        product(first, i)
        out_copy(first, i).start()

    def part(n, _):
        @pl.when((n >= 2) & (n + 1 < n_parts))
        def _():
            start(n + 1)

        @pl.when(n >= 2)
        def _():
            for i in range(2):
                out_copy(n - 2, i).wait()

        w_copy(n).wait()
        for i in range(2):
            sum_copy(n, i).wait()
        for i in range(2):
            product(n, i)
        for i in range(2):
            out_copy(n, i).start()
        return 0

    start(first + 2)
    lax.fori_loop(1, n_parts, part, 0)
    for n in range(n_parts - 2, n_parts):
        for i in range(2):
            out_copy(n, i).wait()


def solution(mesh):
    n_seq = mesh.shape["seq"]

    def per_device(tokens, theta_q, theta_k, theta_v, w_out, w_init, inner_lr):
        n_batch, tok_dev, width_d = tokens.shape
        n_heads, head_dim, _ = w_init.shape
        n_groups = n_heads // HEADS_PER_GROUP
        n_rows, width = n_batch * tok_dev, n_heads * head_dim
        flat = tokens.reshape(n_rows, width_d)
        hbm, smem = pl.BlockSpec(memory_space=pl.ANY), pl.BlockSpec(memory_space=pltpu.SMEM)
        sum_slots = n_rows // (n_batch * head_dim)
        o, first_sum = pl.pallas_call(
            functools.partial(fused_kernel, n_seq, n_batch, tok_dev, n_groups),
            out_shape=(jax.ShapeDtypeStruct((n_batch, tok_dev, width - 256 * N_FIRST), bf16), jax.ShapeDtypeStruct((sum_slots, n_batch, head_dim, width_d), f32)),
            in_specs=[hbm] * 6 + [smem], out_specs=(hbm, hbm),
            scratch_shapes=[pltpu.VMEM((n_rows, width_d), bf16), pltpu.VMEM((3, n_groups, n_batch, tok_dev, 256), bf16),
                            pltpu.VMEM((2, width_d, 256), bf16), pltpu.VMEM((n_rows, 256), bf16), pltpu.VMEM((n_batch, tok_dev, 256), bf16),
                            pltpu.VMEM((n_groups + max(0, 2 * sum_slots - N_FIRST), n_batch, head_dim, 4 * head_dim), f32),
                            pltpu.VMEM((n_batch, head_dim, 4 * head_dim), f32), pltpu.VMEM((n_batch, head_dim, 4 * head_dim), f32),
                            pltpu.VMEM((HEADS_PER_GROUP, head_dim, head_dim), f32),
                            pltpu.SemaphoreType.DMA((2,)), pltpu.SemaphoreType.DMA((2,)), pltpu.SemaphoreType.DMA, pltpu.SemaphoreType.DMA((2,)),
                            pltpu.SemaphoreType.DMA, pltpu.SemaphoreType.DMA, pltpu.SemaphoreType.DMA((n_groups,))],
            compiler_params=pltpu.CompilerParams(collective_id=0, has_side_effects=True, vmem_limit_bytes=67043328),
            name="fused",
        )(flat, theta_k, theta_v, theta_q, w_out, w_init, inner_lr)
        depth = width - 256 * N_FIRST
        result = pl.pallas_call(
            rest_kernel,
            out_shape=jax.ShapeDtypeStruct((n_rows, width_d), bf16),
            in_specs=[hbm] * 3, out_specs=hbm,
            scratch_shapes=[pltpu.VMEM((n_rows, depth), bf16), pltpu.VMEM((3, depth, REST_COLUMNS), bf16),
                            pltpu.VMEM((3, sum_slots, n_batch, head_dim, REST_COLUMNS), f32), pltpu.VMEM((2, n_rows, REST_COLUMNS), bf16),
                            pltpu.SemaphoreType.DMA((2,)), pltpu.SemaphoreType.DMA((3,)), pltpu.SemaphoreType.DMA((3, 2)), pltpu.SemaphoreType.DMA((2, 2))],
            compiler_params=pltpu.CompilerParams(vmem_limit_bytes=67043328),
            name="rest",
        )(o.reshape(n_rows, depth), w_out, first_sum)
        return result.reshape(n_batch, tok_dev, width_d)

    tok_spec = P("data", "seq", None)
    return jax.shard_map(per_device, mesh=mesh, in_specs=(tok_spec, P(), P(), P(), P(), P(), P()), out_specs=tok_spec, check_vma=False)
```

```python
import functools

import jax
import jax.numpy as jnp
from jax import lax
from jax.experimental import pallas as pl
from jax.experimental.pallas import tpu as pltpu
from jax.sharding import PartitionSpec as P

MINI_BATCH = 16
HEADS_PER_GROUP = 4
SCHEDULE = ((0, 7, (0, 0, 0, 0, 0)), (1, 6, (0, 0, 0, 0, 0)), (3, 4, (0, 0, 0, 0, 0)), (3, 1, (0, 0, 0, 0, 0)),
            (4, 0, (0, 3, 3, 3, 3)), (4, 0, (0, 3, 3, 3, 3)), (5, 0, (3, 6, 6, 6, 6)), (5, 0, (4, 7, 7, 7, 7)))
N_FIRST = 7
REST_COLUMNS = 512
bf16, f32 = jnp.bfloat16, jnp.float32


def split3(x):
    a = x.astype(bf16)
    rest = x - a.astype(f32)
    b = rest.astype(bf16)
    return a, b, (rest - b.astype(f32)).astype(bf16)


def per_head_rows(x):
    rows = []
    for half in range(2):
        y = x[:, :, half * 128:(half + 1) * 128]
        turned, low = pltpu.roll(y, 64, 2), low_lanes(y.shape)
        rows += [jnp.where(low, y, turned), jnp.where(low, turned, y)]
    return rows


def low_lanes(shape):
    return lax.broadcasted_iota(jnp.int32, shape, 2) < 64


def under(rows):
    n, t, width = rows[0].shape
    return jnp.concatenate([r.reshape(n, 1, t, width) for r in rows], axis=1).reshape(n, t * len(rows), width)


def own_columns(z, first):
    a, b, c, d = (z[:, first + i * MINI_BATCH:first + (i + 1) * MINI_BATCH, (i // 2) * 128:(i // 2 + 1) * 128] for i in range(4))
    low = low_lanes(a.shape)
    return jnp.concatenate([jnp.where(low, a, b), jnp.where(low, c, d)], axis=2)


def times_w(rows, w):
    m = under(rows)
    return jnp.concatenate([m, m], axis=2), jnp.concatenate([*split3(w), jnp.zeros(w.shape, bf16)], axis=1)


def k_transposed_times(k_rows, r):
    zero = jnp.zeros((*r.shape[:2], 128), bf16)
    low = low_lanes(zero.shape)
    rows = []
    for part in split3(r):
        a, b = part[:, :, :128], part[:, :, 128:]
        rows += [jnp.concatenate(pair, axis=2) for pair in (
            (jnp.where(low, a, zero), zero), (jnp.where(low, zero, a), zero), (zero, jnp.where(low, b, zero)), (zero, jnp.where(low, zero, b)))]
    rhs = jnp.concatenate([under(rows), jnp.zeros((r.shape[0], 4 * MINI_BATCH, 256), bf16)], axis=1)
    twice = under(k_rows + k_rows)
    turned = [twice[i].T[:64] for i in range(r.shape[0])]
    return [jnp.concatenate([t, t], axis=1) for t in turned], rhs


def fused_kernel(n_seq, n_batch, tok_dev, n_groups, x_hbm, theta_k_hbm, theta_v_hbm, theta_q_hbm, w_out_hbm, w_init_hbm, lr_ref, o_hbm, sum_hbm,
                 x_buf, kvq_buf, theta_buf, tile_buf, o_buf, w_buf, w_now, w_send, init_buf, x_sem, theta_sem, out_sem, sum_sem, init_sem, send_sem, recv_sem):
    me = lax.axis_index("seq")
    lag, n_late = jnp.int32(0), jnp.int32(0)
    for place, (ahead, late, _) in enumerate(SCHEDULE):
        lag = jnp.where(me == place, ahead, lag)
        n_late = jnp.where(me == place, late, n_late)

    outs_beside = (n_late == 0) & (lag + 1 + N_FIRST >= n_groups)

    def outs_before(g):
        n = jnp.int32(0)
        for place, (_, _, counts) in enumerate(SCHEDULE):
            for i, count in enumerate(counts):
                n = jnp.where((me == place) & (g >= N_FIRST + i), count, n)
        return n

    n_tiles = 3 * n_groups
    n_out_tiles = sum_hbm.shape[-1] // 256
    w_first = w_buf.shape[0] - n_groups
    first_depth = N_FIRST * 256
    n_rows = n_batch * tok_dev
    n_steps = tok_dev // MINI_BATCH
    chunk = n_rows // n_steps
    depth = x_buf.shape[1]
    thetas = (theta_k_hbm, theta_v_hbm, theta_q_hbm)
    barrier = pltpu.get_barrier_semaphore()

    def columns(g):
        return pl.ds(pl.multiple_of(g * 256, 256), 256)

    def tile_at(c):
        early, body = 2 * n_late, c - 2 * n_late
        kind = jnp.where(c < early, lax.rem(c, 2), jnp.where(c < n_tiles - n_late, lax.rem(body, 3), 2))
        g = jnp.where(c < early, c // 2, jnp.where(c < n_tiles - n_late, n_late + body // 3, c - (n_tiles - n_late)))
        return kind, g

    def start_theta(c):
        kind, g = tile_at(c)
        for i in range(3):
            @pl.when((kind == i) & (c < n_tiles))
            def _():
                pltpu.make_async_copy(thetas[i].at[:, columns(g)], theta_buf.at[lax.rem(c, 2)], theta_sem.at[lax.rem(c, 2)]).start()

        @pl.when((c >= n_tiles) & (c < n_tiles + n_out_tiles))
        def _():
            w_out_copy(c - n_tiles, lax.rem(c, 2)).start()

    def w_out_copy(n, slot):
        return pltpu.make_async_copy(w_out_hbm.at[pl.ds(0, first_depth), columns(n)], theta_buf.at[slot, pl.ds(0, first_depth)], theta_sem.at[slot])

    def wait_theta(c):
        slot = lax.rem(c, 2)
        pltpu.make_async_copy(theta_k_hbm.at[:, pl.ds(0, 256)], theta_buf.at[slot], theta_sem.at[slot]).wait()

    def result(g):
        return pltpu.make_async_copy(o_buf, o_hbm.at[:, :, columns(g - N_FIRST)], out_sem)

    def sum_copy(n):
        part = lax.rem(n, 2)
        return pltpu.make_async_copy(w_buf.at[pl.ds(part * sum_slots, sum_slots)], sum_hbm.at[:, :, :, columns(n)], sum_sem.at[part])

    def hand_on(g):
        return pltpu.make_async_remote_copy(w_send, w_buf.at[w_first + g], send_sem, recv_sem.at[g],
                                            device_id={"seq": lax.rem(me + 1, n_seq)}, device_id_type=pl.DeviceIdType.MESH)

    sum_slots = sum_hbm.shape[0]

    def first_w(g):
        return pltpu.make_async_copy(w_init_hbm.at[pl.ds(g * HEADS_PER_GROUP, HEADS_PER_GROUP)], init_buf, init_sem)

    def x_copy(i):
        rows = pl.ds(i * (n_rows // 2), n_rows // 2)
        return pltpu.make_async_copy(x_hbm.at[rows], x_buf.at[rows], x_sem.at[i])

    start_theta(jnp.int32(0))
    for i in range(2):
        x_copy(i).start()

    @pl.when(me == 0)
    def _():
        first_w(0).start()

    for peer in (lax.rem(me + 1, n_seq), lax.rem(me + n_seq - 1, n_seq)):
        pl.semaphore_signal(barrier, inc=1, device_id={"seq": peer}, device_id_type=pl.DeviceIdType.MESH)

    head = lax.broadcasted_iota(jnp.int32, (1, 256), 1) // 64

    half = n_batch // 2

    def tokens(kind, g, units, j):
        return kvq_buf[kind, g, units, pl.ds(j * MINI_BATCH, MINI_BATCH), :]

    def chain_step(g, eta, j, now, before, w_start=None):
        k_rows = z = None
        if now is not None:
            k_rows = per_head_rows(tokens(0, g, now, j)) if j < n_steps else []
            rows = k_rows + (per_head_rows(tokens(2, g, now, j - 1)) if j > 0 else [])
            lhs, rhs = times_w(rows, w_now[now] if w_start is None or j > 0 else w_start[now])
        if before is not None:
            units, step, keys, inputs = before
            r = (inputs - tokens(1, g, units, step).astype(f32)) * eta
            lhs_u, rhs_u = k_transposed_times(keys, r)
        prod, change = [], []
        for i in range(half):
            if now is not None:
                prod.append(jnp.dot(lhs[i], rhs[i], preferred_element_type=f32))
            if before is not None:
                change.append(jnp.dot(lhs_u[i], rhs_u[i], preferred_element_type=f32))
        if now is not None:
            prod = jnp.stack(prod)
            if j < n_steps:
                z = own_columns(prod, 0)
            if j > 0:
                o_buf[now, pl.ds((j - 1) * MINI_BATCH, MINI_BATCH), :] = own_columns(prod, 4 * MINI_BATCH if j < n_steps else 0).astype(bf16)
        if before is not None:
            w_now[units] = (w_now[units] if w_start is None or step > 0 else w_start[units]) - jnp.stack(change)
        return k_rows, z

    def chain(g, eta, fill, w_start=None):
        one, two = pl.ds(0, half), pl.ds(half, half)
        open_two = None
        for j in range(n_steps):
            put = fill(j)
            open_one = (one, j, *chain_step(g, eta, j, one, open_two, w_start))
            open_two = (two, j, *chain_step(g, eta, j, two, open_one, w_start))
            put()
        chain_step(g, eta, n_steps, None, open_two)

    def whole_tile(c, group=None):
        kind, g = tile_at(c)
        slot = lax.rem(c, 2)
        wait_theta(c)
        start_theta(c + 1)
        for i in range(2):
            rows = pl.ds(i * (n_rows // 2), n_rows // 2)
            if isinstance(c, int):
                x_copy(i).wait()
            pieces = [pl.ds(i * (n_rows // 2) + p * (n_rows // 4), n_rows // 4) for p in range(2)] if isinstance(c, int) else [rows]
            part = jnp.concatenate([jnp.dot(x_buf[p, :], theta_buf[slot], preferred_element_type=f32).astype(bf16) for p in pieces], axis=0)
            if group is not None and i == 0:
                last_results(group)
                before = tile_at(c - 1)
                kvq_buf[before[0], before[1]] = tile_buf[...].reshape(n_batch, tok_dev, 256)
            kvq_buf[kind, g, pl.ds(i * half, half)] = part.reshape(half, tok_dev, 256)

    def out_tile(n):
        c = n_tiles + n
        slot = lax.rem(c, 2)
        w_out_copy(n, slot).wait()
        start_theta(c + 1)

        @pl.when(n >= 2)
        def _():
            sum_copy(n - 2).wait()

        for i in range(2):
            rows = pl.ds(i * (n_rows // 2), n_rows // 2)
            lhs = jnp.concatenate([kvq_buf[2, g, pl.ds(i * half, half)].reshape(n_rows // 2, 256) for g in range(N_FIRST)], axis=1)
            part = jnp.dot(lhs, theta_buf[slot, :first_depth, :], preferred_element_type=f32)
            w_buf[pl.ds(lax.rem(n, 2) * sum_slots + i * (sum_slots // 2), sum_slots // 2)] = part.reshape(sum_slots // 2, *w_buf.shape[1:])
        sum_copy(n).start()

    def inner(g, first_time, c, n=None):
        slot = lax.rem(jnp.where(c < n_tiles, c, c - 1), 2) if n is None else lax.rem(c, 2)

        if n is None:
            @pl.when(c < n_tiles)
            def _():
                wait_theta(c)
                start_theta(c + 1)
        else:
            w_out_copy(n, slot).wait()
            start_theta(c + 1)

            @pl.when(n >= 2)
            def _():
                sum_copy(n - 2).wait()

        @pl.when((me == 0) & first_time)
        def _():
            first_w(g).wait()
            start = jnp.concatenate([init_buf[h] for h in range(HEADS_PER_GROUP)], axis=1)
            for b in range(n_batch):
                w_buf[w_first + g, b] = start

        @pl.when((me == 0) & first_time & (g + 1 < n_groups))
        def _():
            first_w(g + 1).start()

        @pl.when((me > 0) & first_time)
        def _():
            hand_on(g).wait_recv()

        @pl.when(jnp.where(first_time, g > N_FIRST, g == 0))
        def _():
            result(N_FIRST).wait()

        eta = jnp.zeros((1, 256), f32)
        for h in range(HEADS_PER_GROUP):
            eta = jnp.where(head == h, (2.0 / MINI_BATCH) * lr_ref[g * HEADS_PER_GROUP + h], eta)

        if n is not None:
            w_now[...] = w_buf[w_first + g]
            theta_buf[slot, first_depth:, :] = jnp.zeros((depth - first_depth, 256), bf16)

        if n is None:
            def fill(j):
                part = pl.ds(j * chunk, chunk)
                tile_part = jnp.dot(x_buf[part, :], theta_buf[slot], preferred_element_type=f32)

                def put():
                    tile_buf[part, :] = tile_part.astype(bf16)
                return put
        else:
            def fill(j):
                b, first = j * chunk // tok_dev, j * chunk % tok_dev
                lhs = jnp.concatenate([kvq_buf[2, i, b, pl.ds(first, chunk), :] for i in range(N_FIRST)], axis=1)
                lhs = jnp.concatenate([lhs, x_buf[pl.ds(j * chunk, chunk), :depth - first_depth]], axis=1)
                part = jnp.dot(lhs, theta_buf[slot], preferred_element_type=f32)
                rows = n_batch * w_buf.shape[2]
                at, within = j * chunk // rows, j * chunk % rows // w_buf.shape[2]

                def put():
                    w_buf[lax.rem(n, 2) * sum_slots + at, pl.ds(within, chunk // w_buf.shape[2])] = part.reshape(chunk // w_buf.shape[2], *w_buf.shape[2:])
                return put

        chain(g, eta, fill, w_buf.at[w_first + g] if n is None else None)

        @pl.when((me < n_seq - 1) & first_time & (g > 0))
        def _():
            hand_on(0).wait_send()

        @pl.when((me < n_seq - 1) & first_time)
        def _():
            w_send[...] = w_now[...]
            hand_on(g).start()

        if n is not None:
            sum_copy(n).start()

    def last_results(g):
        for units in (pl.ds(0, half), pl.ds(half, half)):
            chain_step(g, None, n_steps, units, None)
        kvq_buf[2, g] = o_buf[...]

    def send_result(g, first_time):
        @pl.when((g >= N_FIRST) & (jnp.logical_not(first_time) | (g >= n_late)))
        def _():
            result(g).start()

    def slot_body(s, _):
        @pl.when(s == 1)
        def _():
            pl.semaphore_wait(barrier, 2)

        first_time = s <= n_groups + lag
        g = jnp.where(first_time, s - 1 - lag, s - (n_groups + 1 + lag))
        fresh = s < n_groups
        c = jnp.where(fresh, 2 * s + jnp.maximum(s - n_late, 0), jnp.minimum(n_tiles - n_late + s - n_groups, n_tiles))
        beside_out = outs_beside & first_time & (g >= N_FIRST)
        n_out = jnp.where(beside_out, outs_before(g) + g - N_FIRST, 0)

        def outs(n, _):
            out_tile(n)
            return 0

        lax.fori_loop(jnp.where(beside_out, outs_before(g - 1) + g - N_FIRST, 0), n_out, outs, 0)

        @pl.when((g >= 0) & jnp.logical_not(beside_out))
        def _():
            inner(g, first_time, c)

        @pl.when(beside_out)
        def _():
            inner(g, first_time, n_tiles + n_out, n_out)

        @pl.when((g >= 0) & fresh)
        def _():
            whole_tile(c + 1, g)
            send_result(g, first_time)

        @pl.when((g >= 0) & jnp.logical_not(fresh))
        def _():
            last_results(g)
            send_result(g, first_time)

            @pl.when(c < n_tiles)
            def _():
                kind, of = tile_at(c)
                kvq_buf[kind, of] = tile_buf[...].reshape(n_batch, tok_dev, 256)

        def rest(i, _):
            whole_tile(c + i)
            return 0

        @pl.when(fresh)
        def _():
            lax.fori_loop(jnp.where(g >= 0, 2, jnp.where(s == 0, 1, 0)), jnp.where(s < n_late, 2, 3), rest, 0)
        return 0

    whole_tile(0)
    lax.fori_loop(0, n_groups + 1 + lag + n_late, slot_body, 0)

    def outs(n, _):
        out_tile(n)
        return 0

    lax.fori_loop(jnp.where(outs_beside, outs_before(n_groups) + n_groups - N_FIRST, 0), n_out_tiles, outs, 0)
    for n in range(2):
        sum_copy(n_out_tiles - 2 + n).wait()

    @pl.when(n_late == 0)
    def _():
        result(N_FIRST).wait()

    @pl.when(me < n_seq - 1)
    def _():
        hand_on(0).wait_send()


def rest_kernel(o_hbm, w_hbm, sum_hbm, out_hbm, o_buf, w_buf, sum_buf, out_buf, o_sem, w_sem, sum_sem, out_sem):
    n_rows, depth = o_buf.shape
    pieces = sum_buf.shape[1]
    piece, half = n_rows // pieces, n_rows // 2
    n_parts = out_hbm.shape[1] // REST_COLUMNS

    def columns(n):
        return pl.ds(pl.multiple_of(n * REST_COLUMNS, REST_COLUMNS), REST_COLUMNS)

    def o_copy(i):
        rows = pl.ds(i * piece, piece)
        return pltpu.make_async_copy(o_hbm.at[rows], o_buf.at[rows], o_sem.at[i])

    def w_copy(n, i):
        slot, rows = lax.rem(n, 3), depth // 2
        return pltpu.make_async_copy(w_hbm.at[pl.ds(w_hbm.shape[0] - depth + i * rows, rows), columns(n)],
                                     w_buf.at[slot, pl.ds(i * rows, rows)], w_sem.at[slot, i])

    def sum_copy(n, i):
        slot = lax.rem(n, 3)
        return pltpu.make_async_copy(sum_hbm.at[i, :, :, columns(n)], sum_buf.at[slot, i], sum_sem.at[slot, i])

    def out_copy(n, i):
        slot, rows = lax.rem(n, 2), pl.ds(i * piece, piece)
        return pltpu.make_async_copy(out_buf.at[slot, rows], out_hbm.at[rows, columns(n)], out_sem.at[slot, i])

    def start(n):
        for i in range(2):
            w_copy(n, i).start()
        for i in range(pieces):
            sum_copy(n, i).start()

    def product(n, i):
        rows = pl.ds(i * half, half)
        so_far = sum_buf[lax.rem(n, 3), pl.ds(i * (pieces // 2), pieces // 2)].reshape(half, REST_COLUMNS)
        part = jnp.dot(o_buf[rows, :], w_buf[lax.rem(n, 3)], preferred_element_type=f32)
        out_buf[lax.rem(n, 2), rows, :] = (part + so_far).astype(bf16)

    first = jnp.int32(0)
    for i in range(2):
        w_copy(first, i).start()
    for i in range(pieces):
        o_copy(i).start()
        sum_copy(first, i).start()
    for i in range(2):
        w_copy(first, i).wait()
    for i in range(pieces):
        o_copy(i).wait()
        sum_copy(first, i).wait()
        if i == pieces // 2 - 1:
            start(first + 1)
            product(first, 0)
    start(first + 2)
    product(first, 1)
    for i in range(pieces):
        out_copy(first, i).start()

    def part(n, _):
        @pl.when(n + 2 < n_parts)
        def _():
            start(n + 2)

        @pl.when(n >= 2)
        def _():
            for i in range(pieces):
                out_copy(n - 2, i).wait()

        for i in range(2):
            w_copy(n, i).wait()
        for i in range(pieces):
            sum_copy(n, i).wait()
        for i in range(2):
            product(n, i)
        for i in range(pieces):
            out_copy(n, i).start()
        return 0

    lax.fori_loop(1, n_parts, part, 0)
    for n in range(n_parts - 2, n_parts):
        for i in range(pieces):
            out_copy(n, i).wait()


def solution(mesh):
    n_seq = mesh.shape["seq"]

    def per_device(tokens, theta_q, theta_k, theta_v, w_out, w_init, inner_lr):
        n_batch, tok_dev, width_d = tokens.shape
        n_heads, head_dim, _ = w_init.shape
        n_groups = n_heads // HEADS_PER_GROUP
        n_rows, width = n_batch * tok_dev, n_heads * head_dim
        flat = tokens.reshape(n_rows, width_d)
        hbm, smem = pl.BlockSpec(memory_space=pl.ANY), pl.BlockSpec(memory_space=pltpu.SMEM)
        sum_slots = n_rows // (n_batch * head_dim)
        o, first_sum = pl.pallas_call(
            functools.partial(fused_kernel, n_seq, n_batch, tok_dev, n_groups),
            out_shape=(jax.ShapeDtypeStruct((n_batch, tok_dev, width - 256 * N_FIRST), bf16), jax.ShapeDtypeStruct((sum_slots, n_batch, head_dim, width_d), f32)),
            in_specs=[hbm] * 6 + [smem], out_specs=(hbm, hbm),
            scratch_shapes=[pltpu.VMEM((n_rows, width_d), bf16), pltpu.VMEM((3, n_groups, n_batch, tok_dev, 256), bf16),
                            pltpu.VMEM((2, width_d, 256), bf16), pltpu.VMEM((n_rows, 256), bf16), pltpu.VMEM((n_batch, tok_dev, 256), bf16),
                            pltpu.VMEM((n_groups + max(0, 2 * sum_slots - N_FIRST), n_batch, head_dim, 4 * head_dim), f32),
                            pltpu.VMEM((n_batch, head_dim, 4 * head_dim), f32), pltpu.VMEM((n_batch, head_dim, 4 * head_dim), f32),
                            pltpu.VMEM((HEADS_PER_GROUP, head_dim, head_dim), f32),
                            pltpu.SemaphoreType.DMA((2,)), pltpu.SemaphoreType.DMA((2,)), pltpu.SemaphoreType.DMA, pltpu.SemaphoreType.DMA((2,)),
                            pltpu.SemaphoreType.DMA, pltpu.SemaphoreType.DMA, pltpu.SemaphoreType.DMA((n_groups,))],
            compiler_params=pltpu.CompilerParams(collective_id=0, has_side_effects=True, vmem_limit_bytes=67043328),
            name="fused",
        )(flat, theta_k, theta_v, theta_q, w_out, w_init, inner_lr)
        depth = width - 256 * N_FIRST
        result = pl.pallas_call(
            rest_kernel,
            out_shape=jax.ShapeDtypeStruct((n_rows, width_d), bf16),
            in_specs=[hbm] * 3, out_specs=hbm,
            scratch_shapes=[pltpu.VMEM((n_rows, depth), bf16), pltpu.VMEM((3, depth, REST_COLUMNS), bf16),
                            pltpu.VMEM((3, sum_slots, n_batch, head_dim, REST_COLUMNS), f32), pltpu.VMEM((2, n_rows, REST_COLUMNS), bf16),
                            pltpu.SemaphoreType.DMA((sum_slots,)), pltpu.SemaphoreType.DMA((3, 2)), pltpu.SemaphoreType.DMA((3, sum_slots)), pltpu.SemaphoreType.DMA((2, sum_slots))],
            compiler_params=pltpu.CompilerParams(vmem_limit_bytes=67043328),
            name="rest",
        )(o.reshape(n_rows, depth), w_out, first_sum)
        return result.reshape(n_batch, tok_dev, width_d)

    tok_spec = P("data", "seq", None)
    return jax.shard_map(per_device, mesh=mesh, in_specs=(tok_spec, P(), P(), P(), P(), P(), P()), out_specs=tok_spec, check_vma=False)
```

```python
import functools

import jax
import jax.numpy as jnp
from jax import lax
from jax.experimental import pallas as pl
from jax.experimental.pallas import tpu as pltpu
from jax.sharding import PartitionSpec as P

MINI_BATCH = 16
HEADS_PER_GROUP = 4
SCHEDULE = ((0, 7, (0, 0, 0, 0, 0)), (1, 6, (0, 0, 0, 0, 0)), (3, 4, (0, 0, 0, 0, 0)), (3, 1, (0, 0, 0, 0, 0)),
            (4, 0, (0, 3, 3, 3, 3)), (4, 0, (0, 3, 3, 3, 3)), (5, 0, (3, 6, 6, 6, 6)), (5, 0, (4, 7, 7, 7, 7)))
N_FIRST = 7
REST_COLUMNS = 512
bf16, f32 = jnp.bfloat16, jnp.float32


def split3(x):
    a = x.astype(bf16)
    rest = x - a.astype(f32)
    b = rest.astype(bf16)
    return a, b, (rest - b.astype(f32)).astype(bf16)


def per_head_rows(x):
    rows = []
    for half in range(2):
        y = x[:, :, half * 128:(half + 1) * 128]
        turned, low = pltpu.roll(y, 64, 2), low_lanes(y.shape)
        rows += [jnp.where(low, y, turned), jnp.where(low, turned, y)]
    return rows


def low_lanes(shape):
    return lax.broadcasted_iota(jnp.int32, shape, 2) < 64


def under(rows):
    n, t, width = rows[0].shape
    return jnp.concatenate([r.reshape(n, 1, t, width) for r in rows], axis=1).reshape(n, t * len(rows), width)


def own_columns(z, first):
    a, b, c, d = (z[:, first + i * MINI_BATCH:first + (i + 1) * MINI_BATCH, (i // 2) * 128:(i // 2 + 1) * 128] for i in range(4))
    low = low_lanes(a.shape)
    return jnp.concatenate([jnp.where(low, a, b), jnp.where(low, c, d)], axis=2)


def times_w(rows, w):
    m = under(rows)
    return jnp.concatenate([m, m], axis=2), jnp.concatenate([*split3(w), jnp.zeros(w.shape, bf16)], axis=1)


def k_transposed_times(k_rows, r):
    zero = jnp.zeros((*r.shape[:2], 128), bf16)
    low = low_lanes(zero.shape)
    rows = []
    for part in split3(r):
        a, b = part[:, :, :128], part[:, :, 128:]
        rows += [jnp.concatenate(pair, axis=2) for pair in (
            (jnp.where(low, a, zero), zero), (jnp.where(low, zero, a), zero), (zero, jnp.where(low, b, zero)), (zero, jnp.where(low, zero, b)))]
    rhs = jnp.concatenate([under(rows), jnp.zeros((r.shape[0], 4 * MINI_BATCH, 256), bf16)], axis=1)
    twice = under(k_rows + k_rows)
    turned = [twice[i].T[:64] for i in range(r.shape[0])]
    return [jnp.concatenate([t, t], axis=1) for t in turned], rhs


def fused_kernel(n_seq, n_batch, tok_dev, n_groups, x_hbm, theta_k_hbm, theta_v_hbm, theta_q_hbm, w_out_hbm, w_init_hbm, lr_ref, o_hbm, sum_hbm,
                 x_buf, kvq_buf, theta_buf, tile_buf, o_buf, w_buf, w_now, w_send, init_buf, x_sem, theta_sem, out_sem, sum_sem, init_sem, send_sem, recv_sem):
    me = lax.axis_index("seq")
    lag, n_late = jnp.int32(0), jnp.int32(0)
    for place, (ahead, late, _) in enumerate(SCHEDULE):
        lag = jnp.where(me == place, ahead, lag)
        n_late = jnp.where(me == place, late, n_late)

    outs_beside = (n_late == 0) & (lag + 1 + N_FIRST >= n_groups)

    def outs_before(g):
        n = jnp.int32(0)
        for place, (_, _, counts) in enumerate(SCHEDULE):
            for i, count in enumerate(counts):
                n = jnp.where((me == place) & (g >= N_FIRST + i), count, n)
        return n

    n_tiles = 3 * n_groups
    n_out_tiles = sum_hbm.shape[-1] // 256
    w_first = w_buf.shape[0] - n_groups
    first_depth = N_FIRST * 256
    n_rows = n_batch * tok_dev
    n_steps = tok_dev // MINI_BATCH
    chunk = n_rows // n_steps
    depth = x_buf.shape[1]
    thetas = (theta_k_hbm, theta_v_hbm, theta_q_hbm)
    barrier = pltpu.get_barrier_semaphore()

    def columns(g):
        return pl.ds(pl.multiple_of(g * 256, 256), 256)

    def tile_at(c):
        early, body = 2 * n_late, c - 2 * n_late
        kind = jnp.where(c < early, lax.rem(c, 2), jnp.where(c < n_tiles - n_late, lax.rem(body, 3), 2))
        g = jnp.where(c < early, c // 2, jnp.where(c < n_tiles - n_late, n_late + body // 3, c - (n_tiles - n_late)))
        return kind, g

    def start_theta(c):
        kind, g = tile_at(c)
        for i in range(3):
            @pl.when((kind == i) & (c < n_tiles))
            def _():
                pltpu.make_async_copy(thetas[i].at[:, columns(g)], theta_buf.at[lax.rem(c, 2)], theta_sem.at[lax.rem(c, 2)]).start()

        @pl.when((c >= n_tiles) & (c < n_tiles + n_out_tiles))
        def _():
            w_out_copy(c - n_tiles, lax.rem(c, 2)).start()

    def w_out_copy(n, slot):
        return pltpu.make_async_copy(w_out_hbm.at[pl.ds(0, first_depth), columns(n)], theta_buf.at[slot, pl.ds(0, first_depth)], theta_sem.at[slot])

    def wait_theta(c):
        slot = lax.rem(c, 2)
        pltpu.make_async_copy(theta_k_hbm.at[:, pl.ds(0, 256)], theta_buf.at[slot], theta_sem.at[slot]).wait()

    def result(g):
        return pltpu.make_async_copy(o_buf, o_hbm.at[:, :, columns(g - N_FIRST)], out_sem)

    def sum_copy(n):
        part = lax.rem(n, 2)
        return pltpu.make_async_copy(w_buf.at[pl.ds(part * sum_slots, sum_slots)], sum_hbm.at[:, :, :, columns(n)], sum_sem.at[part])

    def hand_on(g):
        return pltpu.make_async_remote_copy(w_send, w_buf.at[w_first + g], send_sem, recv_sem.at[g],
                                            device_id={"seq": lax.rem(me + 1, n_seq)}, device_id_type=pl.DeviceIdType.MESH)

    sum_slots = sum_hbm.shape[0]

    def first_w(g):
        return pltpu.make_async_copy(w_init_hbm.at[pl.ds(g * HEADS_PER_GROUP, HEADS_PER_GROUP)], init_buf, init_sem)

    def x_copy(i):
        rows = pl.ds(i * (n_rows // 2), n_rows // 2)
        return pltpu.make_async_copy(x_hbm.at[rows], x_buf.at[rows], x_sem.at[i])

    start_theta(jnp.int32(0))
    for i in range(2):
        x_copy(i).start()

    @pl.when(me == 0)
    def _():
        first_w(0).start()

    for peer in (lax.rem(me + 1, n_seq), lax.rem(me + n_seq - 1, n_seq)):
        pl.semaphore_signal(barrier, inc=1, device_id={"seq": peer}, device_id_type=pl.DeviceIdType.MESH)

    head = lax.broadcasted_iota(jnp.int32, (1, 256), 1) // 64

    half = n_batch // 2

    def tokens(kind, g, units, j):
        return kvq_buf[kind, g, units, pl.ds(j * MINI_BATCH, MINI_BATCH), :]

    def chain_step(g, eta, j, now, before, w_start=None):
        k_rows = z = None
        if now is not None:
            k_rows = per_head_rows(tokens(0, g, now, j)) if j < n_steps else []
            rows = k_rows + (per_head_rows(tokens(2, g, now, j - 1)) if j > 0 else [])
            lhs, rhs = times_w(rows, w_now[now] if w_start is None or j > 0 else w_start[now])
        if before is not None:
            units, step, keys, inputs = before
            r = (inputs - tokens(1, g, units, step).astype(f32)) * eta
            lhs_u, rhs_u = k_transposed_times(keys, r)
        prod, change = [], []
        for i in range(half):
            if now is not None:
                prod.append(jnp.dot(lhs[i], rhs[i], preferred_element_type=f32))
            if before is not None:
                change.append(jnp.dot(lhs_u[i], rhs_u[i], preferred_element_type=f32))
        if now is not None:
            prod = jnp.stack(prod)
            if j < n_steps:
                z = own_columns(prod, 0)
            if j > 0:
                o_buf[now, pl.ds((j - 1) * MINI_BATCH, MINI_BATCH), :] = own_columns(prod, 4 * MINI_BATCH if j < n_steps else 0).astype(bf16)
        if before is not None:
            w_now[units] = (w_now[units] if w_start is None or step > 0 else w_start[units]) - jnp.stack(change)
        return k_rows, z

    def chain(g, eta, fill, w_start=None):
        one, two = pl.ds(0, half), pl.ds(half, half)
        open_two = None
        for j in range(n_steps):
            put = fill(j)
            open_one = (one, j, *chain_step(g, eta, j, one, open_two, w_start))
            open_two = (two, j, *chain_step(g, eta, j, two, open_one, w_start))
            put()
        chain_step(g, eta, n_steps, None, open_two)

    def whole_tile(c, group=None):
        kind, g = tile_at(c)
        slot = lax.rem(c, 2)
        wait_theta(c)
        start_theta(c + 1)
        for i in range(2):
            rows = pl.ds(i * (n_rows // 2), n_rows // 2)
            if isinstance(c, int):
                x_copy(i).wait()
            pieces = [pl.ds(i * (n_rows // 2) + p * (n_rows // 4), n_rows // 4) for p in range(2)] if isinstance(c, int) else [rows]
            part = jnp.concatenate([jnp.dot(x_buf[p, :], theta_buf[slot], preferred_element_type=f32).astype(bf16) for p in pieces], axis=0)
            if group is not None and i == 0:
                last_results(group)
                before = tile_at(c - 1)
                kvq_buf[before[0], before[1]] = tile_buf[...].reshape(n_batch, tok_dev, 256)
            kvq_buf[kind, g, pl.ds(i * half, half)] = part.reshape(half, tok_dev, 256)

    def out_tile(n):
        c = n_tiles + n
        slot = lax.rem(c, 2)
        w_out_copy(n, slot).wait()
        start_theta(c + 1)

        @pl.when(n >= 2)
        def _():
            sum_copy(n - 2).wait()

        for i in range(2):
            rows = pl.ds(i * (n_rows // 2), n_rows // 2)
            lhs = jnp.concatenate([kvq_buf[2, g, pl.ds(i * half, half)].reshape(n_rows // 2, 256) for g in range(N_FIRST)], axis=1)
            part = jnp.dot(lhs, theta_buf[slot, :first_depth, :], preferred_element_type=f32)
            w_buf[pl.ds(lax.rem(n, 2) * sum_slots + i * (sum_slots // 2), sum_slots // 2)] = part.reshape(sum_slots // 2, *w_buf.shape[1:])
        sum_copy(n).start()

    def inner(g, first_time, c, n=None):
        slot = lax.rem(jnp.where(c < n_tiles, c, c - 1), 2) if n is None else lax.rem(c, 2)

        if n is None:
            @pl.when(c < n_tiles)
            def _():
                wait_theta(c)
                start_theta(c + 1)
        else:
            w_out_copy(n, slot).wait()
            start_theta(c + 1)

            @pl.when(n >= 2)
            def _():
                sum_copy(n - 2).wait()

        @pl.when((me == 0) & first_time)
        def _():
            first_w(g).wait()
            start = jnp.concatenate([init_buf[h] for h in range(HEADS_PER_GROUP)], axis=1)
            for b in range(n_batch):
                w_buf[w_first + g, b] = start

        @pl.when((me == 0) & first_time & (g + 1 < n_groups))
        def _():
            first_w(g + 1).start()

        @pl.when((me > 0) & first_time)
        def _():
            hand_on(g).wait_recv()

        @pl.when(jnp.where(first_time, g > N_FIRST, g == 0))
        def _():
            result(N_FIRST).wait()

        eta = jnp.zeros((1, 256), f32)
        for h in range(HEADS_PER_GROUP):
            eta = jnp.where(head == h, (2.0 / MINI_BATCH) * lr_ref[g * HEADS_PER_GROUP + h], eta)

        if n is not None:
            w_now[...] = w_buf[w_first + g]
            theta_buf[slot, first_depth:, :] = jnp.zeros((depth - first_depth, 256), bf16)

        if n is None:
            def fill(j):
                part = pl.ds(j * chunk, chunk)
                tile_part = jnp.dot(x_buf[part, :], theta_buf[slot], preferred_element_type=f32)

                def put():
                    tile_buf[part, :] = tile_part.astype(bf16)
                return put
        else:
            def fill(j):
                b, first = j * chunk // tok_dev, j * chunk % tok_dev
                lhs = jnp.concatenate([kvq_buf[2, i, b, pl.ds(first, chunk), :] for i in range(N_FIRST)], axis=1)
                lhs = jnp.concatenate([lhs, x_buf[pl.ds(j * chunk, chunk), :depth - first_depth]], axis=1)
                part = jnp.dot(lhs, theta_buf[slot], preferred_element_type=f32)
                rows = n_batch * w_buf.shape[2]
                at, within = j * chunk // rows, j * chunk % rows // w_buf.shape[2]

                def put():
                    w_buf[lax.rem(n, 2) * sum_slots + at, pl.ds(within, chunk // w_buf.shape[2])] = part.reshape(chunk // w_buf.shape[2], *w_buf.shape[2:])
                return put

        chain(g, eta, fill, w_buf.at[w_first + g] if n is None else None)

        @pl.when((me < n_seq - 1) & first_time & (g > 0))
        def _():
            hand_on(0).wait_send()

        @pl.when((me < n_seq - 1) & first_time)
        def _():
            w_send[...] = w_now[...]
            hand_on(g).start()

        if n is not None:
            sum_copy(n).start()

    def last_results(g):
        for units in (pl.ds(0, half), pl.ds(half, half)):
            chain_step(g, None, n_steps, units, None)
        kvq_buf[2, g] = o_buf[...]

    def send_result(g, first_time):
        @pl.when((g >= N_FIRST) & (jnp.logical_not(first_time) | (g >= n_late)))
        def _():
            result(g).start()

    def slot_body(s, _):
        @pl.when(s == 1)
        def _():
            pl.semaphore_wait(barrier, 2)

        first_time = s <= n_groups + lag
        g = jnp.where(first_time, s - 1 - lag, s - (n_groups + 1 + lag))
        fresh = s < n_groups
        c = jnp.where(fresh, 2 * s + jnp.maximum(s - n_late, 0), jnp.minimum(n_tiles - n_late + s - n_groups, n_tiles))
        beside_out = outs_beside & first_time & (g >= N_FIRST)
        n_out = jnp.where(beside_out, outs_before(g) + g - N_FIRST, 0)

        def outs(n, _):
            out_tile(n)
            return 0

        lax.fori_loop(jnp.where(beside_out, outs_before(g - 1) + g - N_FIRST, 0), n_out, outs, 0)

        @pl.when((g >= 0) & jnp.logical_not(beside_out))
        def _():
            inner(g, first_time, c)

        @pl.when(beside_out)
        def _():
            inner(g, first_time, n_tiles + n_out, n_out)

        @pl.when((g >= 0) & fresh)
        def _():
            whole_tile(c + 1, g)
            send_result(g, first_time)

        @pl.when((g >= 0) & jnp.logical_not(fresh))
        def _():
            last_results(g)
            send_result(g, first_time)

            @pl.when(c < n_tiles)
            def _():
                kind, of = tile_at(c)
                kvq_buf[kind, of] = tile_buf[...].reshape(n_batch, tok_dev, 256)

        def rest(i, _):
            whole_tile(c + i)
            return 0

        @pl.when(fresh)
        def _():
            lax.fori_loop(jnp.where(g >= 0, 2, jnp.where(s == 0, 1, 0)), jnp.where(s < n_late, 2, 3), rest, 0)
        return 0

    whole_tile(0)
    lax.fori_loop(0, n_groups + 1 + lag + n_late, slot_body, 0)

    def outs(n, _):
        out_tile(n)
        return 0

    lax.fori_loop(jnp.where(outs_beside, outs_before(n_groups) + n_groups - N_FIRST, 0), n_out_tiles, outs, 0)
    for n in range(2):
        sum_copy(n_out_tiles - 2 + n).wait()

    @pl.when(n_late == 0)
    def _():
        result(N_FIRST).wait()

    @pl.when(me < n_seq - 1)
    def _():
        hand_on(0).wait_send()


def rest_kernel(o_hbm, w_hbm, sum_hbm, out_hbm, o_buf, w_buf, sum_buf, out_buf, o_sem, w_sem, sum_sem, out_sem):
    n_rows, depth = o_buf.shape
    pieces = sum_buf.shape[1]
    piece, half = n_rows // pieces, n_rows // 2
    n_parts = out_hbm.shape[1] // REST_COLUMNS

    def columns(n):
        return pl.ds(pl.multiple_of(n * REST_COLUMNS, REST_COLUMNS), REST_COLUMNS)

    def o_copy(i):
        rows = pl.ds(i * piece, piece)
        return pltpu.make_async_copy(o_hbm.at[rows], o_buf.at[rows], o_sem.at[i])

    def w_copy(n, i):
        slot, rows = lax.rem(n, 3), depth // 2
        return pltpu.make_async_copy(w_hbm.at[pl.ds(w_hbm.shape[0] - depth + i * rows, rows), columns(n)],
                                     w_buf.at[slot, pl.ds(i * rows, rows)], w_sem.at[slot, i])

    def sum_copy(n, i):
        slot = lax.rem(n, 3)
        return pltpu.make_async_copy(sum_hbm.at[i, :, :, columns(n)], sum_buf.at[slot, i], sum_sem.at[slot, i])

    def out_copy(n, i):
        slot, rows = lax.rem(n, 2), pl.ds(i * piece, piece)
        return pltpu.make_async_copy(out_buf.at[slot, rows], out_hbm.at[rows, columns(n)], out_sem.at[slot, i])

    def start(n):
        for i in range(2):
            w_copy(n, i).start()
        for i in range(pieces):
            sum_copy(n, i).start()

    def product(n, i):
        rows = pl.ds(i * half, half)
        so_far = sum_buf[lax.rem(n, 3), pl.ds(i * (pieces // 2), pieces // 2)].reshape(half, REST_COLUMNS)
        part = jnp.dot(o_buf[rows, :], w_buf[lax.rem(n, 3)], preferred_element_type=f32)
        out_buf[lax.rem(n, 2), rows, :] = (part + so_far).astype(bf16)

    first = jnp.int32(0)
    for i in range(2):
        w_copy(first, i).start()
    for i in range(pieces // 2):
        o_copy(i).start()
        sum_copy(first, i).start()
    for i in range(2):
        w_copy(first, i).wait()
    for h in range(2):
        for i in range(h * pieces // 2, (h + 1) * pieces // 2):
            o_copy(i).wait()
            sum_copy(first, i).wait()
        if h == 0:
            for i in range(pieces // 2, pieces):
                o_copy(i).start()
                sum_copy(first, i).start()
        else:
            start(first + 1)
        product(first, h)
    start(first + 2)
    for i in range(pieces):
        out_copy(first, i).start()

    def part(n, _):
        @pl.when(n + 2 < n_parts)
        def _():
            start(n + 2)

        @pl.when(n >= 2)
        def _():
            for i in range(pieces):
                out_copy(n - 2, i).wait()

        for i in range(2):
            w_copy(n, i).wait()
        for i in range(pieces):
            sum_copy(n, i).wait()
        for i in range(2):
            product(n, i)
        for i in range(pieces):
            out_copy(n, i).start()
        return 0

    lax.fori_loop(1, n_parts, part, 0)
    for n in range(n_parts - 2, n_parts):
        for i in range(pieces):
            out_copy(n, i).wait()


def solution(mesh):
    n_seq = mesh.shape["seq"]

    def per_device(tokens, theta_q, theta_k, theta_v, w_out, w_init, inner_lr):
        n_batch, tok_dev, width_d = tokens.shape
        n_heads, head_dim, _ = w_init.shape
        n_groups = n_heads // HEADS_PER_GROUP
        n_rows, width = n_batch * tok_dev, n_heads * head_dim
        flat = tokens.reshape(n_rows, width_d)
        hbm, smem = pl.BlockSpec(memory_space=pl.ANY), pl.BlockSpec(memory_space=pltpu.SMEM)
        sum_slots = n_rows // (n_batch * head_dim)
        o, first_sum = pl.pallas_call(
            functools.partial(fused_kernel, n_seq, n_batch, tok_dev, n_groups),
            out_shape=(jax.ShapeDtypeStruct((n_batch, tok_dev, width - 256 * N_FIRST), bf16), jax.ShapeDtypeStruct((sum_slots, n_batch, head_dim, width_d), f32)),
            in_specs=[hbm] * 6 + [smem], out_specs=(hbm, hbm),
            scratch_shapes=[pltpu.VMEM((n_rows, width_d), bf16), pltpu.VMEM((3, n_groups, n_batch, tok_dev, 256), bf16),
                            pltpu.VMEM((2, width_d, 256), bf16), pltpu.VMEM((n_rows, 256), bf16), pltpu.VMEM((n_batch, tok_dev, 256), bf16),
                            pltpu.VMEM((n_groups + max(0, 2 * sum_slots - N_FIRST), n_batch, head_dim, 4 * head_dim), f32),
                            pltpu.VMEM((n_batch, head_dim, 4 * head_dim), f32), pltpu.VMEM((n_batch, head_dim, 4 * head_dim), f32),
                            pltpu.VMEM((HEADS_PER_GROUP, head_dim, head_dim), f32),
                            pltpu.SemaphoreType.DMA((2,)), pltpu.SemaphoreType.DMA((2,)), pltpu.SemaphoreType.DMA, pltpu.SemaphoreType.DMA((2,)),
                            pltpu.SemaphoreType.DMA, pltpu.SemaphoreType.DMA, pltpu.SemaphoreType.DMA((n_groups,))],
            compiler_params=pltpu.CompilerParams(collective_id=0, has_side_effects=True, vmem_limit_bytes=67043328),
            name="fused",
        )(flat, theta_k, theta_v, theta_q, w_out, w_init, inner_lr)
        depth = width - 256 * N_FIRST
        result = pl.pallas_call(
            rest_kernel,
            out_shape=jax.ShapeDtypeStruct((n_rows, width_d), bf16),
            in_specs=[hbm] * 3, out_specs=hbm,
            scratch_shapes=[pltpu.VMEM((n_rows, depth), bf16), pltpu.VMEM((3, depth, REST_COLUMNS), bf16),
                            pltpu.VMEM((3, sum_slots, n_batch, head_dim, REST_COLUMNS), f32), pltpu.VMEM((2, n_rows, REST_COLUMNS), bf16),
                            pltpu.SemaphoreType.DMA((sum_slots,)), pltpu.SemaphoreType.DMA((3, 2)), pltpu.SemaphoreType.DMA((3, sum_slots)), pltpu.SemaphoreType.DMA((2, sum_slots))],
            compiler_params=pltpu.CompilerParams(vmem_limit_bytes=67043328),
            name="rest",
        )(o.reshape(n_rows, depth), w_out, first_sum)
        return result.reshape(n_batch, tok_dev, width_d)

    tok_spec = P("data", "seq", None)
    return jax.shard_map(per_device, mesh=mesh, in_specs=(tok_spec, P(), P(), P(), P(), P(), P()), out_specs=tok_spec, check_vma=False)
```

```python
import functools

import jax
import jax.numpy as jnp
from jax import lax
from jax.experimental import pallas as pl
from jax.experimental.pallas import tpu as pltpu
from jax.sharding import PartitionSpec as P

MINI_BATCH = 16
HEADS_PER_GROUP = 4
SCHEDULE = ((0, 7, (0, 0, 0, 0, 0)), (1, 6, (0, 0, 0, 0, 0)), (3, 4, (0, 0, 0, 0, 0)), (3, 1, (0, 0, 0, 0, 0)),
            (4, 0, (0, 3, 3, 3, 3)), (4, 0, (0, 3, 3, 3, 3)), (5, 0, (3, 6, 6, 6, 6)), (5, 0, (4, 7, 7, 7, 7)))
N_FIRST = 7
REST_COLUMNS = 512
bf16, f32 = jnp.bfloat16, jnp.float32


def split3(x):
    a = x.astype(bf16)
    rest = x - a.astype(f32)
    b = rest.astype(bf16)
    return a, b, (rest - b.astype(f32)).astype(bf16)


def per_head_rows(x):
    rows = []
    for half in range(2):
        y = x[:, :, half * 128:(half + 1) * 128]
        turned, low = pltpu.roll(y, 64, 2), low_lanes(y.shape)
        rows += [jnp.where(low, y, turned), jnp.where(low, turned, y)]
    return rows


def low_lanes(shape):
    return lax.broadcasted_iota(jnp.int32, shape, 2) < 64


def under(rows):
    n, t, width = rows[0].shape
    return jnp.concatenate([r.reshape(n, 1, t, width) for r in rows], axis=1).reshape(n, t * len(rows), width)


def own_columns(z, first):
    a, b, c, d = (z[:, first + i * MINI_BATCH:first + (i + 1) * MINI_BATCH, (i // 2) * 128:(i // 2 + 1) * 128] for i in range(4))
    low = low_lanes(a.shape)
    return jnp.concatenate([jnp.where(low, a, b), jnp.where(low, c, d)], axis=2)


def times_w(rows, w):
    m = under(rows)
    return jnp.concatenate([m, m], axis=2), jnp.concatenate([*split3(w), jnp.zeros(w.shape, bf16)], axis=1)


def k_transposed_times(k_rows, r):
    zero = jnp.zeros((*r.shape[:2], 128), bf16)
    low = low_lanes(zero.shape)
    rows = []
    for part in split3(r):
        a, b = part[:, :, :128], part[:, :, 128:]
        rows += [jnp.concatenate(pair, axis=2) for pair in (
            (jnp.where(low, a, zero), zero), (jnp.where(low, zero, a), zero), (zero, jnp.where(low, b, zero)), (zero, jnp.where(low, zero, b)))]
    rhs = jnp.concatenate([under(rows), jnp.zeros((r.shape[0], 4 * MINI_BATCH, 256), bf16)], axis=1)
    twice = under(k_rows + k_rows)
    turned = [twice[i].T[:64] for i in range(r.shape[0])]
    return [jnp.concatenate([t, t], axis=1) for t in turned], rhs


def fused_kernel(n_seq, n_batch, tok_dev, n_groups, x_hbm, theta_k_hbm, theta_v_hbm, theta_q_hbm, w_out_hbm, w_init_hbm, lr_ref, o_hbm, sum_hbm,
                 x_buf, kvq_buf, theta_buf, tile_buf, o_buf, w_buf, w_now, w_send, init_buf, x_sem, theta_sem, out_sem, sum_sem, init_sem, send_sem, recv_sem):
    me = lax.axis_index("seq")
    lag, n_late = jnp.int32(0), jnp.int32(0)
    for place, (ahead, late, _) in enumerate(SCHEDULE):
        lag = jnp.where(me == place, ahead, lag)
        n_late = jnp.where(me == place, late, n_late)

    outs_beside = (n_late == 0) & (lag + 1 + N_FIRST >= n_groups)

    def outs_before(g):
        n = jnp.int32(0)
        for place, (_, _, counts) in enumerate(SCHEDULE):
            for i, count in enumerate(counts):
                n = jnp.where((me == place) & (g >= N_FIRST + i), count, n)
        return n

    n_tiles = 3 * n_groups
    n_out_tiles = sum_hbm.shape[0]
    w_first = w_buf.shape[0] - n_groups
    first_depth = N_FIRST * 256
    n_rows = n_batch * tok_dev
    n_steps = tok_dev // MINI_BATCH
    chunk = n_rows // n_steps
    depth = x_buf.shape[1]
    thetas = (theta_k_hbm, theta_v_hbm, theta_q_hbm)
    barrier = pltpu.get_barrier_semaphore()

    def columns(g):
        return pl.ds(pl.multiple_of(g * 256, 256), 256)

    def tile_at(c):
        early, body = 2 * n_late, c - 2 * n_late
        kind = jnp.where(c < early, lax.rem(c, 2), jnp.where(c < n_tiles - n_late, lax.rem(body, 3), 2))
        g = jnp.where(c < early, c // 2, jnp.where(c < n_tiles - n_late, n_late + body // 3, c - (n_tiles - n_late)))
        return kind, g

    def start_theta(c):
        kind, g = tile_at(c)
        for i in range(3):
            @pl.when((kind == i) & (c < n_tiles))
            def _():
                pltpu.make_async_copy(thetas[i].at[:, columns(g)], theta_buf.at[lax.rem(c, 2)], theta_sem.at[lax.rem(c, 2)]).start()

        @pl.when((c >= n_tiles) & (c < n_tiles + n_out_tiles))
        def _():
            w_out_copy(c - n_tiles, lax.rem(c, 2)).start()

    def w_out_copy(n, slot):
        return pltpu.make_async_copy(w_out_hbm.at[pl.ds(0, first_depth), columns(n)], theta_buf.at[slot, pl.ds(0, first_depth)], theta_sem.at[slot])

    def wait_theta(c):
        slot = lax.rem(c, 2)
        pltpu.make_async_copy(theta_k_hbm.at[:, pl.ds(0, 256)], theta_buf.at[slot], theta_sem.at[slot]).wait()

    def result(g):
        return pltpu.make_async_copy(o_buf, o_hbm.at[:, :, columns(g - N_FIRST)], out_sem)

    def sum_copy(n):
        part = lax.rem(n, 2)
        return pltpu.make_async_copy(w_buf.at[pl.ds(part * sum_slots, sum_slots)], sum_hbm.at[n], sum_sem.at[part])

    def hand_on(g):
        return pltpu.make_async_remote_copy(w_send, w_buf.at[w_first + g], send_sem, recv_sem.at[g],
                                            device_id={"seq": lax.rem(me + 1, n_seq)}, device_id_type=pl.DeviceIdType.MESH)

    sum_slots = sum_hbm.shape[1]

    def first_w(g):
        return pltpu.make_async_copy(w_init_hbm.at[pl.ds(g * HEADS_PER_GROUP, HEADS_PER_GROUP)], init_buf, init_sem)

    def x_copy(i):
        rows = pl.ds(i * (n_rows // 2), n_rows // 2)
        return pltpu.make_async_copy(x_hbm.at[rows], x_buf.at[rows], x_sem.at[i])

    start_theta(jnp.int32(0))
    for i in range(2):
        x_copy(i).start()

    @pl.when(me == 0)
    def _():
        first_w(0).start()

    for peer in (lax.rem(me + 1, n_seq), lax.rem(me + n_seq - 1, n_seq)):
        pl.semaphore_signal(barrier, inc=1, device_id={"seq": peer}, device_id_type=pl.DeviceIdType.MESH)

    head = lax.broadcasted_iota(jnp.int32, (1, 256), 1) // 64

    half = n_batch // 2

    def tokens(kind, g, units, j):
        return kvq_buf[kind, g, units, pl.ds(j * MINI_BATCH, MINI_BATCH), :]

    def chain_step(g, eta, j, now, before, w_start=None):
        k_rows = z = None
        if now is not None:
            k_rows = per_head_rows(tokens(0, g, now, j)) if j < n_steps else []
            rows = k_rows + (per_head_rows(tokens(2, g, now, j - 1)) if j > 0 else [])
            lhs, rhs = times_w(rows, w_now[now] if w_start is None or j > 0 else w_start[now])
        if before is not None:
            units, step, keys, inputs = before
            r = (inputs - tokens(1, g, units, step).astype(f32)) * eta
            lhs_u, rhs_u = k_transposed_times(keys, r)
        prod, change = [], []
        for i in range(half):
            if now is not None:
                prod.append(jnp.dot(lhs[i], rhs[i], preferred_element_type=f32))
            if before is not None:
                change.append(jnp.dot(lhs_u[i], rhs_u[i], preferred_element_type=f32))
        if now is not None:
            prod = jnp.stack(prod)
            if j < n_steps:
                z = own_columns(prod, 0)
            if j > 0:
                o_buf[now, pl.ds((j - 1) * MINI_BATCH, MINI_BATCH), :] = own_columns(prod, 4 * MINI_BATCH if j < n_steps else 0).astype(bf16)
        if before is not None:
            w_now[units] = (w_now[units] if w_start is None or step > 0 else w_start[units]) - jnp.stack(change)
        return k_rows, z

    def chain(g, eta, fill, w_start=None):
        one, two = pl.ds(0, half), pl.ds(half, half)
        open_two = None
        for j in range(n_steps):
            put = fill(j)
            open_one = (one, j, *chain_step(g, eta, j, one, open_two, w_start))
            open_two = (two, j, *chain_step(g, eta, j, two, open_one, w_start))
            put()
        chain_step(g, eta, n_steps, None, open_two)

    def whole_tile(c, group=None):
        kind, g = tile_at(c)
        slot = lax.rem(c, 2)
        wait_theta(c)
        start_theta(c + 1)
        for i in range(2):
            rows = pl.ds(i * (n_rows // 2), n_rows // 2)
            if isinstance(c, int):
                x_copy(i).wait()
            pieces = [pl.ds(i * (n_rows // 2) + p * (n_rows // 4), n_rows // 4) for p in range(2)] if isinstance(c, int) else [rows]
            part = jnp.concatenate([jnp.dot(x_buf[p, :], theta_buf[slot], preferred_element_type=f32).astype(bf16) for p in pieces], axis=0)
            if group is not None and i == 0:
                last_results(group)
                before = tile_at(c - 1)
                kvq_buf[before[0], before[1]] = tile_buf[...].reshape(n_batch, tok_dev, 256)
            kvq_buf[kind, g, pl.ds(i * half, half)] = part.reshape(half, tok_dev, 256)

    def out_tile(n):
        c = n_tiles + n
        slot = lax.rem(c, 2)
        w_out_copy(n, slot).wait()
        start_theta(c + 1)

        @pl.when(n >= 2)
        def _():
            sum_copy(n - 2).wait()

        for i in range(2):
            rows = pl.ds(i * (n_rows // 2), n_rows // 2)
            lhs = jnp.concatenate([kvq_buf[2, g, pl.ds(i * half, half)].reshape(n_rows // 2, 256) for g in range(N_FIRST)], axis=1)
            part = jnp.dot(lhs, theta_buf[slot, :first_depth, :], preferred_element_type=f32)
            w_buf[pl.ds(lax.rem(n, 2) * sum_slots + i * (sum_slots // 2), sum_slots // 2)] = part.reshape(sum_slots // 2, *w_buf.shape[1:])
        sum_copy(n).start()

    def inner(g, first_time, c, n=None):
        slot = lax.rem(jnp.where(c < n_tiles, c, c - 1), 2) if n is None else lax.rem(c, 2)

        if n is None:
            @pl.when(c < n_tiles)
            def _():
                wait_theta(c)
                start_theta(c + 1)
        else:
            w_out_copy(n, slot).wait()
            start_theta(c + 1)

            @pl.when(n >= 2)
            def _():
                sum_copy(n - 2).wait()

        @pl.when((me == 0) & first_time)
        def _():
            first_w(g).wait()
            start = jnp.concatenate([init_buf[h] for h in range(HEADS_PER_GROUP)], axis=1)
            for b in range(n_batch):
                w_buf[w_first + g, b] = start

        @pl.when((me == 0) & first_time & (g + 1 < n_groups))
        def _():
            first_w(g + 1).start()

        @pl.when((me > 0) & first_time)
        def _():
            hand_on(g).wait_recv()

        @pl.when(jnp.where(first_time, g > N_FIRST, g == 0))
        def _():
            result(N_FIRST).wait()

        eta = jnp.zeros((1, 256), f32)
        for h in range(HEADS_PER_GROUP):
            eta = jnp.where(head == h, (2.0 / MINI_BATCH) * lr_ref[g * HEADS_PER_GROUP + h], eta)

        if n is not None:
            w_now[...] = w_buf[w_first + g]
            theta_buf[slot, first_depth:, :] = jnp.zeros((depth - first_depth, 256), bf16)

        if n is None:
            def fill(j):
                part = pl.ds(j * chunk, chunk)
                tile_part = jnp.dot(x_buf[part, :], theta_buf[slot], preferred_element_type=f32)

                def put():
                    tile_buf[part, :] = tile_part.astype(bf16)
                return put
        else:
            def fill(j):
                b, first = j * chunk // tok_dev, j * chunk % tok_dev
                lhs = jnp.concatenate([kvq_buf[2, i, b, pl.ds(first, chunk), :] for i in range(N_FIRST)], axis=1)
                lhs = jnp.concatenate([lhs, x_buf[pl.ds(j * chunk, chunk), :depth - first_depth]], axis=1)
                part = jnp.dot(lhs, theta_buf[slot], preferred_element_type=f32)
                rows = n_batch * w_buf.shape[2]
                at, within = j * chunk // rows, j * chunk % rows // w_buf.shape[2]

                def put():
                    w_buf[lax.rem(n, 2) * sum_slots + at, pl.ds(within, chunk // w_buf.shape[2])] = part.reshape(chunk // w_buf.shape[2], *w_buf.shape[2:])
                return put

        chain(g, eta, fill, w_buf.at[w_first + g] if n is None else None)

        @pl.when((me < n_seq - 1) & first_time & (g > 0))
        def _():
            hand_on(0).wait_send()

        @pl.when((me < n_seq - 1) & first_time)
        def _():
            w_send[...] = w_now[...]
            hand_on(g).start()

        if n is not None:
            sum_copy(n).start()

    def last_results(g):
        for units in (pl.ds(0, half), pl.ds(half, half)):
            chain_step(g, None, n_steps, units, None)
        kvq_buf[2, g] = o_buf[...]

    def send_result(g, first_time):
        @pl.when((g >= N_FIRST) & (jnp.logical_not(first_time) | (g >= n_late)))
        def _():
            result(g).start()

    def slot_body(s, _):
        @pl.when(s == 1)
        def _():
            pl.semaphore_wait(barrier, 2)

        first_time = s <= n_groups + lag
        g = jnp.where(first_time, s - 1 - lag, s - (n_groups + 1 + lag))
        fresh = s < n_groups
        c = jnp.where(fresh, 2 * s + jnp.maximum(s - n_late, 0), jnp.minimum(n_tiles - n_late + s - n_groups, n_tiles))
        beside_out = outs_beside & first_time & (g >= N_FIRST)
        n_out = jnp.where(beside_out, outs_before(g) + g - N_FIRST, 0)

        def outs(n, _):
            out_tile(n)
            return 0

        lax.fori_loop(jnp.where(beside_out, outs_before(g - 1) + g - N_FIRST, 0), n_out, outs, 0)

        @pl.when((g >= 0) & jnp.logical_not(beside_out))
        def _():
            inner(g, first_time, c)

        @pl.when(beside_out)
        def _():
            inner(g, first_time, n_tiles + n_out, n_out)

        @pl.when((g >= 0) & fresh)
        def _():
            whole_tile(c + 1, g)
            send_result(g, first_time)

        @pl.when((g >= 0) & jnp.logical_not(fresh))
        def _():
            last_results(g)
            send_result(g, first_time)

            @pl.when(c < n_tiles)
            def _():
                kind, of = tile_at(c)
                kvq_buf[kind, of] = tile_buf[...].reshape(n_batch, tok_dev, 256)

        def rest(i, _):
            whole_tile(c + i)
            return 0

        @pl.when(fresh)
        def _():
            lax.fori_loop(jnp.where(g >= 0, 2, jnp.where(s == 0, 1, 0)), jnp.where(s < n_late, 2, 3), rest, 0)
        return 0

    whole_tile(0)
    lax.fori_loop(0, n_groups + 1 + lag + n_late, slot_body, 0)

    def outs(n, _):
        out_tile(n)
        return 0

    lax.fori_loop(jnp.where(outs_beside, outs_before(n_groups) + n_groups - N_FIRST, 0), n_out_tiles, outs, 0)
    for n in range(2):
        sum_copy(n_out_tiles - 2 + n).wait()

    @pl.when(n_late == 0)
    def _():
        result(N_FIRST).wait()

    @pl.when(me < n_seq - 1)
    def _():
        hand_on(0).wait_send()


def rest_kernel(o_hbm, w_hbm, sum_hbm, out_hbm, o_buf, w_buf, sum_buf, out_buf, o_sem, w_sem, sum_sem, out_sem):
    n_rows, depth = o_buf.shape
    per_part, pieces = sum_buf.shape[1:3]
    piece, half = n_rows // pieces, n_rows // 2
    n_parts = out_hbm.shape[1] // REST_COLUMNS

    def columns(n):
        return pl.ds(pl.multiple_of(n * REST_COLUMNS, REST_COLUMNS), REST_COLUMNS)

    def o_copy(i):
        rows = pl.ds(i * piece, piece)
        return pltpu.make_async_copy(o_hbm.at[rows], o_buf.at[rows], o_sem.at[i])

    def w_copy(n, i):
        slot, rows = lax.rem(n, 3), depth // 2
        return pltpu.make_async_copy(w_hbm.at[pl.ds(w_hbm.shape[0] - depth + i * rows, rows), columns(n)],
                                     w_buf.at[slot, pl.ds(i * rows, rows)], w_sem.at[slot, i])

    def sum_copy(n, i):
        slot, at = lax.rem(n, 3), pl.ds(i % 2 * (pieces // 2), pieces // 2)
        return pltpu.make_async_copy(sum_hbm.at[n * per_part + i // 2, at], sum_buf.at[slot, i // 2, at], sum_sem.at[slot, i])

    def out_copy(n, i):
        slot, rows = lax.rem(n, 2), pl.ds(i * piece, piece)
        return pltpu.make_async_copy(out_buf.at[slot, rows], out_hbm.at[rows, columns(n)], out_sem.at[slot, i])

    def start(n):
        for i in range(2):
            w_copy(n, i).start()
        for i in range(2 * per_part):
            sum_copy(n, i).start()

    def product(n, i):
        rows = pl.ds(i * half, half)
        so_far = jnp.concatenate([sum_buf[lax.rem(n, 3), p, pl.ds(i * (pieces // 2), pieces // 2)].reshape(half, 256) for p in range(per_part)], axis=1)
        part = jnp.dot(o_buf[rows, :], w_buf[lax.rem(n, 3)], preferred_element_type=f32)
        out_buf[lax.rem(n, 2), rows, :] = (part + so_far).astype(bf16)

    first = jnp.int32(0)
    for i in range(2):
        w_copy(first, i).start()
    for i in range(pieces):
        o_copy(i).start()
    for i in range(2 * per_part):
        sum_copy(first, i).start()
    for i in range(2):
        w_copy(first, i).wait()
    start(first + 1)
    for h in range(2):
        for i in range(h * pieces // 2, (h + 1) * pieces // 2):
            o_copy(i).wait()
        for i in range(h, 2 * per_part, 2):
            sum_copy(first, i).wait()
        product(first, h)
        if h == 0:
            start(first + 2)
    for i in range(pieces):
        out_copy(first, i).start()

    def part(n, _):
        @pl.when(n + 2 < n_parts)
        def _():
            start(n + 2)

        @pl.when(n >= 2)
        def _():
            for i in range(pieces):
                out_copy(n - 2, i).wait()

        for i in range(2):
            w_copy(n, i).wait()
        for i in range(2 * per_part):
            sum_copy(n, i).wait()
        for i in range(2):
            product(n, i)
        for i in range(pieces):
            out_copy(n, i).start()
        return 0

    lax.fori_loop(1, n_parts, part, 0)
    for n in range(n_parts - 2, n_parts):
        for i in range(pieces):
            out_copy(n, i).wait()


def solution(mesh):
    n_seq = mesh.shape["seq"]

    def per_device(tokens, theta_q, theta_k, theta_v, w_out, w_init, inner_lr):
        n_batch, tok_dev, width_d = tokens.shape
        n_heads, head_dim, _ = w_init.shape
        n_groups = n_heads // HEADS_PER_GROUP
        n_rows, width = n_batch * tok_dev, n_heads * head_dim
        flat = tokens.reshape(n_rows, width_d)
        hbm, smem = pl.BlockSpec(memory_space=pl.ANY), pl.BlockSpec(memory_space=pltpu.SMEM)
        sum_slots = n_rows // (n_batch * head_dim)
        o, first_sum = pl.pallas_call(
            functools.partial(fused_kernel, n_seq, n_batch, tok_dev, n_groups),
            out_shape=(jax.ShapeDtypeStruct((n_batch, tok_dev, width - 256 * N_FIRST), bf16), jax.ShapeDtypeStruct((width_d // 256, sum_slots, n_batch, head_dim, 256), f32)),
            in_specs=[hbm] * 6 + [smem], out_specs=(hbm, hbm),
            scratch_shapes=[pltpu.VMEM((n_rows, width_d), bf16), pltpu.VMEM((3, n_groups, n_batch, tok_dev, 256), bf16),
                            pltpu.VMEM((2, width_d, 256), bf16), pltpu.VMEM((n_rows, 256), bf16), pltpu.VMEM((n_batch, tok_dev, 256), bf16),
                            pltpu.VMEM((n_groups + max(0, 2 * sum_slots - N_FIRST), n_batch, head_dim, 4 * head_dim), f32),
                            pltpu.VMEM((n_batch, head_dim, 4 * head_dim), f32), pltpu.VMEM((n_batch, head_dim, 4 * head_dim), f32),
                            pltpu.VMEM((HEADS_PER_GROUP, head_dim, head_dim), f32),
                            pltpu.SemaphoreType.DMA((2,)), pltpu.SemaphoreType.DMA((2,)), pltpu.SemaphoreType.DMA, pltpu.SemaphoreType.DMA((2,)),
                            pltpu.SemaphoreType.DMA, pltpu.SemaphoreType.DMA, pltpu.SemaphoreType.DMA((n_groups,))],
            compiler_params=pltpu.CompilerParams(collective_id=0, has_side_effects=True, vmem_limit_bytes=67043328),
            name="fused",
        )(flat, theta_k, theta_v, theta_q, w_out, w_init, inner_lr)
        depth = width - 256 * N_FIRST
        result = pl.pallas_call(
            rest_kernel,
            out_shape=jax.ShapeDtypeStruct((n_rows, width_d), bf16),
            in_specs=[hbm] * 3, out_specs=hbm,
            scratch_shapes=[pltpu.VMEM((n_rows, depth), bf16), pltpu.VMEM((3, depth, REST_COLUMNS), bf16),
                            pltpu.VMEM((3, REST_COLUMNS // 256, sum_slots, n_batch, head_dim, 256), f32), pltpu.VMEM((2, n_rows, REST_COLUMNS), bf16),
                            pltpu.SemaphoreType.DMA((sum_slots,)), pltpu.SemaphoreType.DMA((3, 2)), pltpu.SemaphoreType.DMA((3, 2 * REST_COLUMNS // 256)), pltpu.SemaphoreType.DMA((2, sum_slots))],
            compiler_params=pltpu.CompilerParams(vmem_limit_bytes=67043328),
            name="rest",
        )(o.reshape(n_rows, depth), w_out, first_sum)
        return result.reshape(n_batch, tok_dev, width_d)

    tok_spec = P("data", "seq", None)
    return jax.shard_map(per_device, mesh=mesh, in_specs=(tok_spec, P(), P(), P(), P(), P(), P()), out_specs=tok_spec, check_vma=False)
```

```python
import functools

import jax
import jax.numpy as jnp
from jax import lax
from jax.experimental import pallas as pl
from jax.experimental.pallas import tpu as pltpu
from jax.sharding import PartitionSpec as P

MINI_BATCH = 16
HEADS_PER_GROUP = 4
SCHEDULE = ((0, 7, (0, 0, 0, 0, 0)), (1, 6, (0, 0, 0, 0, 0)), (3, 4, (0, 0, 0, 0, 0)), (3, 1, (0, 0, 0, 0, 0)),
            (4, 0, (0, 3, 3, 3, 3)), (4, 0, (0, 3, 3, 3, 3)), (5, 0, (3, 6, 6, 6, 6)), (5, 0, (4, 7, 7, 7, 7)))
N_FIRST = 7
REST_COLUMNS = 512
bf16, f32 = jnp.bfloat16, jnp.float32


def split3(x):
    a = x.astype(bf16)
    rest = x - a.astype(f32)
    b = rest.astype(bf16)
    return a, b, (rest - b.astype(f32)).astype(bf16)


def per_head_rows(x):
    rows = []
    for half in range(2):
        y = x[:, :, half * 128:(half + 1) * 128]
        turned, low = pltpu.roll(y, 64, 2), low_lanes(y.shape)
        rows += [jnp.where(low, y, turned), jnp.where(low, turned, y)]
    return rows


def low_lanes(shape):
    return lax.broadcasted_iota(jnp.int32, shape, 2) < 64


def under(rows):
    n, t, width = rows[0].shape
    return jnp.concatenate([r.reshape(n, 1, t, width) for r in rows], axis=1).reshape(n, t * len(rows), width)


def own_columns(z, first):
    a, b, c, d = (z[:, first + i * MINI_BATCH:first + (i + 1) * MINI_BATCH, (i // 2) * 128:(i // 2 + 1) * 128] for i in range(4))
    low = low_lanes(a.shape)
    return jnp.concatenate([jnp.where(low, a, b), jnp.where(low, c, d)], axis=2)


def times_w(rows, w):
    m = under(rows)
    return jnp.concatenate([m, m], axis=2), jnp.concatenate([*split3(w), jnp.zeros(w.shape, bf16)], axis=1)


def k_transposed_times(k_rows, r):
    zero = jnp.zeros((*r.shape[:2], 128), bf16)
    low = low_lanes(zero.shape)
    rows = []
    for part in split3(r):
        a, b = part[:, :, :128], part[:, :, 128:]
        rows += [jnp.concatenate(pair, axis=2) for pair in (
            (jnp.where(low, a, zero), zero), (jnp.where(low, zero, a), zero), (zero, jnp.where(low, b, zero)), (zero, jnp.where(low, zero, b)))]
    rhs = jnp.concatenate([under(rows), jnp.zeros((r.shape[0], 4 * MINI_BATCH, 256), bf16)], axis=1)
    twice = under(k_rows + k_rows)
    turned = [twice[i].T[:64] for i in range(r.shape[0])]
    return [jnp.concatenate([t, t], axis=1) for t in turned], rhs


def fused_kernel(n_seq, n_batch, tok_dev, n_groups, x_hbm, theta_k_hbm, theta_v_hbm, theta_q_hbm, w_out_hbm, w_init_hbm, lr_ref, o_hbm, sum_hbm,
                 x_buf, kvq_buf, theta_buf, tile_buf, o_buf, w_buf, w_now, w_send, init_buf, x_sem, theta_sem, out_sem, sum_sem, init_sem, send_sem, recv_sem):
    me = lax.axis_index("seq")
    lag, n_late = jnp.int32(0), jnp.int32(0)
    for place, (ahead, late, _) in enumerate(SCHEDULE):
        lag = jnp.where(me == place, ahead, lag)
        n_late = jnp.where(me == place, late, n_late)

    outs_beside = (n_late == 0) & (lag + 1 + N_FIRST >= n_groups)

    def outs_before(g):
        n = jnp.int32(0)
        for place, (_, _, counts) in enumerate(SCHEDULE):
            for i, count in enumerate(counts):
                n = jnp.where((me == place) & (g >= N_FIRST + i), count, n)
        return n

    n_tiles = 3 * n_groups
    n_out_tiles = sum_hbm.shape[0]
    w_first = w_buf.shape[0] - n_groups
    first_depth = N_FIRST * 256
    n_rows = n_batch * tok_dev
    n_steps = tok_dev // MINI_BATCH
    chunk = n_rows // n_steps
    depth = x_buf.shape[1]
    thetas = (theta_k_hbm, theta_v_hbm, theta_q_hbm)
    barrier = pltpu.get_barrier_semaphore()

    def columns(g):
        return pl.ds(pl.multiple_of(g * 256, 256), 256)

    def tile_at(c):
        early, body = 2 * n_late, c - 2 * n_late
        kind = jnp.where(c < early, lax.rem(c, 2), jnp.where(c < n_tiles - n_late, lax.rem(body, 3), 2))
        g = jnp.where(c < early, c // 2, jnp.where(c < n_tiles - n_late, n_late + body // 3, c - (n_tiles - n_late)))
        return kind, g

    def start_theta(c):
        kind, g = tile_at(c)
        for i in range(3):
            @pl.when((kind == i) & (c < n_tiles))
            def _():
                pltpu.make_async_copy(thetas[i].at[:, columns(g)], theta_buf.at[lax.rem(c, 2)], theta_sem.at[lax.rem(c, 2)]).start()

        @pl.when((c >= n_tiles) & (c < n_tiles + n_out_tiles))
        def _():
            w_out_copy(c - n_tiles, lax.rem(c, 2)).start()

    def w_out_copy(n, slot):
        return pltpu.make_async_copy(w_out_hbm.at[pl.ds(0, first_depth), columns(n)], theta_buf.at[slot, pl.ds(0, first_depth)], theta_sem.at[slot])

    def wait_theta(c):
        slot = lax.rem(c, 2)
        pltpu.make_async_copy(theta_k_hbm.at[:, pl.ds(0, 256)], theta_buf.at[slot], theta_sem.at[slot]).wait()

    def result(g):
        return pltpu.make_async_copy(o_buf, o_hbm.at[:, :, columns(g - N_FIRST)], out_sem)

    def sum_copy(n):
        part = lax.rem(n, 2)
        return pltpu.make_async_copy(w_buf.at[pl.ds(part * sum_slots, sum_slots)], sum_hbm.at[n], sum_sem.at[part])

    def hand_on(g):
        return pltpu.make_async_remote_copy(w_send, w_buf.at[w_first + g], send_sem, recv_sem.at[g],
                                            device_id={"seq": lax.rem(me + 1, n_seq)}, device_id_type=pl.DeviceIdType.MESH)

    sum_slots = sum_hbm.shape[1]

    def first_w(g):
        return pltpu.make_async_copy(w_init_hbm.at[pl.ds(g * HEADS_PER_GROUP, HEADS_PER_GROUP)], init_buf, init_sem)

    def x_copy(i):
        rows = pl.ds(i * (n_rows // 2), n_rows // 2)
        return pltpu.make_async_copy(x_hbm.at[rows], x_buf.at[rows], x_sem.at[i])

    start_theta(jnp.int32(0))
    for i in range(2):
        x_copy(i).start()

    @pl.when(me == 0)
    def _():
        first_w(0).start()

    for peer in (lax.rem(me + 1, n_seq), lax.rem(me + n_seq - 1, n_seq)):
        pl.semaphore_signal(barrier, inc=1, device_id={"seq": peer}, device_id_type=pl.DeviceIdType.MESH)

    head = lax.broadcasted_iota(jnp.int32, (1, 256), 1) // 64

    half = n_batch // 2

    def tokens(kind, g, units, j):
        return kvq_buf[kind, g, units, pl.ds(j * MINI_BATCH, MINI_BATCH), :]

    def chain_step(g, eta, j, now, before, w_start=None):
        k_rows = z = None
        if now is not None:
            k_rows = per_head_rows(tokens(0, g, now, j)) if j < n_steps else []
            rows = k_rows + (per_head_rows(tokens(2, g, now, j - 1)) if j > 0 else [])
            lhs, rhs = times_w(rows, w_now[now] if w_start is None or j > 0 else w_start[now])
        if before is not None:
            units, step, keys, inputs = before
            r = (inputs - tokens(1, g, units, step).astype(f32)) * eta
            lhs_u, rhs_u = k_transposed_times(keys, r)
        prod, change = [], []
        for i in range(half):
            if now is not None:
                prod.append(jnp.dot(lhs[i], rhs[i], preferred_element_type=f32))
            if before is not None:
                change.append(jnp.dot(lhs_u[i], rhs_u[i], preferred_element_type=f32))
        if now is not None:
            prod = jnp.stack(prod)
            if j < n_steps:
                z = own_columns(prod, 0)
            if j > 0:
                o_buf[now, pl.ds((j - 1) * MINI_BATCH, MINI_BATCH), :] = own_columns(prod, 4 * MINI_BATCH if j < n_steps else 0).astype(bf16)
        if before is not None:
            w_now[units] = (w_now[units] if w_start is None or step > 0 else w_start[units]) - jnp.stack(change)
        return k_rows, z

    def chain(g, eta, fill, w_start=None):
        one, two = pl.ds(0, half), pl.ds(half, half)
        open_two = None
        for j in range(n_steps):
            put = fill(j)
            open_one = (one, j, *chain_step(g, eta, j, one, open_two, w_start))
            open_two = (two, j, *chain_step(g, eta, j, two, open_one, w_start))
            put()
        chain_step(g, eta, n_steps, None, open_two)

    def whole_tile(c, group=None):
        kind, g = tile_at(c)
        slot = lax.rem(c, 2)
        wait_theta(c)
        start_theta(c + 1)
        for i in range(2):
            rows = pl.ds(i * (n_rows // 2), n_rows // 2)
            if isinstance(c, int):
                x_copy(i).wait()
            pieces = [pl.ds(i * (n_rows // 2) + p * (n_rows // 4), n_rows // 4) for p in range(2)] if isinstance(c, int) else [rows]
            part = jnp.concatenate([jnp.dot(x_buf[p, :], theta_buf[slot], preferred_element_type=f32).astype(bf16) for p in pieces], axis=0)
            if group is not None and i == 0:
                last_results(group)
                before = tile_at(c - 1)
                kvq_buf[before[0], before[1]] = tile_buf[...].reshape(n_batch, tok_dev, 256)
            kvq_buf[kind, g, pl.ds(i * half, half)] = part.reshape(half, tok_dev, 256)

    def out_tile(n):
        c = n_tiles + n
        slot = lax.rem(c, 2)
        w_out_copy(n, slot).wait()
        start_theta(c + 1)

        @pl.when(n >= 2)
        def _():
            sum_copy(n - 2).wait()

        for i in range(2):
            rows = pl.ds(i * (n_rows // 2), n_rows // 2)
            lhs = jnp.concatenate([kvq_buf[2, g, pl.ds(i * half, half)].reshape(n_rows // 2, 256) for g in range(N_FIRST)], axis=1)
            part = jnp.dot(lhs, theta_buf[slot, :first_depth, :], preferred_element_type=f32)
            w_buf[pl.ds(lax.rem(n, 2) * sum_slots + i * (sum_slots // 2), sum_slots // 2)] = part.reshape(sum_slots // 2, *w_buf.shape[1:])
        sum_copy(n).start()

    def inner(g, first_time, c, n=None):
        slot = lax.rem(jnp.where(c < n_tiles, c, c - 1), 2) if n is None else lax.rem(c, 2)

        if n is None:
            @pl.when(c < n_tiles)
            def _():
                wait_theta(c)
                start_theta(c + 1)
        else:
            w_out_copy(n, slot).wait()
            start_theta(c + 1)

            @pl.when(n >= 2)
            def _():
                sum_copy(n - 2).wait()

        @pl.when((me == 0) & first_time)
        def _():
            first_w(g).wait()
            start = jnp.concatenate([init_buf[h] for h in range(HEADS_PER_GROUP)], axis=1)
            for b in range(n_batch):
                w_buf[w_first + g, b] = start

        @pl.when((me == 0) & first_time & (g + 1 < n_groups))
        def _():
            first_w(g + 1).start()

        @pl.when((me > 0) & first_time)
        def _():
            hand_on(g).wait_recv()

        @pl.when(jnp.where(first_time, g > N_FIRST, g == 0))
        def _():
            result(N_FIRST).wait()

        eta = jnp.zeros((1, 256), f32)
        for h in range(HEADS_PER_GROUP):
            eta = jnp.where(head == h, (2.0 / MINI_BATCH) * lr_ref[g * HEADS_PER_GROUP + h], eta)

        if n is not None:
            w_now[...] = w_buf[w_first + g]
            theta_buf[slot, first_depth:, :] = jnp.zeros((depth - first_depth, 256), bf16)

        if n is None:
            def fill(j):
                part = pl.ds(j * chunk, chunk)
                tile_part = jnp.dot(x_buf[part, :], theta_buf[slot], preferred_element_type=f32)

                def put():
                    tile_buf[part, :] = tile_part.astype(bf16)
                return put
        else:
            def fill(j):
                b, first = j * chunk // tok_dev, j * chunk % tok_dev
                lhs = jnp.concatenate([kvq_buf[2, i, b, pl.ds(first, chunk), :] for i in range(N_FIRST)], axis=1)
                lhs = jnp.concatenate([lhs, x_buf[pl.ds(j * chunk, chunk), :depth - first_depth]], axis=1)
                part = jnp.dot(lhs, theta_buf[slot], preferred_element_type=f32)
                rows = n_batch * w_buf.shape[2]
                at, within = j * chunk // rows, j * chunk % rows // w_buf.shape[2]

                def put():
                    w_buf[lax.rem(n, 2) * sum_slots + at, pl.ds(within, chunk // w_buf.shape[2])] = part.reshape(chunk // w_buf.shape[2], *w_buf.shape[2:])
                return put

        chain(g, eta, fill, w_buf.at[w_first + g] if n is None else None)

        @pl.when((me < n_seq - 1) & first_time & (g > 0))
        def _():
            hand_on(0).wait_send()

        @pl.when((me < n_seq - 1) & first_time)
        def _():
            w_send[...] = w_now[...]
            hand_on(g).start()

        if n is not None:
            sum_copy(n).start()

    def last_results(g):
        for units in (pl.ds(0, half), pl.ds(half, half)):
            chain_step(g, None, n_steps, units, None)
        kvq_buf[2, g] = o_buf[...]

    def send_result(g, first_time):
        @pl.when((g >= N_FIRST) & (jnp.logical_not(first_time) | (g >= n_late)))
        def _():
            result(g).start()

    def slot_body(s, _):
        @pl.when(s == 1)
        def _():
            pl.semaphore_wait(barrier, 2)

        first_time = s <= n_groups + lag
        g = jnp.where(first_time, s - 1 - lag, s - (n_groups + 1 + lag))
        fresh = s < n_groups
        c = jnp.where(fresh, 2 * s + jnp.maximum(s - n_late, 0), jnp.minimum(n_tiles - n_late + s - n_groups, n_tiles))
        beside_out = outs_beside & first_time & (g >= N_FIRST)
        n_out = jnp.where(beside_out, outs_before(g) + g - N_FIRST, 0)

        def outs(n, _):
            out_tile(n)
            return 0

        lax.fori_loop(jnp.where(beside_out, outs_before(g - 1) + g - N_FIRST, 0), n_out, outs, 0)

        @pl.when((g >= 0) & jnp.logical_not(beside_out))
        def _():
            inner(g, first_time, c)

        @pl.when(beside_out)
        def _():
            inner(g, first_time, n_tiles + n_out, n_out)

        @pl.when((g >= 0) & fresh)
        def _():
            whole_tile(c + 1, g)
            send_result(g, first_time)

        @pl.when((g >= 0) & jnp.logical_not(fresh))
        def _():
            last_results(g)
            send_result(g, first_time)

            @pl.when(c < n_tiles)
            def _():
                kind, of = tile_at(c)
                kvq_buf[kind, of] = tile_buf[...].reshape(n_batch, tok_dev, 256)

        def rest(i, _):
            whole_tile(c + i)
            return 0

        @pl.when(fresh)
        def _():
            lax.fori_loop(jnp.where(g >= 0, 2, jnp.where(s == 0, 1, 0)), jnp.where(s < n_late, 2, 3), rest, 0)
        return 0

    whole_tile(0)
    lax.fori_loop(0, n_groups + 1 + lag + n_late, slot_body, 0)

    def outs(n, _):
        out_tile(n)
        return 0

    lax.fori_loop(jnp.where(outs_beside, outs_before(n_groups) + n_groups - N_FIRST, 0), n_out_tiles, outs, 0)
    for n in range(2):
        sum_copy(n_out_tiles - 2 + n).wait()

    @pl.when(n_late == 0)
    def _():
        result(N_FIRST).wait()

    @pl.when(me < n_seq - 1)
    def _():
        hand_on(0).wait_send()


def rest_kernel(o_hbm, w_hbm, sum_hbm, out_hbm, o_buf, w_buf, sum_buf, out_buf, o_sem, w_sem, sum_sem, out_sem):
    n_rows, depth = o_buf.shape
    per_part, pieces = sum_buf.shape[1:3]
    piece, half = n_rows // pieces, n_rows // 2
    n_parts = out_hbm.shape[1] // REST_COLUMNS

    def columns(n):
        return pl.ds(pl.multiple_of(n * REST_COLUMNS, REST_COLUMNS), REST_COLUMNS)

    def o_copy(i):
        rows = pl.ds(i * piece, piece)
        return pltpu.make_async_copy(o_hbm.at[rows], o_buf.at[rows], o_sem.at[i])

    def w_copy(n, i):
        slot, rows = lax.rem(n, 3), depth // 2
        return pltpu.make_async_copy(w_hbm.at[pl.ds(w_hbm.shape[0] - depth + i * rows, rows), columns(n)],
                                     w_buf.at[slot, pl.ds(i * rows, rows)], w_sem.at[slot, i])

    def sum_copy(n, i):
        slot, at = lax.rem(n, 3), pl.ds(i % 2 * (pieces // 2), pieces // 2)
        return pltpu.make_async_copy(sum_hbm.at[n * per_part + i // 2, at], sum_buf.at[slot, i // 2, at], sum_sem.at[slot, i])

    def out_copy(n, i):
        slot, rows = lax.rem(n, 2), pl.ds(i * piece, piece)
        return pltpu.make_async_copy(out_buf.at[slot, rows], out_hbm.at[rows, columns(n)], out_sem.at[slot, i])

    def start(n):
        for i in range(2):
            w_copy(n, i).start()
        for i in range(2 * per_part):
            sum_copy(n, i).start()

    def product(n, i):
        rows = pl.ds(i * half, half)
        so_far = jnp.concatenate([sum_buf[lax.rem(n, 3), p, pl.ds(i * (pieces // 2), pieces // 2)].reshape(half, 256) for p in range(per_part)], axis=1)
        part = jnp.dot(o_buf[rows, :], w_buf[lax.rem(n, 3)], preferred_element_type=f32)
        out_buf[lax.rem(n, 2), rows, :] = (part + so_far).astype(bf16)

    first = jnp.int32(0)
    for i in range(2):
        w_copy(first, i).start()
    def start_half(h):
        for i in range(h * pieces // 2, (h + 1) * pieces // 2):
            o_copy(i).start()
        for i in range(h, 2 * per_part, 2):
            sum_copy(first, i).start()

    def wait_half(h):
        for i in range(h * pieces // 2, (h + 1) * pieces // 2):
            o_copy(i).wait()
        for i in range(h, 2 * per_part, 2):
            sum_copy(first, i).wait()

    start_half(0)
    for i in range(2):
        w_copy(first, i).wait()
    start_half(1)
    wait_half(0)
    start(first + 1)
    product(first, 0)
    wait_half(1)
    start(first + 2)
    product(first, 1)
    for i in range(pieces):
        out_copy(first, i).start()

    def part(n, _):
        @pl.when(n + 2 < n_parts)
        def _():
            start(n + 2)

        @pl.when(n >= 2)
        def _():
            for i in range(pieces):
                out_copy(n - 2, i).wait()

        for i in range(2):
            w_copy(n, i).wait()
        for i in range(2 * per_part):
            sum_copy(n, i).wait()
        for i in range(2):
            product(n, i)
        for i in range(pieces):
            out_copy(n, i).start()
        return 0

    lax.fori_loop(1, n_parts, part, 0)
    for n in range(n_parts - 2, n_parts):
        for i in range(pieces):
            out_copy(n, i).wait()


def solution(mesh):
    n_seq = mesh.shape["seq"]

    def per_device(tokens, theta_q, theta_k, theta_v, w_out, w_init, inner_lr):
        n_batch, tok_dev, width_d = tokens.shape
        n_heads, head_dim, _ = w_init.shape
        n_groups = n_heads // HEADS_PER_GROUP
        n_rows, width = n_batch * tok_dev, n_heads * head_dim
        flat = tokens.reshape(n_rows, width_d)
        hbm, smem = pl.BlockSpec(memory_space=pl.ANY), pl.BlockSpec(memory_space=pltpu.SMEM)
        sum_slots = n_rows // (n_batch * head_dim)
        o, first_sum = pl.pallas_call(
            functools.partial(fused_kernel, n_seq, n_batch, tok_dev, n_groups),
            out_shape=(jax.ShapeDtypeStruct((n_batch, tok_dev, width - 256 * N_FIRST), bf16), jax.ShapeDtypeStruct((width_d // 256, sum_slots, n_batch, head_dim, 256), f32)),
            in_specs=[hbm] * 6 + [smem], out_specs=(hbm, hbm),
            scratch_shapes=[pltpu.VMEM((n_rows, width_d), bf16), pltpu.VMEM((3, n_groups, n_batch, tok_dev, 256), bf16),
                            pltpu.VMEM((2, width_d, 256), bf16), pltpu.VMEM((n_rows, 256), bf16), pltpu.VMEM((n_batch, tok_dev, 256), bf16),
                            pltpu.VMEM((n_groups + max(0, 2 * sum_slots - N_FIRST), n_batch, head_dim, 4 * head_dim), f32),
                            pltpu.VMEM((n_batch, head_dim, 4 * head_dim), f32), pltpu.VMEM((n_batch, head_dim, 4 * head_dim), f32),
                            pltpu.VMEM((HEADS_PER_GROUP, head_dim, head_dim), f32),
                            pltpu.SemaphoreType.DMA((2,)), pltpu.SemaphoreType.DMA((2,)), pltpu.SemaphoreType.DMA, pltpu.SemaphoreType.DMA((2,)),
                            pltpu.SemaphoreType.DMA, pltpu.SemaphoreType.DMA, pltpu.SemaphoreType.DMA((n_groups,))],
            compiler_params=pltpu.CompilerParams(collective_id=0, has_side_effects=True, vmem_limit_bytes=67043328),
            name="fused",
        )(flat, theta_k, theta_v, theta_q, w_out, w_init, inner_lr)
        depth = width - 256 * N_FIRST
        result = pl.pallas_call(
            rest_kernel,
            out_shape=jax.ShapeDtypeStruct((n_rows, width_d), bf16),
            in_specs=[hbm] * 3, out_specs=hbm,
            scratch_shapes=[pltpu.VMEM((n_rows, depth), bf16), pltpu.VMEM((3, depth, REST_COLUMNS), bf16),
                            pltpu.VMEM((3, REST_COLUMNS // 256, sum_slots, n_batch, head_dim, 256), f32), pltpu.VMEM((2, n_rows, REST_COLUMNS), bf16),
                            pltpu.SemaphoreType.DMA((sum_slots,)), pltpu.SemaphoreType.DMA((3, 2)), pltpu.SemaphoreType.DMA((3, 2 * REST_COLUMNS // 256)), pltpu.SemaphoreType.DMA((2, sum_slots))],
            compiler_params=pltpu.CompilerParams(vmem_limit_bytes=67043328),
            name="rest",
        )(o.reshape(n_rows, depth), w_out, first_sum)
        return result.reshape(n_batch, tok_dev, width_d)

    tok_spec = P("data", "seq", None)
    return jax.shard_map(per_device, mesh=mesh, in_specs=(tok_spec, P(), P(), P(), P(), P(), P()), out_specs=tok_spec, check_vma=False)
```
